32 devices in a mesh: seq: 16 (over z, y, x), head: 2 (over core).
Axes of the slice: x: 2, y: 2, z: 4, core: 2. Of those that a mesh axis runs over, the one named last changes fastest.
Arguments:
- queries: bfloat16 [3072, 32, 128], P('seq', 'head'), may hold values from -180 to 180
- key_rows: bfloat16 [3072, 8, 128], P('seq', 'head'), may hold values from -4.5 to 4.5
- value_rows: bfloat16 [3072, 8, 128], P('seq', 'head'), may hold values from -24 to 24
- windows: int32 [32], P('head'), may hold values from 768 to 1536, as said below
- sink_counts: int32 [32], P('head'), may hold values from 1 to 4, as said below
- sink_bias: float32 [32], P('head'), may hold values from 3 to 7
- out_weight: bfloat16 [4096, 4096], P('head'), may hold values from -0.09375 to 0.09375
Outputs:
- attn_out: bfloat16 [3072, 4096], P(('seq', 'head'))
The draws below stay inside these ranges and needn't reach their ends.
Inputs may be any that keep to these rules, and one draw needn't show every extreme that they name: `windows`: each head's window lies between 768 and 1536, and some head has exactly 1536. `sink_counts`: each head has 1 to 4 sink tokens, and some head has exactly 4.
All inputs are finite; a program needn't handle non-finite values.
Results may differ from the reference program's by a relative error of at most 0.018.
Values may be sent and summed in bfloat16 or wider, within the bound.
A program may use at most 128 MiB of HBM per device.

```python
import jax
import jax.numpy as jnp
from jax import lax

D = 4096
H = 32
KVH = 8
HD = 128
WINDOW = 1536
SINKS = 4
TOK_DEV = 192
TOKENS = 3072
N_SEQ = 16
N_HEAD = 2


def shared_keys(key):
    return jnp.clip(jax.random.normal(jax.random.fold_in(key, 11), (TOKENS, KVH, HD), jnp.float32), -4.5, 4.5)


def draw_key_rows(key, part):
    return shared_keys(key).astype(jnp.bfloat16)


def draw_queries(key, part):
    base = jnp.clip(jax.random.normal(jax.random.fold_in(key, 12), (TOKENS, H, HD), jnp.float32), -4.5, 4.5)
    return base.astype(jnp.bfloat16)


def draw_windows(key, part):
    spread = jax.random.randint(jax.random.fold_in(key, 21), (H,), WINDOW // 2, WINDOW + 1)
    chosen = jax.random.randint(jax.random.fold_in(key, 22), (), 0, H)
    return jnp.where(jnp.arange(H) == chosen, WINDOW, spread).astype(jnp.int32)


def draw_sink_counts(key, part):
    spread = jax.random.randint(jax.random.fold_in(key, 31), (H,), 1, SINKS + 1)
    chosen = jax.random.randint(jax.random.fold_in(key, 32), (), 0, H)
    return jnp.where(jnp.arange(H) == chosen, SINKS, spread).astype(jnp.int32)


def steps_of(stream_key, dims, split, least, high):
    def one(dim, blocks):
        draws = jax.random.uniform(jax.random.fold_in(jax.random.fold_in(stream_key, 6), dim), (blocks,), jnp.float32, least / len(split), high / len(split))
        return jnp.repeat(jnp.exp(draws), dims[dim] // blocks).reshape((-1,) + (1,) * (len(dims) - dim - 1))

    level = one(*split[0])
    for cut in split[1:]:
        level = level * one(*cut)
    return level


def noise(own_key, extent, scale, most, pieces=(), held_as=jnp.bfloat16):
    values = jax.random.normal(own_key, extent, jnp.float32) * scale
    if len(pieces) > 0:
        values = steps_of(own_key, extent, pieces, -0.22, 0.18) * values
    return jnp.clip(values, min=-most, max=most).astype(held_as)


def setup_inputs(seed: int = 0) -> dict:
    streams_of = jax.random.split(jax.random.key(seed), 8)
    return {
        "queries": draw_queries(jax.random.fold_in(streams_of[7], 71), 0),
        "key_rows": draw_key_rows(jax.random.fold_in(streams_of[7], 71), 0),
        "value_rows": noise(streams_of[2], (TOKENS, KVH, HD), 4.0, 24.0, ((0, 16), (1, 2))),
        "windows": draw_windows(jax.random.fold_in(streams_of[7], 71), 0),
        "sink_counts": draw_sink_counts(jax.random.fold_in(streams_of[7], 71), 0),
        "sink_bias": jnp.clip(3.0 + 4.0 * jax.random.uniform(streams_of[5], (H,), jnp.float32) ** steps_of(streams_of[5], (H,), ((0, 2),), -0.2, 0.2), 3.0, 7.0),
        "out_weight": noise(streams_of[6], (H * HD, D), (H * HD) ** -0.5, 0.09375, ((0, 2),)),
    }


def attend_block(query_block, band_rows, sink_rows, first_pos, windows, sink_counts, sink_bias):
    tok_rows, local_heads, head_width = query_block.shape
    kv_local = band_rows.shape[2]
    group_size = local_heads // kv_local
    band_span = band_rows.shape[1]
    all_keys = jnp.concatenate([sink_rows[0], band_rows[0]], axis=0)
    all_values = jnp.concatenate([sink_rows[1], band_rows[1]], axis=0)
    grouped = query_block.reshape(tok_rows, kv_local, group_size, head_width)
    score_scale = 1.0 / (head_width ** 0.5)
    scores = jnp.einsum("tkgd,skd->kgts", grouped.astype(jnp.float32), all_keys.astype(jnp.float32)) * score_scale
    query_pos = first_pos + jnp.arange(tok_rows, dtype=jnp.int32)
    band_pos = first_pos + tok_rows - band_span + jnp.arange(band_span, dtype=jnp.int32)
    sink_pos = jnp.arange(SINKS, dtype=jnp.int32)
    key_pos = jnp.concatenate([sink_pos, band_pos])
    is_sink = jnp.concatenate([jnp.ones((SINKS,), bool), jnp.zeros((band_span,), bool)])
    head_window = windows.reshape(kv_local, group_size, 1, 1)
    head_sinks = sink_counts.reshape(kv_local, group_size, 1, 1)
    head_bias = sink_bias.reshape(kv_local, group_size, 1, 1)
    distance = query_pos[:, None] - key_pos[None, :]
    visible = (distance >= 0) & jnp.where(is_sink, key_pos < head_sinks, (distance < head_window) & (key_pos >= head_sinks))
    scores = scores + jnp.where(is_sink, head_bias, 0.0)
    masked = jnp.where(visible, scores, -1e30)
    highest = jnp.max(masked, axis=-1, keepdims=True)
    weights = jnp.where(visible, jnp.exp(masked - highest), 0.0)
    normed = (weights / jnp.sum(weights, axis=-1, keepdims=True)).astype(jnp.bfloat16)
    mixed = jnp.einsum("kgts,skd->tkgd", normed.astype(jnp.float32), all_values.astype(jnp.float32))
    return mixed.astype(jnp.bfloat16).reshape(tok_rows, local_heads * head_width)


def reference(queries, key_rows, value_rows, windows, sink_counts, sink_bias, out_weight):
    stacked = jnp.stack([key_rows, value_rows])
    padding = jnp.zeros((2, WINDOW, KVH, HD), jnp.bfloat16)
    padded = jnp.concatenate([padding, stacked], axis=1)
    sink_rows = stacked[:, :SINKS]

    def one_shard(shard_index):
        first_pos = (shard_index * TOK_DEV).astype(jnp.int32)
        query_block = lax.dynamic_slice_in_dim(queries, first_pos, TOK_DEV, 0)
        band_rows = lax.dynamic_slice_in_dim(padded, first_pos, TOK_DEV + WINDOW, 1)
        return attend_block(query_block, band_rows, sink_rows, first_pos, windows, sink_counts, sink_bias)

    attended = lax.map(one_shard, jnp.arange(N_SEQ, dtype=jnp.int32)).reshape(TOKENS, H * HD)
    group_rows = H * HD // N_HEAD
    total = jnp.zeros((TOKENS, D), jnp.float32)
    for member in range(N_HEAD):
        lower = member * group_rows
        term = jnp.dot(attended[:, lower:lower + group_rows], out_weight[lower:lower + group_rows], preferred_element_type=jnp.float32)
        total = total + lax.optimization_barrier(term.astype(jnp.bfloat16)).astype(jnp.float32)
    return total.astype(jnp.bfloat16)
```

```python
import functools
import heapq

import jax
import jax.numpy as jnp
from jax import lax
from jax.experimental import pallas as pl
from jax.experimental.pallas import tpu as pltpu
from jax.sharding import PartitionSpec as P

WINDOW = 1536
SINKS = 4
PLANE = 4
SINK_ROWS = 16
HIDDEN = -1e30
LOG2E = 1.4426950408889634
MESH = pl.DeviceIdType.MESH

KINDS = 8
SINK_EARLY, SINK_MID, SINK_LATE, CLOSE = 8, 9, 10, 11
CHUNK_US, HOP_US = 2.1, 1.7
BITS, PER_WORD = 6, 5


def kinds_of(p):
    b0, b1 = p % 2, p // 2
    px, py, pd = p ^ 1, p ^ 2, 3 - p
    return [(1, p), (2, p), (1, px), (1, py), (1, pd), (2 - 2 * b0, px), (2 - 2 * b1, py), (2 - 2 * b1, pd)]


def forwards(z, p, plane, src):
    b0, b1 = p % 2, p // 2
    px, py = p ^ 1, p ^ 2
    out = []
    if (plane, src) == (0, p):
        out.append(("z", z + 1, p, 1))
        if b0 == 0:
            out.append(("x", z, px, 0))
        if b1 == 0:
            out.append(("y", z, py, 0))
    if (plane, src) == (1, p):
        out += [("z", z + 1, p, 2), ("x", z, px, 1), ("y", z, py, 1)]
    if (plane, src) == (2, p):
        if b0 == 1:
            out.append(("x", z, px, 2))
        if b1 == 1:
            out.append(("y", z, py, 2))
    if (plane, src) == (1, px):
        out.append(("y", z, py, 1))
    if (plane, src) == (2 - 2 * b1, py):
        out.append(("x", z, px, plane))
    return out


def arrivals(heads):
    queue, free, landed, tick = [], {}, {}, 0
    for c in range(heads):
        for z in range(3):
            for p in range(PLANE):
                heapq.heappush(queue, (1e-3 * c, tick, z, p, 0, p, c))
                tick += 1
    while queue:
        t, _, z, p, plane, src, c = heapq.heappop(queue)
        landed[z, p, plane, src, c] = t
        for link, z_to, p_to, plane_to in forwards(z, p, plane, src):
            if z_to < 3:
                start = max(t, free.get((z, p, link), 0.0))
                free[z, p, link] = start + CHUNK_US
                heapq.heappush(queue, (start + CHUNK_US + HOP_US, tick, z_to, p_to, plane_to, src, c))
                tick += 1
    return landed


def agenda(heads):
    landed = arrivals(heads)
    plans = []
    for p in range(PLANE):
        due = [(landed[2, p, plane, src, c], k, c) for k, (plane, src) in enumerate(kinds_of(p)) for c in range(heads)]
        due += [(11.0, SINK_EARLY, 0), (19.3, SINK_MID, 0), (21.7, SINK_LATE, 0)]
        due.sort()
        last = [max(i for i, e in enumerate(due) if e[2] == c or e[1] == SINK_LATE) for c in range(heads)]
        plan, ready = [], 0
        for i, (_, k, c) in enumerate(due):
            plan.append(k * heads + c)
            while ready < heads - 1 and all(last[r] <= i for r in range(ready + 1)):
                plan.append(CLOSE * heads + ready)
                ready += 1
        assert ready == heads - 1 and max(plan) < 1 << BITS
        plans.append(plan)
    return plans


def kernel(
    n_seq, n_head, tile, wide, plans,
    win_ref, cnt_ref, bias_ref, k_hbm, v_hbm, q_hbm, w_hbm, out_ref,
    k_raw, v_raw, q_raw, k_wide, v_wide, q_wide,
    own, kv, sink, qt, low, few, lift, top, norm, acc, att, w, total, part, got,
    send_sem, recv_sem, sink_send, sink_recv, raw_sem, w_sem, part_send, part_recv,
):
    me, side = lax.axis_index("seq"), lax.axis_index("head")
    heads_kv, _, rows, width = own.shape
    lanes = qt.shape[2]
    group = lanes // rows
    heads = heads_kv * group
    model = w.shape[1]
    depth = group * width
    share = rows // n_head
    z, p = me // PLANE, lax.rem(me, PLANE)
    bit0, bit1 = lax.rem(p, 2), p // 2
    px, py = p + 1 - 2 * bit0, p + 2 - 4 * bit1
    pd = 3 - p
    base = z * PLANE
    n_z = n_seq // PLANE
    scale = LOG2E / width**0.5

    barrier = pltpu.get_barrier_semaphore()

    def greet(where):
        pl.semaphore_signal(barrier, inc=1, device_id=where, device_id_type=MESH)

    above, below = (z + 1 < n_z).astype(jnp.int32), (z > 0).astype(jnp.int32)
    loads = [
        pltpu.make_async_copy(source, target, raw_sem.at[i])
        for i, (source, target) in enumerate(((k_hbm, k_raw), (v_hbm, v_raw), (q_hbm, q_raw)))
    ]
    for load in loads:
        load.start()
    greet({"seq": base + px})
    greet({"seq": base + py})

    @pl.when(z + 1 < n_z)
    def _():
        greet({"seq": me + PLANE})

    @pl.when(z > 0)
    def _():
        greet({"seq": me - PLANE})

    for step in range(1, n_head):
        greet({"head": lax.rem(side + step, n_head)})

    def send(kind, src, plane, source, c, target):
        return pltpu.make_async_remote_copy(
            src_ref=src,
            dst_ref=kv.at[plane * PLANE + source, c],
            send_sem=send_sem.at[kind, c],
            recv_sem=recv_sem.at[plane * PLANE + source, c],
            device_id={"seq": target},
            device_id_type=MESH,
        )

    def landed(plane, source, c):
        send(0, own.at[c], plane, source, c, me).wait_recv()

    def held(plane, source, c):
        return kv.at[plane * PLANE + source, c]

    x_old, y_old = 2 * bit0, 2 * bit1
    x_from, y_from = 2 - 2 * bit0, 2 - 2 * bit1

    def sink_copy(way, source, target):
        return pltpu.make_async_remote_copy(
            src_ref=source,
            dst_ref=sink,
            send_sem=sink_send.at[way],
            recv_sem=sink_recv,
            device_id={"seq": target},
            device_id_type=MESH,
        )

    first_rows = own.at[:, :, pl.ds(0, SINK_ROWS)]

    for i, (raw, spread) in enumerate(((k_raw, k_wide), (v_raw, v_wide))):
        loads[i].wait()
        spread[...] = raw[...].astype(jnp.float32)
        for c in range(heads_kv):
            own[c, i] = spread[pl.ds(c, rows, stride=heads_kv), :].astype(jnp.bfloat16)
    pl.semaphore_wait(barrier, n_head + 1 + above + below)

    @pl.when(me == 0)
    def _():
        sink_copy(0, first_rows, base + px).start()
        sink_copy(1, first_rows, base + py).start()

        @pl.when(z + 1 < n_z)
        def _():
            sink_copy(2, first_rows, me + PLANE).start()
        sink[...] = own[:, :, :SINK_ROWS]

    for c in range(heads_kv):
        @pl.when(z + 1 < n_z)
        def _():
            send(0, own.at[c], 1, p, c, me + PLANE).start()

        @pl.when(x_old == 0)
        def _():
            send(2, own.at[c], 0, p, c, base + px).start()

        @pl.when(y_old == 0)
        def _():
            send(3, own.at[c], 0, p, c, base + py).start()

    def fetch(c):
        part_of = pl.ds(pl.multiple_of(c * depth, depth), depth)
        return pltpu.make_async_copy(w_hbm.at[part_of], w.at[part_of], w_sem.at[c])

    loads[2].wait()
    for c in range(heads_kv):
        fetch(c).start()
    q_wide[...] = q_raw[...].astype(jnp.float32)
    column = lax.broadcasted_iota(jnp.int32, (1, lanes), 1)
    for c in range(heads_kv):
        window, count, bias, token = (jnp.zeros((1, lanes), t) for t in (jnp.int32, jnp.int32, jnp.float32, jnp.int32))
        for g in range(group):
            mine = (column >= g * rows) & (column < (g + 1) * rows)
            h = c * group + g
            window = jnp.where(mine, win_ref[h], window)
            count = jnp.where(mine, cnt_ref[h], count)
            bias = jnp.where(mine, bias_ref[h], bias)
            token = jnp.where(mine, column - g * rows, token)
        token = token + me * rows
        low[c] = jnp.maximum(token - window, count - 1)
        few[c] = jnp.minimum(token, count - 1)
        lift[c] = bias * LOG2E
        picked = [q_wide[pl.ds(c * group + g, rows, stride=heads), :].astype(jnp.bfloat16) for g in range(group)]
        qt[c] = jnp.concatenate(picked, axis=0).T
        top[c] = jnp.full((1, lanes), HIDDEN, jnp.float32)
        norm[c] = jnp.zeros((1, lanes), jnp.float32)
        acc[c] = jnp.zeros((width, lanes), jnp.float32)

    def attend(block, c, shard, causal=False, sinks=False):
        keys, values = block[0], block[1]
        key_row = lax.broadcasted_iota(jnp.int32, (keys.shape[0], 1), 0)
        step = min(256, lanes)
        parts = [slice(n, n + step) for n in range(0, lanes, step)]
        scores = [jnp.dot(keys, qt[c, :, cols], preferred_element_type=jnp.float32) for cols in parts]
        turned = values.T
        olds = [top[c, :, cols] for cols in parts]
        weights, news, fades, sums = [], [], [], []
        for s, old, cols in zip(scores, olds, parts):
            s = s * scale
            if sinks:
                s = jnp.where(key_row <= few[c, :, cols], s + lift[c, :, cols], HIDDEN)
            else:
                seen = key_row > low[c, :, cols] - shard * rows
                if causal:
                    column = lax.broadcasted_iota(jnp.int32, (1, step), 1) + cols.start
                    seen = seen & (key_row <= lax.rem(column, rows))
                s = jnp.where(seen, s, HIDDEN)
            new = jnp.maximum(old, jnp.max(s, axis=0, keepdims=True))
            e = jnp.exp2(s - new)
            weights.append(e.astype(jnp.bfloat16))
            news.append(new)
            fades.append(jnp.exp2(old - new))
            sums.append(jnp.sum(e, axis=0, keepdims=True))
        adds = [jnp.dot(turned, e, preferred_element_type=jnp.float32) for e in weights]
        for new, fade, added, add, cols in zip(news, fades, sums, adds, parts):
            top[c, :, cols] = new
            norm[c, :, cols] = norm[c, :, cols] * fade + added
            acc[c, :, cols] = acc[c, :, cols] * fade + add

    def each(body):
        def one(c, carry):
            body(c)
            return carry
        lax.fori_loop(0, heads_kv, one, 0)

    each(lambda c: attend(own.at[c], c, me, causal=True))
    total[...] = jnp.zeros(total.shape, jnp.float32)

    def pass_on():
        sink_copy(0, sink, me).wait_recv()

        @pl.when(me == 1)
        def _():
            sink_copy(1, sink, base + py).start()

        @pl.when(z + 1 < n_z)
        def _():
            sink_copy(2, sink, me + PLANE).start()

    def close(c):
        mixed = (acc[c] / norm[c]).T.astype(jnp.bfloat16)
        for g in range(group):
            att[:, g * width:(g + 1) * width] = mixed[g * rows:(g + 1) * rows]
        fetch(c).wait()

    def rows_of(c):
        return pl.ds(pl.multiple_of(c * depth, depth), depth)

    n_words = (max(len(plan) for plan in plans) + PER_WORD - 1) // PER_WORD
    words = []
    for i in range(n_words):
        packed = []
        for plan in plans:
            value = 0
            for j, code in enumerate(plan[i * PER_WORD:(i + 1) * PER_WORD]):
                value += code << (BITS * j)
            packed.append(value)
        word = jnp.int32(packed[0])
        for q in range(1, PLANE):
            word = jnp.where(p == q, jnp.int32(packed[q]), word)
        words.append(word)

    def pick(index, choices):
        chosen = choices[-1]
        for i in range(len(choices) - 2, -1, -1):
            chosen = jnp.where(index == i, choices[i], chosen)
        return chosen

    def event(i, carry):
        word = pick(i // PER_WORD, words)
        code = lax.shift_right_logical(word, BITS * lax.rem(i, PER_WORD)) & ((1 << BITS) - 1)
        kind, c = code // heads_kv, lax.rem(code, heads_kv)
        plane = pick(kind, [1, 2, 1, 1, 1, x_from, y_from, y_from])
        source = pick(kind, [p, p, px, py, pd, px, py, pd])

        @pl.when((kind < KINDS) & (z >= plane))
        def _():
            landed(plane, source, c)

            @pl.when(kind == 0)
            def _():
                @pl.when(z + 1 < n_z)
                def _():
                    send(1, held(1, p, c), 2, p, c, me + PLANE).start()
                send(4, held(1, p, c), 1, p, c, base + px).start()
                send(5, held(1, p, c), 1, p, c, base + py).start()

            @pl.when((kind == 1) & (x_old == 2))
            def _():
                send(2, held(2, p, c), 2, p, c, base + px).start()

            @pl.when((kind == 1) & (y_old == 2))
            def _():
                send(3, held(2, p, c), 2, p, c, base + py).start()

            @pl.when(kind == 2)
            def _():
                send(6, held(1, px, c), 1, px, c, base + py).start()

            @pl.when(kind == 6)
            def _():
                send(7, held(y_from, py, c), y_from, py, c, base + px).start()

            attend(held(plane, source, c), c, base - plane * PLANE + source)

        turn = jnp.where(z <= 1, SINK_EARLY, jnp.where(z == 2, SINK_MID, SINK_LATE))

        @pl.when(kind == turn)
        def _():
            @pl.when(me > 0)
            def _():
                pass_on()
            each(lambda c: attend(sink.at[c], c, 0, sinks=True))

        @pl.when(kind == CLOSE)
        def _():
            close(c)

            def project(t, carry):
                cols = pl.ds(pl.multiple_of(t * wide, wide), wide)
                total[:, cols] += jnp.dot(att[...], w[rows_of(c), cols], preferred_element_type=jnp.float32)
                return carry
            lax.fori_loop(0, model // wide, project, 0)
        return carry
    lax.fori_loop(0, len(plans[0]), event, 0)

    close(heads_kv - 1)
    tiles = model // tile

    def give(t, step):
        target = lax.rem(side + step, n_head)
        return pltpu.make_async_remote_copy(
            src_ref=part.at[t, target],
            dst_ref=got.at[t, step - 1],
            send_sem=part_send.at[t, step - 1],
            recv_sem=part_recv.at[t, step - 1],
            device_id={"head": target},
            device_id_type=MESH,
        )

    def project(t, carry):
        cols = pl.ds(pl.multiple_of(t * tile, tile), tile)
        whole = total[:, cols] + jnp.dot(att[...], w[rows_of(heads_kv - 1), cols], preferred_element_type=jnp.float32)
        for d in range(n_head):
            part[t, d] = whole[d * share:(d + 1) * share].astype(jnp.bfloat16)

        @pl.when(t >= 1)
        def _():
            for step in range(1, n_head):
                give(t - 1, step).start()
        return carry
    lax.fori_loop(0, tiles, project, 0)
    for step in range(1, n_head):
        give(tiles - 1, step).start()

    def finish(t, carry):
        whole = part[t, side].astype(jnp.float32)
        for step in range(1, n_head):
            give(t, step).wait_recv()
            whole = whole + got[t, step - 1].astype(jnp.float32)
        out_ref[:, pl.ds(pl.multiple_of(t * tile, tile), tile)] = whole.astype(jnp.bfloat16)
        return carry
    lax.fori_loop(0, tiles, finish, 0)

    def sent(kind, plane, source, c, target):
        send(kind, held(plane, source, c), plane, source, c, target).wait_send()

    def drain(c):
        @pl.when(z + 1 < n_z)
        def _():
            sent(0, 1, p, c, me + PLANE)

        @pl.when(z >= x_old)
        def _():
            sent(2, x_old, p, c, base + px)

        @pl.when(z >= y_old)
        def _():
            sent(3, y_old, p, c, base + py)

        @pl.when(z >= 1)
        def _():
            @pl.when(z + 1 < n_z)
            def _():
                sent(1, 2, p, c, me + PLANE)
            sent(4, 1, p, c, base + px)
            sent(5, 1, p, c, base + py)
            sent(6, 1, px, c, base + py)

        @pl.when(z >= y_from)
        def _():
            sent(7, y_from, py, c, base + px)
    each(drain)

    @pl.when(me == 0)
    def _():
        sink_copy(0, sink, base + px).wait_send()

    @pl.when(me <= 1)
    def _():
        sink_copy(1, sink, base + py).wait_send()

    @pl.when(z + 1 < n_z)
    def _():
        sink_copy(2, sink, me + PLANE).wait_send()

    def gone(t, carry):
        for step in range(1, n_head):
            give(t, step).wait_send()
        return carry
    lax.fori_loop(0, tiles, gone, 0)


def shards(n_seq, n_head, queries, key_rows, value_rows, windows, sink_counts, sink_bias, out_weight):
    rows, heads, width = queries.shape
    kv_heads = key_rows.shape[1]
    group = heads // kv_heads
    lanes = group * rows
    depth, model = out_weight.shape
    assert (WINDOW - 1) // rows + 1 == 2 * PLANE and n_seq % PLANE == 0
    tile, wide = min(512, model), min(1024, model)
    tiles = model // tile
    share = rows // n_head
    bf16, f32, i32 = jnp.bfloat16, jnp.float32, jnp.int32
    vmem = pl.BlockSpec(memory_space=pltpu.VMEM)
    smem = pl.BlockSpec(memory_space=pltpu.SMEM)
    dma = pltpu.SemaphoreType.DMA
    return pl.pallas_call(
        functools.partial(kernel, n_seq, n_head, tile, wide, agenda(kv_heads)),
        out_shape=jax.ShapeDtypeStruct((share, model), bf16),
        in_specs=[smem, smem, smem] + [pl.BlockSpec(memory_space=pl.ANY)] * 4,
        out_specs=vmem,
        scratch_shapes=[
            pltpu.VMEM((rows * kv_heads, width), bf16),
            pltpu.VMEM((rows * kv_heads, width), bf16),
            pltpu.VMEM((rows * heads, width), bf16),
            pltpu.VMEM((rows * kv_heads, width), f32),
            pltpu.VMEM((rows * kv_heads, width), f32),
            pltpu.VMEM((rows * heads, width), f32),
            pltpu.VMEM((kv_heads, 2, rows, width), bf16),
            pltpu.VMEM((3 * PLANE, kv_heads, 2, rows, width), bf16),
            pltpu.VMEM((kv_heads, 2, SINK_ROWS, width), bf16),
            pltpu.VMEM((kv_heads, width, lanes), bf16),
            pltpu.VMEM((kv_heads, 1, lanes), i32),
            pltpu.VMEM((kv_heads, 1, lanes), i32),
            pltpu.VMEM((kv_heads, 1, lanes), f32),
            pltpu.VMEM((kv_heads, 1, lanes), f32),
            pltpu.VMEM((kv_heads, 1, lanes), f32),
            pltpu.VMEM((kv_heads, width, lanes), f32),
            pltpu.VMEM((rows, group * width), bf16),
            pltpu.VMEM((depth, model), bf16),
            pltpu.VMEM((rows, model), f32),
            pltpu.VMEM((tiles, n_head, share, tile), bf16),
            pltpu.VMEM((tiles, n_head - 1, share, tile), bf16),
            dma((8, kv_heads)),
            dma((3 * PLANE, kv_heads)),
            dma((3,)),
            dma,
            dma((3,)),
            dma((kv_heads,)),
            dma((tiles, n_head - 1)),
            dma((tiles, n_head - 1)),
        ],
        compiler_params=pltpu.CompilerParams(
            collective_id=0, has_side_effects=True, vmem_limit_bytes=56 * 1024 * 1024
        ),
    )(
        windows,
        sink_counts,
        sink_bias,
        key_rows.reshape(rows * kv_heads, width),
        value_rows.reshape(rows * kv_heads, width),
        queries.reshape(rows * heads, width),
        out_weight,
    )


def solution(mesh):
    in_specs = (
        P("seq", "head", None),
        P("seq", "head", None),
        P("seq", "head", None),
        P("head"),
        P("head"),
        P("head"),
        P("head", None),
    )
    body = functools.partial(shards, mesh.shape["seq"], mesh.shape["head"])
    out_specs = P(("seq", "head"), None)
    return jax.shard_map(body, mesh=mesh, in_specs=in_specs, out_specs=out_specs, check_vma=False)
```

```python
import functools
import heapq

import jax
import jax.numpy as jnp
from jax import lax
from jax.experimental import pallas as pl
from jax.experimental.pallas import tpu as pltpu
from jax.sharding import PartitionSpec as P

WINDOW = 1536
SINKS = 4
PLANE = 4
SINK_ROWS = 16
HIDDEN = -1e30
LOG2E = 1.4426950408889634
MESH = pl.DeviceIdType.MESH

KINDS = 8
PAIRS = KINDS // 2
PAIR = KINDS
SINK_EARLY, SINK_MID, SINK_LATE = PAIR + PAIRS, PAIR + PAIRS + 1, PAIR + PAIRS + 2
CHUNK_US, HOP_US = 2.1, 1.7
BITS, PER_WORD = 6, 5


def kinds_of(p):
    b0, b1 = p % 2, p // 2
    px, py, pd = p ^ 1, p ^ 2, 3 - p
    return [(1, p), (2, p), (1, px), (1, py), (1, pd), (2 - 2 * b0, px), (2 - 2 * b1, py), (2 - 2 * b1, pd)]


def forwards(z, p, plane, src):
    b0, b1 = p % 2, p // 2
    px, py = p ^ 1, p ^ 2
    out = []
    if (plane, src) == (0, p):
        out.append(("z", z + 1, p, 1))
        if b0 == 0:
            out.append(("x", z, px, 0))
        if b1 == 0:
            out.append(("y", z, py, 0))
    if (plane, src) == (1, p):
        out += [("z", z + 1, p, 2), ("x", z, px, 1), ("y", z, py, 1)]
    if (plane, src) == (2, p):
        if b0 == 1:
            out.append(("x", z, px, 2))
        if b1 == 1:
            out.append(("y", z, py, 2))
    if (plane, src) == (1, px):
        out.append(("y", z, py, 1))
    if (plane, src) == (2 - 2 * b1, py):
        out.append(("x", z, px, plane))
    return out


def arrivals(heads):
    queue, free, landed, tick = [], {}, {}, 0
    for c in range(heads):
        for z in range(3):
            for p in range(PLANE):
                heapq.heappush(queue, (1e-3 * c, tick, z, p, 0, p, c))
                tick += 1
    while queue:
        t, _, z, p, plane, src, c = heapq.heappop(queue)
        landed[z, p, plane, src, c] = t
        for link, z_to, p_to, plane_to in forwards(z, p, plane, src):
            if z_to < 3:
                start = max(t, free.get((z, p, link), 0.0))
                free[z, p, link] = start + CHUNK_US
                heapq.heappush(queue, (start + CHUNK_US + HOP_US, tick, z_to, p_to, plane_to, src, c))
                tick += 1
    return landed


def agenda(heads):
    landed = arrivals(heads)
    plans, orders = [], []
    for p in range(PLANE):
        kinds = kinds_of(p)
        when = [[landed[2, p, plane, src, c] for c in range(heads)] for plane, src in kinds]
        order = sorted(range(KINDS), key=lambda k: (sum(when[k]), k))
        due = [(when[k][c], k, c) for k in range(KINDS) for c in range(heads)]
        due += [(11.0, SINK_EARLY, 0), (19.3, SINK_MID, 0), (21.7, SINK_LATE, 0)]
        for j in range(PAIRS):
            for c in range(heads):
                if j < PAIRS - 1 or c < heads - 1:
                    ready = max(when[k][c] for k in order[2 * j:2 * j + 2])
                    due.append((max(ready, 21.7) if j == PAIRS - 1 else ready, PAIR + j, c))
        due.sort(key=lambda e: (e[0], PAIR <= e[1] < SINK_EARLY, e[1], e[2]))
        plans.append([k * heads + c for _, k, c in due])
        assert max(plans[-1]) < 1 << BITS
        orders.append(order)
    return plans, orders


def kernel(
    n_seq, n_head, tile, wide, plans, orders,
    win_ref, cnt_ref, bias_ref, k_hbm, v_hbm, q_hbm, w_hbm, out_ref,
    k_raw, v_raw, q_raw, k_wide, v_wide, q_wide,
    own, kv, sink, qt, low, few, lift, top, norm, acc, att, w, total, part, got,
    send_sem, recv_sem, sink_send, sink_recv, raw_sem, w_sem, part_send, part_recv,
):
    me, side = lax.axis_index("seq"), lax.axis_index("head")
    heads_kv, _, rows, width = own.shape
    lanes = qt.shape[2]
    group = lanes // rows
    heads = heads_kv * group
    model = w.shape[1]
    depth = group * width
    share = rows // n_head
    z, p = me // PLANE, lax.rem(me, PLANE)
    bit0, bit1 = lax.rem(p, 2), p // 2
    px, py = p + 1 - 2 * bit0, p + 2 - 4 * bit1
    pd = 3 - p
    base = z * PLANE
    n_z = n_seq // PLANE
    scale = LOG2E / width**0.5

    barrier = pltpu.get_barrier_semaphore()

    def greet(where):
        pl.semaphore_signal(barrier, inc=1, device_id=where, device_id_type=MESH)

    above, below = (z + 1 < n_z).astype(jnp.int32), (z > 0).astype(jnp.int32)
    loads = [
        pltpu.make_async_copy(source, target, raw_sem.at[i])
        for i, (source, target) in enumerate(((k_hbm, k_raw), (v_hbm, v_raw), (q_hbm, q_raw)))
    ]
    for load in loads:
        load.start()
    greet({"seq": base + px})
    greet({"seq": base + py})

    @pl.when(z + 1 < n_z)
    def _():
        greet({"seq": me + PLANE})

    @pl.when(z > 0)
    def _():
        greet({"seq": me - PLANE})

    for step in range(1, n_head):
        greet({"head": lax.rem(side + step, n_head)})

    def send(kind, src, plane, source, c, target):
        return pltpu.make_async_remote_copy(
            src_ref=src,
            dst_ref=kv.at[plane * PLANE + source, c],
            send_sem=send_sem.at[kind, c],
            recv_sem=recv_sem.at[plane * PLANE + source, c],
            device_id={"seq": target},
            device_id_type=MESH,
        )

    def landed(plane, source, c):
        send(0, own.at[c], plane, source, c, me).wait_recv()

    def held(plane, source, c):
        return kv.at[plane * PLANE + source, c]

    x_old, y_old = 2 * bit0, 2 * bit1
    x_from, y_from = 2 - 2 * bit0, 2 - 2 * bit1

    def sink_copy(way, source, target):
        return pltpu.make_async_remote_copy(
            src_ref=source,
            dst_ref=sink,
            send_sem=sink_send.at[way],
            recv_sem=sink_recv,
            device_id={"seq": target},
            device_id_type=MESH,
        )

    first_rows = own.at[:, :, pl.ds(0, SINK_ROWS)]

    for i, (raw, spread) in enumerate(((k_raw, k_wide), (v_raw, v_wide))):
        loads[i].wait()
        spread[...] = raw[...].astype(jnp.float32)
        for c in range(heads_kv):
            own[c, i] = spread[pl.ds(c, rows, stride=heads_kv), :].astype(jnp.bfloat16)
    pl.semaphore_wait(barrier, n_head + 1 + above + below)

    @pl.when(me == 0)
    def _():
        sink_copy(0, first_rows, base + px).start()
        sink_copy(1, first_rows, base + py).start()

        @pl.when(z + 1 < n_z)
        def _():
            sink_copy(2, first_rows, me + PLANE).start()
        sink[...] = own[:, :, :SINK_ROWS]

    for c in range(heads_kv):
        @pl.when(z + 1 < n_z)
        def _():
            send(0, own.at[c], 1, p, c, me + PLANE).start()

        @pl.when(x_old == 0)
        def _():
            send(2, own.at[c], 0, p, c, base + px).start()

        @pl.when(y_old == 0)
        def _():
            send(3, own.at[c], 0, p, c, base + py).start()

    def fetch(c):
        part_of = pl.ds(pl.multiple_of(c * depth, depth), depth)
        return pltpu.make_async_copy(w_hbm.at[part_of], w.at[part_of], w_sem.at[c])

    loads[2].wait()
    for c in range(heads_kv):
        fetch(c).start()
    q_wide[...] = q_raw[...].astype(jnp.float32)
    column = lax.broadcasted_iota(jnp.int32, (1, lanes), 1)
    for c in range(heads_kv):
        window, count, bias, token = (jnp.zeros((1, lanes), t) for t in (jnp.int32, jnp.int32, jnp.float32, jnp.int32))
        for g in range(group):
            mine = (column >= g * rows) & (column < (g + 1) * rows)
            h = c * group + g
            window = jnp.where(mine, win_ref[h], window)
            count = jnp.where(mine, cnt_ref[h], count)
            bias = jnp.where(mine, bias_ref[h], bias)
            token = jnp.where(mine, column - g * rows, token)
        token = token + me * rows
        low[c] = jnp.maximum(token - window, count - 1)
        few[c] = jnp.minimum(token, count - 1)
        lift[c] = bias * LOG2E
        picked = [q_wide[pl.ds(c * group + g, rows, stride=heads), :].astype(jnp.bfloat16) for g in range(group)]
        qt[c] = jnp.concatenate(picked, axis=0).T
        top[c] = jnp.full((1, lanes), HIDDEN, jnp.float32)
        norm[c] = jnp.zeros((1, lanes), jnp.float32)
        acc[c] = jnp.zeros((width, lanes), jnp.float32)

    step = min(256, lanes)
    parts = [slice(n, n + step) for n in range(0, lanes, step)]

    def attend(blocks, c, shards, causal=False, last=False):
        keys = [block[0] for block in blocks] + ([sink[c, 0]] if last else [])
        values = [block[1] for block in blocks] + ([sink[c, 1]] if last else [])
        turned = jnp.concatenate(values, axis=0).T
        key_row = lax.broadcasted_iota(jnp.int32, (rows, 1), 0)
        scores = [[jnp.dot(k, qt[c, :, cols], preferred_element_type=jnp.float32) for k in keys] for cols in parts]
        olds = [top[c, :, cols] for cols in parts]
        weights, news, fades, sums = [], [], [], []
        for pieces, old, cols in zip(scores, olds, parts):
            shown = []
            for s, shard in zip(pieces, shards):
                seen = key_row > low[c, :, cols] - shard * rows
                if causal:
                    column = lax.broadcasted_iota(jnp.int32, (1, step), 1) + cols.start
                    seen = seen & (key_row <= lax.rem(column, rows))
                shown.append(jnp.where(seen, s * scale, HIDDEN))
            if last:
                sink_row = lax.broadcasted_iota(jnp.int32, (SINK_ROWS, 1), 0)
                shown.append(jnp.where(sink_row <= few[c, :, cols], pieces[-1] * scale + lift[c, :, cols], HIDDEN))
            new = old
            for s in shown:
                new = jnp.maximum(new, jnp.max(s, axis=0, keepdims=True))
            e = [jnp.exp2(s - new) for s in shown]
            weights.append(jnp.concatenate([x.astype(jnp.bfloat16) for x in e], axis=0))
            news.append(new)
            fades.append(jnp.exp2(old - new))
            sums.append(functools.reduce(jnp.add, [jnp.sum(x, axis=0, keepdims=True) for x in e]))
        adds = [jnp.dot(turned, e, preferred_element_type=jnp.float32) for e in weights]
        mixed = []
        for new, fade, added, add, cols in zip(news, fades, sums, adds, parts):
            whole = acc[c, :, cols] * fade + add
            weight = norm[c, :, cols] * fade + added
            if last:
                mixed.append((whole * (1.0 / weight)).T.astype(jnp.bfloat16))
            else:
                top[c, :, cols] = new
                norm[c, :, cols] = weight
                acc[c, :, cols] = whole
        if last:
            mixed = jnp.concatenate(mixed, axis=0)
            for g in range(group):
                att[:, g * width:(g + 1) * width] = mixed[g * rows:(g + 1) * rows]

    def each(body):
        def one(c, carry):
            body(c)
            return carry
        lax.fori_loop(0, heads_kv, one, 0)

    each(lambda c: attend([own.at[c]], c, [me], causal=True))
    total[...] = jnp.zeros(total.shape, jnp.float32)

    @pl.when(z < 2)
    def _():
        def clear(i, carry):
            kv[i // heads_kv, lax.rem(i, heads_kv)] = jnp.zeros(own.shape[1:], jnp.bfloat16)
            return carry
        lax.fori_loop((z + 1) * PLANE * heads_kv, 3 * PLANE * heads_kv, clear, 0)

    def pass_on():
        sink_copy(0, sink, me).wait_recv()

        @pl.when(me == 1)
        def _():
            sink_copy(1, sink, base + py).start()

        @pl.when(z + 1 < n_z)
        def _():
            sink_copy(2, sink, me + PLANE).start()

    def rows_of(c):
        return pl.ds(pl.multiple_of(c * depth, depth), depth)

    def at_position(choices):
        chosen = jnp.int32(choices[0])
        for q in range(1, PLANE):
            chosen = jnp.where(p == q, jnp.int32(choices[q]), chosen)
        return chosen

    def packed(codes, bits):
        return sum(code << (bits * j) for j, code in enumerate(codes))

    n_words = (len(plans[0]) + PER_WORD - 1) // PER_WORD
    words = [
        at_position([packed(plan[i * PER_WORD:(i + 1) * PER_WORD], BITS) for plan in plans]) for i in range(n_words)
    ]
    landing = at_position([packed(order, 3) for order in orders])

    def pick(index, choices):
        chosen = choices[-1]
        for i in range(len(choices) - 2, -1, -1):
            chosen = jnp.where(index == i, choices[i], chosen)
        return chosen

    def where_is(kind):
        return pick(kind, [1, 2, 1, 1, 1, x_from, y_from, y_from]), pick(kind, [p, p, px, py, pd, px, py, pd])

    def pair(j, c, last=False):
        blocks, shards, nearest = [], [], 2
        for i in range(2):
            plane, source = where_is(lax.shift_right_logical(landing, 3 * (2 * j + i)) & 7)
            blocks.append(held(plane, source, c))
            shards.append(base - plane * PLANE + source)
            nearest = jnp.minimum(nearest, plane)
        if last:
            attend(blocks, c, shards, last=True)
            fetch(c).wait()
        else:
            @pl.when(z >= nearest)
            def _():
                attend(blocks, c, shards)

    def event(i, carry):
        word = pick(i // PER_WORD, words)
        code = lax.shift_right_logical(word, BITS * lax.rem(i, PER_WORD)) & ((1 << BITS) - 1)
        kind, c = code // heads_kv, lax.rem(code, heads_kv)
        plane, source = where_is(kind)

        @pl.when((kind < KINDS) & (z >= plane))
        def _():
            landed(plane, source, c)

            @pl.when(kind == 0)
            def _():
                @pl.when(z + 1 < n_z)
                def _():
                    send(1, held(1, p, c), 2, p, c, me + PLANE).start()
                send(4, held(1, p, c), 1, p, c, base + px).start()
                send(5, held(1, p, c), 1, p, c, base + py).start()

            @pl.when((kind == 1) & (x_old == 2))
            def _():
                send(2, held(2, p, c), 2, p, c, base + px).start()

            @pl.when((kind == 1) & (y_old == 2))
            def _():
                send(3, held(2, p, c), 2, p, c, base + py).start()

            @pl.when(kind == 2)
            def _():
                send(6, held(1, px, c), 1, px, c, base + py).start()

            @pl.when(kind == 6)
            def _():
                send(7, held(y_from, py, c), y_from, py, c, base + px).start()

        turn = jnp.where(z <= 1, SINK_EARLY, jnp.where(z == 2, SINK_MID, SINK_LATE))

        @pl.when((kind == turn) & (me > 0))
        def _():
            pass_on()

        @pl.when((kind >= PAIR) & (kind < PAIR + PAIRS - 1))
        def _():
            pair(kind - PAIR, c)

        @pl.when(kind == PAIR + PAIRS - 1)
        def _():
            pair(PAIRS - 1, c, last=True)

            def project(t, carry):
                cols = pl.ds(pl.multiple_of(t * wide, wide), wide)
                total[:, cols] += jnp.dot(att[...], w[rows_of(c), cols], preferred_element_type=jnp.float32)
                return carry
            lax.fori_loop(0, model // wide, project, 0)
        return carry
    lax.fori_loop(0, len(plans[0]), event, 0)

    pair(PAIRS - 1, heads_kv - 1, last=True)
    tiles = model // tile

    def give(t, step):
        target = lax.rem(side + step, n_head)
        return pltpu.make_async_remote_copy(
            src_ref=part.at[t, target],
            dst_ref=got.at[t, step - 1],
            send_sem=part_send.at[t, step - 1],
            recv_sem=part_recv.at[t, step - 1],
            device_id={"head": target},
            device_id_type=MESH,
        )

    def project(t, carry):
        cols = pl.ds(pl.multiple_of(t * tile, tile), tile)
        whole = total[:, cols] + jnp.dot(att[...], w[rows_of(heads_kv - 1), cols], preferred_element_type=jnp.float32)
        for d in range(n_head):
            part[t, d] = whole[d * share:(d + 1) * share].astype(jnp.bfloat16)

        @pl.when(t >= 1)
        def _():
            for step in range(1, n_head):
                give(t - 1, step).start()
        return carry
    lax.fori_loop(0, tiles, project, 0)
    for step in range(1, n_head):
        give(tiles - 1, step).start()

    def sent(kind, plane, source, c, target):
        send(kind, held(plane, source, c), plane, source, c, target).wait_send()

    def drain(c):
        @pl.when(z + 1 < n_z)
        def _():
            sent(0, 1, p, c, me + PLANE)

        @pl.when(z >= x_old)
        def _():
            sent(2, x_old, p, c, base + px)

        @pl.when(z >= y_old)
        def _():
            sent(3, y_old, p, c, base + py)

        @pl.when(z >= 1)
        def _():
            @pl.when(z + 1 < n_z)
            def _():
                sent(1, 2, p, c, me + PLANE)
            sent(4, 1, p, c, base + px)
            sent(5, 1, p, c, base + py)
            sent(6, 1, px, c, base + py)

        @pl.when(z >= y_from)
        def _():
            sent(7, y_from, py, c, base + px)
    each(drain)

    @pl.when(me == 0)
    def _():
        sink_copy(0, sink, base + px).wait_send()

    @pl.when(me <= 1)
    def _():
        sink_copy(1, sink, base + py).wait_send()

    @pl.when(z + 1 < n_z)
    def _():
        sink_copy(2, sink, me + PLANE).wait_send()

    def finish(t, carry):
        whole = part[t, side].astype(jnp.float32)
        for step in range(1, n_head):
            give(t, step).wait_recv()
            whole = whole + got[t, step - 1].astype(jnp.float32)
        out_ref[:, pl.ds(pl.multiple_of(t * tile, tile), tile)] = whole.astype(jnp.bfloat16)
        return carry
    lax.fori_loop(0, tiles, finish, 0)

    def gone(t, carry):
        for step in range(1, n_head):
            give(t, step).wait_send()
        return carry
    lax.fori_loop(0, tiles, gone, 0)


def shards(n_seq, n_head, queries, key_rows, value_rows, windows, sink_counts, sink_bias, out_weight):
    rows, heads, width = queries.shape
    kv_heads = key_rows.shape[1]
    group = heads // kv_heads
    lanes = group * rows
    depth, model = out_weight.shape
    assert (WINDOW - 1) // rows + 1 == 2 * PLANE and n_seq % PLANE == 0
    tile, wide = min(1024, model), min(2048, model)
    tiles = model // tile
    share = rows // n_head
    bf16, f32, i32 = jnp.bfloat16, jnp.float32, jnp.int32
    vmem = pl.BlockSpec(memory_space=pltpu.VMEM)
    smem = pl.BlockSpec(memory_space=pltpu.SMEM)
    dma = pltpu.SemaphoreType.DMA
    return pl.pallas_call(
        functools.partial(kernel, n_seq, n_head, tile, wide, *agenda(kv_heads)),
        out_shape=pltpu.VMEM((share, model), bf16),
        in_specs=[smem, smem, smem] + [pl.BlockSpec(memory_space=pl.ANY)] * 4,
        out_specs=vmem,
        scratch_shapes=[
            pltpu.VMEM((rows * kv_heads, width), bf16),
            pltpu.VMEM((rows * kv_heads, width), bf16),
            pltpu.VMEM((rows * heads, width), bf16),
            pltpu.VMEM((rows * kv_heads, width), f32),
            pltpu.VMEM((rows * kv_heads, width), f32),
            pltpu.VMEM((rows * heads, width), f32),
            pltpu.VMEM((kv_heads, 2, rows, width), bf16),
            pltpu.VMEM((3 * PLANE, kv_heads, 2, rows, width), bf16),
            pltpu.VMEM((kv_heads, 2, SINK_ROWS, width), bf16),
            pltpu.VMEM((kv_heads, width, lanes), bf16),
            pltpu.VMEM((kv_heads, 1, lanes), i32),
            pltpu.VMEM((kv_heads, 1, lanes), i32),
            pltpu.VMEM((kv_heads, 1, lanes), f32),
            pltpu.VMEM((kv_heads, 1, lanes), f32),
            pltpu.VMEM((kv_heads, 1, lanes), f32),
            pltpu.VMEM((kv_heads, width, lanes), f32),
            pltpu.VMEM((rows, group * width), bf16),
            pltpu.VMEM((depth, model), bf16),
            pltpu.VMEM((rows, model), f32),
            pltpu.VMEM((tiles, n_head, share, tile), bf16),
            pltpu.VMEM((tiles, n_head - 1, share, tile), bf16),
            dma((8, kv_heads)),
            dma((3 * PLANE, kv_heads)),
            dma((3,)),
            dma,
            dma((3,)),
            dma((kv_heads,)),
            dma((tiles, n_head - 1)),
            dma((tiles, n_head - 1)),
        ],
        compiler_params=pltpu.CompilerParams(
            collective_id=0, has_side_effects=True, vmem_limit_bytes=56 * 1024 * 1024
        ),
    )(
        windows,
        sink_counts,
        sink_bias,
        key_rows.reshape(rows * kv_heads, width),
        value_rows.reshape(rows * kv_heads, width),
        queries.reshape(rows * heads, width),
        out_weight,
    )


def solution(mesh):
    in_specs = (
        P("seq", "head", None),
        P("seq", "head", None),
        P("seq", "head", None),
        P("head"),
        P("head"),
        P("head"),
        P("head", None),
    )
    body = functools.partial(shards, mesh.shape["seq"], mesh.shape["head"])
    out_specs = P(("seq", "head"), None)
    return jax.shard_map(body, mesh=mesh, in_specs=in_specs, out_specs=out_specs, check_vma=False)
```

```python
import functools
import heapq

import jax
import jax.numpy as jnp
from jax import lax
from jax.experimental import pallas as pl
from jax.experimental.pallas import tpu as pltpu
from jax.sharding import PartitionSpec as P

WINDOW = 1536
SINKS = 4
PLANE = 4
SINK_ROWS = 16
HIDDEN = -1e30
LOG2E = 1.4426950408889634
MESH = pl.DeviceIdType.MESH

KINDS = 8
PAIRS = KINDS // 2
PAIR, LAST, SINK, NOTHING = KINDS, KINDS + PAIRS, KINDS + 2 * PAIRS, KINDS + 2 * PAIRS + 3
BITS, PER_WORD = 10, 3
AHEAD = 2
CHUNK_US, HOP_US = 2.13, 2.0
BY_Z, BY_X, BY_Y = 1, 2, 4
ORDERS = {
    4: (
        ((1, 2), (2,), (1, 3)),
        [
            [0, 8, 1, 4, 2, 16, 5, 24, 9, 17, 6, 20, 13, 14, 3, 10, 21, 25, 12, 15, 28, 27, 11, 29, 26, 7, 18, 22, 30, 19, 23, 31],
            [0, 20, 1, 4, 12, 13, 2, 22, 24, 8, 23, 21, 14, 6, 3, 9, 25, 16, 10, 17, 7, 26, 15, 5, 28, 29, 27, 11, 18, 19, 31, 30],
            [0, 1, 4, 8, 24, 26, 2, 5, 12, 25, 28, 29, 27, 3, 13, 9, 7, 6, 16, 30, 14, 20, 31, 21, 10, 11, 15, 18, 17, 22, 19, 23],
            [0, 24, 1, 21, 22, 25, 4, 26, 2, 23, 20, 27, 5, 8, 3, 30, 12, 13, 28, 14, 7, 6, 15, 16, 10, 29, 18, 11, 31, 9, 17, 19],
        ],
        [[0, 3, 1, 2, 5, 7, 6, 4], [0, 5, 6, 3, 2, 1, 7, 4], [0, 6, 2, 1, 3, 7, 5, 4], [3, 7, 0, 5, 1, 6, 2, 4]],
        ((1, 5, 16), (3, 12, 17), (2, 13, 16), (8, 15, 23)),
    ),
}


def kinds_of(p):
    b0, b1 = p % 2, p // 2
    px, py, pd = p ^ 1, p ^ 2, 3 - p
    return [(1, p), (2, p), (1, px), (1, py), (1, pd), (2 - 2 * b0, px), (2 - 2 * b1, py), (2 - 2 * b1, pd)]


def forwards(p, plane, src, c, routes):
    over_z_x, over_z_y, corner_by_x = routes
    b0, b1 = p % 2, p // 2
    px, py = p ^ 1, p ^ 2
    links = 0
    if (plane, src) == (0, p):
        links |= BY_Z | (BY_X if b0 == 0 else 0) | (BY_Y if b1 == 0 else 0)
    if (plane, src) == (1, p):
        links |= BY_Z | BY_X | BY_Y
    if (plane, src) == (2, p):
        links |= (BY_X if b0 == 1 and c not in over_z_x else 0) | (BY_Y if b1 == 1 and c not in over_z_y else 0)
    if (plane, src) == (1, px):
        links |= (0 if c in corner_by_x else BY_Y) | (BY_Z if b0 == 0 and c in over_z_x else 0)
    if (plane, src) == (1, py):
        links |= (BY_X if c in corner_by_x else 0) | (BY_Z if b1 == 0 and c in over_z_y else 0)
    if (plane, src) == (2 - 2 * b1, py):
        links |= BY_X
    return links


def arrivals(heads, routes):
    queue, free, landed, tick = [], {}, {}, 0
    for c in range(heads):
        for z in range(3):
            for p in range(PLANE):
                heapq.heappush(queue, (1e-3 * c, tick, z, p, 0, p, c))
                tick += 1
    while queue:
        t, _, z, p, plane, src, c = heapq.heappop(queue)
        landed[z, p, plane, src, c] = t
        links = forwards(p, plane, src, c, routes)
        for link, z_to, p_to, plane_to in ((BY_Z, z + 1, p, plane + 1), (BY_X, z, p ^ 1, plane), (BY_Y, z, p ^ 2, plane)):
            if links & link and z_to < 3:
                start = max(t, free.get((z, p, link), 0.0))
                free[z, p, link] = start + CHUNK_US
                heapq.heappush(queue, (start + CHUNK_US + HOP_US, tick, z_to, p_to, plane_to, src, c))
                tick += 1
    return landed


def agenda(heads):
    if heads in ORDERS:
        routes, takes, orders, sinks = ORDERS[heads]
    else:
        routes, takes, orders, sinks = ((), (), ()), [], [], ((0, 0, 0),) * PLANE
        landed = arrivals(heads, routes)
        for p in range(PLANE):
            kinds = kinds_of(p)
            when = {k * heads + c: landed[2, p, *kinds[k], c] for k in range(KINDS) for c in range(heads)}
            takes.append(sorted(when, key=lambda i: (when[i], i)))
            orders.append(sorted(range(KINDS), key=lambda k: (sum(when[k * heads + c] for c in range(heads)), k)))
    plans, finals = [], []
    for p in range(PLANE):
        plan, seen = [], set()
        for i, take in enumerate(takes[p]):
            for turn in range(3):
                if sinks[p][turn] == i:
                    plan.append((SINK + turn, 0, 0))
            k, c = divmod(take, heads)
            plan.append((k, c, forwards(p, *kinds_of(p)[k], c, routes)))
            seen.add(take)
            for j in range(PAIRS):
                both = orders[p][2 * j:2 * j + 2]
                if k in both and all(i * heads + c in seen for i in both):
                    plan.append((PAIR + j, c, 0))
        for c in range(heads):
            i = max(i for i, e in enumerate(plan) if PAIR <= e[0] < LAST and e[1] == c)
            plan[i] = (plan[i][0] - PAIR + LAST, c, 0)
        final = max(i for i, e in enumerate(plan) if LAST <= e[0] < SINK)
        finals.append((plan[final][0] - LAST, plan.pop(final)[1]))
        assert len(seen) == KINDS * heads
        plan += [(NOTHING, 0, 0)] * (-len(plan) % PER_WORD)
        plans.append(plan)
    return plans, orders, finals


def kernel(
    n_seq, n_head, tile, wide, plans, orders, finals,
    win_ref, cnt_ref, bias_ref, k_hbm, v_hbm, q_hbm, w_hbm, out_ref,
    k_raw, v_raw, q_raw, k_wide, v_wide, q_wide,
    own, kv, sink, qt, low, few, lift, top, norm, acc, att, w, total, part, got,
    send_sem, recv_sem, sink_send, sink_recv, raw_sem, w_sem, part_send, part_recv,
):
    me, side = lax.axis_index("seq"), lax.axis_index("head")
    heads_kv, _, rows, width = own.shape
    lanes = qt.shape[2]
    group = lanes // rows
    heads = heads_kv * group
    model = w.shape[1]
    depth = group * width
    share = rows // n_head
    z, p = me // PLANE, lax.rem(me, PLANE)
    bit0, bit1 = lax.rem(p, 2), p // 2
    px, py = p + 1 - 2 * bit0, p + 2 - 4 * bit1
    pd = 3 - p
    base = z * PLANE
    n_z = n_seq // PLANE
    scale = LOG2E / width**0.5

    barrier = pltpu.get_barrier_semaphore()

    def greet(where):
        pl.semaphore_signal(barrier, inc=1, device_id=where, device_id_type=MESH)

    above, below = (z + 1 < n_z).astype(jnp.int32), (z > 0).astype(jnp.int32)
    loads = [
        pltpu.make_async_copy(source, target, raw_sem.at[i])
        for i, (source, target) in enumerate(((k_hbm, k_raw), (v_hbm, v_raw), (q_hbm, q_raw)))
    ]
    for load in loads:
        load.start()
    greet({"seq": base + px})
    greet({"seq": base + py})

    @pl.when(z + 1 < n_z)
    def _():
        greet({"seq": me + PLANE})

    @pl.when(z > 0)
    def _():
        greet({"seq": me - PLANE})

    for step in range(1, n_head):
        greet({"head": lax.rem(side + step, n_head)})

    def send(link, kind, c, slot, src):
        way = {BY_Z: 0, BY_X: 1, BY_Y: 2}[link]
        slot_to = slot + PLANE if link == BY_Z else slot
        return pltpu.make_async_remote_copy(
            src_ref=src,
            dst_ref=kv.at[slot_to, c],
            send_sem=send_sem.at[way, kind, c],
            recv_sem=recv_sem.at[slot_to, c],
            device_id={"seq": [me + PLANE, base + px, base + py][way]},
            device_id_type=MESH,
        )

    def own_up(c, act):
        @pl.when(z + 1 < n_z)
        def _():
            act(send(BY_Z, KINDS, c, p, own.at[c]))

    def own_aside(c, act):
        @pl.when(bit0 == 0)
        def _():
            act(send(BY_X, KINDS, c, p, own.at[c]))

        @pl.when(bit1 == 0)
        def _():
            act(send(BY_Y, KINDS, c, p, own.at[c]))

    def begin(copy):
        copy.start()

    def sent(copy):
        copy.wait_send()

    def send(link, kind, c, slot, src):
        way = {BY_Z: 0, BY_X: 1, BY_Y: 2}[link]
        slot_to = slot + PLANE if link == BY_Z else slot
        return pltpu.make_async_remote_copy(
            src_ref=src,
            dst_ref=kv.at[slot_to, c],
            send_sem=send_sem.at[way, kind, c],
            recv_sem=recv_sem.at[slot_to, c],
            device_id={"seq": [me + PLANE, base + px, base + py][way]},
            device_id_type=MESH,
        )

    def own_up(c, act):
        @pl.when(z + 1 < n_z)
        def _():
            act(send(BY_Z, KINDS, c, p, own.at[c]))

    def own_aside(c, act):
        @pl.when(bit0 == 0)
        def _():
            act(send(BY_X, KINDS, c, p, own.at[c]))

        @pl.when(bit1 == 0)
        def _():
            act(send(BY_Y, KINDS, c, p, own.at[c]))

    def begin(copy):
        copy.start()

    def sent(copy):
        copy.wait_send()

    def held(plane, source, c):
        return kv.at[plane * PLANE + source, c]

    def sink_copy(way, source, target):
        return pltpu.make_async_remote_copy(
            src_ref=source,
            dst_ref=sink,
            send_sem=sink_send.at[way],
            recv_sem=sink_recv,
            device_id={"seq": target},
            device_id_type=MESH,
        )

    first_rows = own.at[:, :, pl.ds(0, SINK_ROWS)]

    for i, (raw, spread) in enumerate(((k_raw, k_wide), (v_raw, v_wide))):
        loads[i].wait()
        spread[...] = raw[...].astype(jnp.float32)
        for c in range(heads_kv):
            own[c, i] = spread[pl.ds(c, rows, stride=heads_kv), :].astype(jnp.bfloat16)
    pl.semaphore_wait(barrier, n_head + 1 + above + below)

    def sinks_on(source, act):
        @pl.when(me == 0)
        def _():
            act(sink_copy(0, source, base + px))

        @pl.when(me <= 1)
        def _():
            act(sink_copy(1, source, base + py))

        @pl.when(z + 1 < n_z)
        def _():
            act(sink_copy(2, source, me + PLANE))

    @pl.when(me == 0)
    def _():
        sinks_on(first_rows, begin)
        sink[...] = own[:, :, :SINK_ROWS]

    for c in range(heads_kv):
        if c < AHEAD:
            own_up(c, begin)
        own_aside(c, begin)

    def fetch(c):
        part_of = pl.ds(pl.multiple_of(c * depth, depth), depth)
        return pltpu.make_async_copy(w_hbm.at[part_of], w.at[part_of], w_sem.at[c])

    loads[2].wait()
    for c in range(heads_kv):
        fetch(c).start()
    q_wide[...] = q_raw[...].astype(jnp.float32)
    column = lax.broadcasted_iota(jnp.int32, (1, lanes), 1)
    for c in range(heads_kv):
        window, count, bias, token = (jnp.zeros((1, lanes), t) for t in (jnp.int32, jnp.int32, jnp.float32, jnp.int32))
        for g in range(group):
            mine = (column >= g * rows) & (column < (g + 1) * rows)
            h = c * group + g
            window = jnp.where(mine, win_ref[h], window)
            count = jnp.where(mine, cnt_ref[h], count)
            bias = jnp.where(mine, bias_ref[h], bias)
            token = jnp.where(mine, column - g * rows, token)
        token = token + me * rows
        low[c] = jnp.maximum(token - window, count - 1)
        few[c] = jnp.minimum(token, count - 1)
        lift[c] = bias * LOG2E
        picked = [q_wide[pl.ds(c * group + g, rows, stride=heads), :].astype(jnp.bfloat16) for g in range(group)]
        qt[c] = jnp.concatenate(picked, axis=0).T
        top[c] = jnp.full((1, lanes), HIDDEN, jnp.float32)
        norm[c] = jnp.zeros((1, lanes), jnp.float32)
        acc[c] = jnp.zeros((width, lanes), jnp.float32)

    step = min(256, lanes)
    parts = [slice(n, n + step) for n in range(0, lanes, step)]

    def attend(blocks, c, shards, causal=False, last=False):
        keys = [block[0] for block in blocks] + ([sink[c, 0]] if last else [])
        values = [block[1] for block in blocks] + ([sink[c, 1]] if last else [])
        turned = jnp.concatenate(values, axis=0).T
        turned = jnp.concatenate([turned, jnp.ones((SINK_ROWS, turned.shape[1]), jnp.bfloat16)], axis=0)
        key_row = lax.broadcasted_iota(jnp.int32, (rows, 1), 0)
        scores = [[jnp.dot(k, qt[c, :, cols], preferred_element_type=jnp.float32) for k in keys] for cols in parts]
        olds = [top[c, :, cols] for cols in parts]
        weights, news, fades = [], [], []
        for pieces, old, cols in zip(scores, olds, parts):
            shown = []
            for s, shard in zip(pieces, shards):
                seen = key_row > low[c, :, cols] - shard * rows
                if causal:
                    column = lax.broadcasted_iota(jnp.int32, (1, step), 1) + cols.start
                    seen = seen & (key_row <= lax.rem(column, rows))
                shown.append(jnp.where(seen, s * scale, HIDDEN))
            if last:
                sink_row = lax.broadcasted_iota(jnp.int32, (SINK_ROWS, 1), 0)
                shown.append(jnp.where(sink_row <= few[c, :, cols], pieces[-1] * scale + lift[c, :, cols], HIDDEN))
            new = old
            for s in shown:
                new = jnp.maximum(new, jnp.max(s, axis=0, keepdims=True))
            e = [jnp.exp2(s - new) for s in shown]
            weights.append(jnp.concatenate([x.astype(jnp.bfloat16) for x in e], axis=0))
            news.append(new)
            fades.append(jnp.exp2(old - new))
        adds = [jnp.dot(turned, e, preferred_element_type=jnp.float32) for e in weights]
        mixed = []
        for new, fade, add, cols in zip(news, fades, adds, parts):
            whole = acc[c, :, cols] * fade + add[:width]
            weight = norm[c, :, cols] * fade + add[width:width + 1]
            if last:
                mixed.append((whole * (1.0 / weight)).T.astype(jnp.bfloat16))
            else:
                top[c, :, cols] = new
                norm[c, :, cols] = weight
                acc[c, :, cols] = whole
        if last:
            mixed = jnp.concatenate(mixed, axis=0)
            for g in range(group):
                att[:, g * width:(g + 1) * width] = mixed[g * rows:(g + 1) * rows]

    def each(body):
        def one(c, carry):
            body(c)
            return carry
        lax.fori_loop(0, heads_kv, one, 0)

    each(lambda c: attend([own.at[c]], c, [me], causal=True))
    total[...] = jnp.zeros(total.shape, jnp.float32)

    @pl.when(z < 2)
    def _():
        def clear(i, carry):
            kv[i // heads_kv, lax.rem(i, heads_kv)] = jnp.zeros(own.shape[1:], jnp.bfloat16)
            return carry
        lax.fori_loop((z + 1) * PLANE * heads_kv, 3 * PLANE * heads_kv, clear, 0)

    @pl.when((z == 0) & (me > 0))
    def _():
        sink_copy(0, sink, me).wait_recv()
        sinks_on(sink, begin)

    @pl.when(z == 0)
    def _():
        for c in range(AHEAD, heads_kv):
            own_up(c, begin)

    def rows_of(c):
        return pl.ds(pl.multiple_of(c * depth, depth), depth)

    def at_position(choices):
        chosen = choices[0]
        for q in range(1, PLANE):
            chosen = jnp.where(p == q, choices[q], chosen)
        return chosen

    def packed(codes, bits):
        word = sum(code << (bits * j) for j, code in enumerate(codes))
        return jnp.int32(word - (1 << 32) if word >> 31 else word)

    def shifted(word, bits):
        return lax.shift_right_logical(word, bits)

    head_bits = (heads_kv - 1).bit_length()
    coded = [[((kind << head_bits | c) << 3) | links for kind, c, links in plan] for plan in plans]
    words = [
        at_position([packed(codes[i:i + PER_WORD], BITS) for codes in coded])
        for i in range(0, len(plans[0]), PER_WORD)
    ]
    slots_of = [[plane * PLANE + src for plane, src in kinds_of(q)] for q in range(PLANE)]
    kind_slots = at_position([packed(slots, 4) for slots in slots_of])
    pair_slots = at_position([packed([slots[k] for k in order], 4) for slots, order in zip(slots_of, orders)])

    def pair(j, c, last=False):
        both = shifted(pair_slots, 8 * j)
        slots = [both & 15, shifted(both, 4) & 15]
        blocks = [kv.at[slot, c] for slot in slots]
        shards = [base + (slot & 3) - (slot & 12) for slot in slots]
        if last:
            attend(blocks, c, shards, last=True)
            fetch(c).wait()
        else:
            @pl.when(z >= shifted(jnp.minimum(*slots), 2))
            def _():
                attend(blocks, c, shards)

    def event(code):
        links, c, kind = code & 7, shifted(code, 3) & ((1 << head_bits) - 1), shifted(code, 3 + head_bits)

        @pl.when(kind < KINDS)
        def _():
            slot = shifted(kind_slots, 4 * kind) & 15

            @pl.when(z >= shifted(slot, 2))
            def _():
                block = kv.at[slot, c]
                send(BY_X, kind, c, slot, block).wait_recv()

                @pl.when(links != 0)
                def _():
                    @pl.when(((links & BY_Z) != 0) & (z + 1 < n_z))
                    def _():
                        send(BY_Z, kind, c, slot, block).start()

                    @pl.when((links & BY_X) != 0)
                    def _():
                        send(BY_X, kind, c, slot, block).start()

                    @pl.when((links & BY_Y) != 0)
                    def _():
                        send(BY_Y, kind, c, slot, block).start()

                    @pl.when((kind == 0) & (c + AHEAD < heads_kv))
                    def _():
                        own_up(c + AHEAD, begin)

        @pl.when(kind >= KINDS)
        def _():
            @pl.when(kind < LAST)
            def _():
                pair(kind - PAIR, c)

            @pl.when((kind >= LAST) & (kind < SINK))
            def _():
                pair(kind - LAST, c, last=True)

                def project(t, carry):
                    cols = pl.ds(pl.multiple_of(t * wide, wide), wide)
                    total[:, cols] += jnp.dot(att[...], w[rows_of(c), cols], preferred_element_type=jnp.float32)
                    return carry
                lax.fori_loop(0, model // wide, project, 0)

            @pl.when((kind == SINK + jnp.minimum(z, 3) - 1) & (z > 0))
            def _():
                sink_copy(0, sink, me).wait_recv()
                sinks_on(sink, begin)

    def pick(index, choices):
        chosen = choices[-1]
        for i in range(len(choices) - 2, -1, -1):
            chosen = jnp.where(index == i, choices[i], chosen)
        return chosen

    def few_events(i, carry):
        def one(_, word):
            event(word & ((1 << BITS) - 1))
            return shifted(word, BITS)
        lax.fori_loop(0, PER_WORD, one, pick(i, words))
        return carry
    lax.fori_loop(0, len(words), few_events, 0)

    final = at_position([c for _, c in finals])
    pair(at_position([j for j, _ in finals]), final, last=True)
    tiles = model // tile

    def give(t, step):
        target = lax.rem(side + step, n_head)
        return pltpu.make_async_remote_copy(
            src_ref=part.at[t, target],
            dst_ref=got.at[t, step - 1],
            send_sem=part_send.at[t, step - 1],
            recv_sem=part_recv.at[t, step - 1],
            device_id={"head": target},
            device_id_type=MESH,
        )

    def project(t, carry):
        cols = pl.ds(pl.multiple_of(t * tile, tile), tile)
        whole = total[:, cols] + jnp.dot(att[...], w[rows_of(final), cols], preferred_element_type=jnp.float32)
        for d in range(n_head):
            part[t, d] = whole[d * share:(d + 1) * share].astype(jnp.bfloat16)

        @pl.when(t >= 1)
        def _():
            for step in range(1, n_head):
                give(t - 1, step).start()
        return carry
    lax.fori_loop(0, tiles, project, 0)
    for step in range(1, n_head):
        give(tiles - 1, step).start()

    def drain(q):
        for plane in range(3):
            kinds = [(k, c, links) for k, c, links in plans[q] if k < KINDS and kinds_of(q)[k][0] == plane]

            @pl.when(z >= plane)
            def _():
                for k, c, links in kinds:
                    for link in (BY_X, BY_Y):
                        if links & link:
                            send(link, k, c, 0, own.at[0]).wait_send()

            @pl.when((z >= plane) & (z + 1 < n_z))
            def _():
                for k, c, links in kinds:
                    if links & BY_Z:
                        send(BY_Z, k, c, 0, own.at[0]).wait_send()

    for q in range(PLANE):
        @pl.when(p == q)
        def _():
            drain(q)
    for c in range(heads_kv):
        own_up(c, sent)
        own_aside(c, sent)

    @pl.when((z > 0) | (me <= 1) | (n_z > 1))
    def _():
        sinks_on(sink, sent)

    def finish(t, carry):
        whole = part[t, side].astype(jnp.float32)
        for step in range(1, n_head):
            give(t, step).wait_recv()
            whole = whole + got[t, step - 1].astype(jnp.float32)
        out_ref[:, pl.ds(pl.multiple_of(t * tile, tile), tile)] = whole.astype(jnp.bfloat16)
        return carry
    lax.fori_loop(0, tiles, finish, 0)

    def gone(t, carry):
        for step in range(1, n_head):
            give(t, step).wait_send()
        return carry
    lax.fori_loop(0, tiles, gone, 0)


def shards(n_seq, n_head, queries, key_rows, value_rows, windows, sink_counts, sink_bias, out_weight):
    rows, heads, width = queries.shape
    kv_heads = key_rows.shape[1]
    group = heads // kv_heads
    lanes = group * rows
    depth, model = out_weight.shape
    assert (WINDOW - 1) // rows + 1 == 2 * PLANE and n_seq % PLANE == 0
    tile, wide = min(1024, model), min(2048, model)
    tiles = model // tile
    share = rows // n_head
    bf16, f32, i32 = jnp.bfloat16, jnp.float32, jnp.int32
    vmem = pl.BlockSpec(memory_space=pltpu.VMEM)
    smem = pl.BlockSpec(memory_space=pltpu.SMEM)
    dma = pltpu.SemaphoreType.DMA
    return pl.pallas_call(
        functools.partial(kernel, n_seq, n_head, tile, wide, *agenda(kv_heads)),
        out_shape=pltpu.VMEM((share, model), bf16),
        in_specs=[smem, smem, smem] + [pl.BlockSpec(memory_space=pl.ANY)] * 4,
        out_specs=vmem,
        scratch_shapes=[
            pltpu.VMEM((rows * kv_heads, width), bf16),
            pltpu.VMEM((rows * kv_heads, width), bf16),
            pltpu.VMEM((rows * heads, width), bf16),
            pltpu.VMEM((rows * kv_heads, width), f32),
            pltpu.VMEM((rows * kv_heads, width), f32),
            pltpu.VMEM((rows * heads, width), f32),
            pltpu.VMEM((kv_heads, 2, rows, width), bf16),
            pltpu.VMEM((3 * PLANE, kv_heads, 2, rows, width), bf16),
            pltpu.VMEM((kv_heads, 2, SINK_ROWS, width), bf16),
            pltpu.VMEM((kv_heads, width, lanes), bf16),
            pltpu.VMEM((kv_heads, 1, lanes), i32),
            pltpu.VMEM((kv_heads, 1, lanes), i32),
            pltpu.VMEM((kv_heads, 1, lanes), f32),
            pltpu.VMEM((kv_heads, 1, lanes), f32),
            pltpu.VMEM((kv_heads, 1, lanes), f32),
            pltpu.VMEM((kv_heads, width, lanes), f32),
            pltpu.VMEM((rows, group * width), bf16),
            pltpu.VMEM((depth, model), bf16),
            pltpu.VMEM((rows, model), f32),
            pltpu.VMEM((tiles, n_head, share, tile), bf16),
            pltpu.VMEM((tiles, n_head - 1, share, tile), bf16),
            dma((3, KINDS + 1, kv_heads)),
            dma((3 * PLANE, kv_heads)),
            dma((3,)),
            dma,
            dma((3,)),
            dma((kv_heads,)),
            dma((tiles, n_head - 1)),
            dma((tiles, n_head - 1)),
        ],
        compiler_params=pltpu.CompilerParams(
            collective_id=0, has_side_effects=True, vmem_limit_bytes=56 * 1024 * 1024
        ),
    )(
        windows,
        sink_counts,
        sink_bias,
        key_rows.reshape(rows * kv_heads, width),
        value_rows.reshape(rows * kv_heads, width),
        queries.reshape(rows * heads, width),
        out_weight,
    )


def solution(mesh):
    in_specs = (
        P("seq", "head", None),
        P("seq", "head", None),
        P("seq", "head", None),
        P("head"),
        P("head"),
        P("head"),
        P("head", None),
    )
    body = functools.partial(shards, mesh.shape["seq"], mesh.shape["head"])
    out_specs = P(("seq", "head"), None)
    return jax.shard_map(body, mesh=mesh, in_specs=in_specs, out_specs=out_specs, check_vma=False)
```

```python
import functools
import heapq

import jax
import jax.numpy as jnp
from jax import lax
from jax.experimental import pallas as pl
from jax.experimental.pallas import tpu as pltpu
from jax.sharding import PartitionSpec as P

WINDOW = 1536
SINKS = 4
PLANE = 4
SINK_ROWS = 16
HIDDEN = -1e30
LOG2E = 1.4426950408889634
MESH = pl.DeviceIdType.MESH

KINDS = 8
PAIRS = KINDS // 2
PAIR, LAST, SINK, NOTHING = KINDS, KINDS + PAIRS, KINDS + 2 * PAIRS, KINDS + 2 * PAIRS + 3
BITS, PER_WORD = 10, 3
AHEAD = 2
SEND_USES = (1, 0, 2, 3, 0, 0, 2, 0, 0)
CHUNK_US, HOP_US = 2.13, 2.0
BY_Z, BY_X, BY_Y = 1, 2, 4
ORDERS = {
    4: (
        ((1, 2), (2,), (1, 3)),
        [
            [0, 8, 1, 4, 2, 16, 5, 24, 9, 17, 6, 20, 13, 14, 3, 10, 21, 25, 12, 15, 28, 27, 11, 29, 26, 7, 18, 22, 30, 19, 23, 31],
            [0, 20, 1, 4, 12, 13, 2, 22, 24, 8, 23, 21, 14, 6, 3, 9, 25, 16, 10, 17, 7, 26, 15, 5, 28, 29, 27, 11, 18, 19, 31, 30],
            [0, 1, 4, 8, 24, 26, 2, 5, 12, 25, 28, 29, 27, 3, 13, 9, 7, 6, 16, 30, 14, 20, 31, 21, 10, 11, 15, 18, 17, 22, 19, 23],
            [0, 24, 1, 21, 22, 25, 4, 26, 2, 23, 20, 27, 5, 8, 3, 30, 12, 13, 28, 14, 7, 6, 15, 16, 10, 29, 18, 11, 31, 9, 17, 19],
        ],
        [[0, 3, 1, 2, 5, 7, 6, 4], [0, 5, 6, 3, 2, 1, 7, 4], [0, 6, 2, 1, 3, 7, 5, 4], [3, 7, 0, 5, 1, 6, 2, 4]],
        ((1, 5, 16), (3, 12, 17), (2, 13, 16), (8, 15, 23)),
    ),
}


def kinds_of(p):
    b0, b1 = p % 2, p // 2
    px, py, pd = p ^ 1, p ^ 2, 3 - p
    return [(1, p), (2, p), (1, px), (1, py), (1, pd), (2 - 2 * b0, px), (2 - 2 * b1, py), (2 - 2 * b1, pd)]


def forwards(p, plane, src, c, routes):
    over_z_x, over_z_y, corner_by_x = routes
    b0, b1 = p % 2, p // 2
    px, py = p ^ 1, p ^ 2
    links = 0
    if (plane, src) == (0, p):
        links |= BY_Z | (BY_X if b0 == 0 else 0) | (BY_Y if b1 == 0 else 0)
    if (plane, src) == (1, p):
        links |= BY_Z | BY_X | BY_Y
    if (plane, src) == (2, p):
        links |= (BY_X if b0 == 1 and c not in over_z_x else 0) | (BY_Y if b1 == 1 and c not in over_z_y else 0)
    if (plane, src) == (1, px):
        links |= (0 if c in corner_by_x else BY_Y) | (BY_Z if b0 == 0 and c in over_z_x else 0)
    if (plane, src) == (1, py):
        links |= (BY_X if c in corner_by_x else 0) | (BY_Z if b1 == 0 and c in over_z_y else 0)
    if (plane, src) == (2 - 2 * b1, py):
        links |= BY_X
    return links


def arrivals(heads, routes):
    queue, free, landed, tick = [], {}, {}, 0
    for c in range(heads):
        for z in range(3):
            for p in range(PLANE):
                heapq.heappush(queue, (1e-3 * c, tick, z, p, 0, p, c))
                tick += 1
    while queue:
        t, _, z, p, plane, src, c = heapq.heappop(queue)
        landed[z, p, plane, src, c] = t
        links = forwards(p, plane, src, c, routes)
        for link, z_to, p_to, plane_to in ((BY_Z, z + 1, p, plane + 1), (BY_X, z, p ^ 1, plane), (BY_Y, z, p ^ 2, plane)):
            if links & link and z_to < 3:
                start = max(t, free.get((z, p, link), 0.0))
                free[z, p, link] = start + CHUNK_US
                heapq.heappush(queue, (start + CHUNK_US + HOP_US, tick, z_to, p_to, plane_to, src, c))
                tick += 1
    return landed


def agenda(heads):
    if heads in ORDERS:
        routes, takes, orders, sinks = ORDERS[heads]
    else:
        routes, takes, orders, sinks = ((), (), ()), [], [], ((0, 0, 0),) * PLANE
        landed = arrivals(heads, routes)
        for p in range(PLANE):
            kinds = kinds_of(p)
            when = {k * heads + c: landed[2, p, *kinds[k], c] for k in range(KINDS) for c in range(heads)}
            takes.append(sorted(when, key=lambda i: (when[i], i)))
            orders.append(sorted(range(KINDS), key=lambda k: (sum(when[k * heads + c] for c in range(heads)), k)))
    plans, finals = [], []
    for p in range(PLANE):
        plan, seen = [], set()
        for i, take in enumerate(takes[p]):
            for turn in range(3):
                if sinks[p][turn] == i:
                    plan.append((SINK + turn, 0, 0))
            k, c = divmod(take, heads)
            plan.append((k, c, forwards(p, *kinds_of(p)[k], c, routes)))
            seen.add(take)
            for j in range(PAIRS):
                both = orders[p][2 * j:2 * j + 2]
                if k in both and all(i * heads + c in seen for i in both):
                    plan.append((PAIR + j, c, 0))
        for c in range(heads):
            i = max(i for i, e in enumerate(plan) if PAIR <= e[0] < LAST and e[1] == c)
            plan[i] = (plan[i][0] - PAIR + LAST, c, 0)
        final = max(i for i, e in enumerate(plan) if LAST <= e[0] < SINK)
        finals.append((plan[final][0] - LAST, plan.pop(final)[1]))
        assert len(seen) == KINDS * heads
        plan += [(NOTHING, 0, 0)] * (-len(plan) % PER_WORD)
        plans.append(plan)
    return plans, orders, finals


def kernel(
    n_seq, n_head, tile, wide, plans, orders, finals,
    win_ref, cnt_ref, bias_ref, k_hbm, v_hbm, q_hbm, w_hbm, out_ref,
    k_raw, v_raw, q_raw, k_wide, v_wide, q_wide,
    own, kv, sink, qt, low, few, lift, top, norm, acc, att, att_for, w, total, part, got,
    send_sem, recv_sem, sink_send, sink_recv, raw_sem, w_sem, part_send, part_recv,
):
    me, side = lax.axis_index("seq"), lax.axis_index("head")
    heads_kv, _, rows, width = own.shape
    lanes = qt.shape[2]
    group = lanes // rows
    heads = heads_kv * group
    model = w.shape[1]
    depth = group * width
    share = rows // n_head
    z, p = me // PLANE, lax.rem(me, PLANE)
    bit0, bit1 = lax.rem(p, 2), p // 2
    px, py = p + 1 - 2 * bit0, p + 2 - 4 * bit1
    pd = 3 - p
    base = z * PLANE
    n_z = n_seq // PLANE
    scale = LOG2E / width**0.5

    barrier = pltpu.get_barrier_semaphore()

    def greet(where):
        pl.semaphore_signal(barrier, inc=1, device_id=where, device_id_type=MESH)

    above, below = (z + 1 < n_z).astype(jnp.int32), (z > 0).astype(jnp.int32)
    loads = [
        pltpu.make_async_copy(source, target, raw_sem.at[i])
        for i, (source, target) in enumerate(((k_hbm, k_raw), (v_hbm, v_raw), (q_hbm, q_raw)))
    ]
    for load in loads:
        load.start()
    greet({"seq": base + px})
    greet({"seq": base + py})

    @pl.when(z + 1 < n_z)
    def _():
        greet({"seq": me + PLANE})

    @pl.when(z > 0)
    def _():
        greet({"seq": me - PLANE})

    for step in range(1, n_head):
        greet({"head": lax.rem(side + step, n_head)})

    def use_of(kind):
        if isinstance(kind, int):
            return SEND_USES[kind]
        return lax.shift_right_logical(jnp.int32(sum(use << (2 * k) for k, use in enumerate(SEND_USES))), 2 * kind) & 3

    def send(link, kind, c, slot, src):
        way = {BY_Z: 0, BY_X: 1, BY_Y: 2}[link]
        slot_to = slot + PLANE if link == BY_Z else slot
        return pltpu.make_async_remote_copy(
            src_ref=src,
            dst_ref=kv.at[slot_to, c],
            send_sem=send_sem.at[way, use_of(kind), c],
            recv_sem=recv_sem.at[slot_to & (2 * PLANE - 1), c],
            device_id={"seq": [me + PLANE, base + px, base + py][way]},
            device_id_type=MESH,
        )

    def own_up(c, act):
        @pl.when(z + 1 < n_z)
        def _():
            act(send(BY_Z, KINDS, c, p, own.at[c]))

    def own_aside(c, act):
        @pl.when(bit0 == 0)
        def _():
            act(send(BY_X, KINDS, c, p, own.at[c]))

        @pl.when(bit1 == 0)
        def _():
            act(send(BY_Y, KINDS, c, p, own.at[c]))

    def begin(copy):
        copy.start()

    def sent(copy):
        copy.wait_send()

    def sink_copy(way, source, target):
        return pltpu.make_async_remote_copy(
            src_ref=source,
            dst_ref=sink,
            send_sem=sink_send.at[way],
            recv_sem=sink_recv,
            device_id={"seq": target},
            device_id_type=MESH,
        )

    first_rows = own.at[:, :, pl.ds(0, SINK_ROWS)]

    for i, (raw, spread) in enumerate(((k_raw, k_wide), (v_raw, v_wide))):
        loads[i].wait()
        spread[...] = raw[...].astype(jnp.float32)
        for c in range(heads_kv):
            own[c, i] = spread[pl.ds(c, rows, stride=heads_kv), :].astype(jnp.bfloat16)
    pl.semaphore_wait(barrier, n_head + 1 + above + below)

    def sinks_on(source, act):
        @pl.when(me == 0)
        def _():
            act(sink_copy(0, source, base + px))

        @pl.when(me <= 1)
        def _():
            act(sink_copy(1, source, base + py))

        @pl.when(z + 1 < n_z)
        def _():
            act(sink_copy(2, source, me + PLANE))

    @pl.when(me == 0)
    def _():
        sinks_on(first_rows, begin)
        sink[...] = own[:, :, :SINK_ROWS]

    for c in range(heads_kv):
        if c < AHEAD:
            own_up(c, begin)
        own_aside(c, begin)

    def fetch(c):
        part_of = pl.ds(pl.multiple_of(c * depth, depth), depth)
        return pltpu.make_async_copy(w_hbm.at[part_of], w.at[part_of], w_sem.at[c])

    loads[2].wait()
    for c in range(heads_kv):
        fetch(c).start()
    q_wide[...] = q_raw[...].astype(jnp.float32)
    column = lax.broadcasted_iota(jnp.int32, (1, lanes), 1)
    for c in range(heads_kv):
        window, count, bias, token = (jnp.zeros((1, lanes), t) for t in (jnp.int32, jnp.int32, jnp.float32, jnp.int32))
        for g in range(group):
            mine = (column >= g * rows) & (column < (g + 1) * rows)
            h = c * group + g
            window = jnp.where(mine, win_ref[h], window)
            count = jnp.where(mine, cnt_ref[h], count)
            bias = jnp.where(mine, bias_ref[h], bias)
            token = jnp.where(mine, column - g * rows, token)
        token = token + me * rows
        low[c] = jnp.maximum(token - window, count - 1)
        few[c] = jnp.minimum(token, count - 1)
        lift[c] = bias * LOG2E
        picked = [q_wide[pl.ds(c * group + g, rows, stride=heads), :].astype(jnp.bfloat16) for g in range(group)]
        qt[c] = jnp.concatenate(picked, axis=0).T
        top[c] = jnp.full((1, lanes), HIDDEN, jnp.float32)
        norm[c] = jnp.zeros((1, lanes), jnp.float32)
        acc[c] = jnp.zeros((width, lanes), jnp.float32)

    step = min(256, lanes)
    parts = [slice(n, n + step) for n in range(0, lanes, step)]

    def attend(blocks, c, shards, causal=False, last=False):
        keys = [block[0] for block in blocks] + ([sink[c, 0]] if last else [])
        values = [block[1] for block in blocks] + ([sink[c, 1]] if last else [])
        turned = jnp.concatenate(values, axis=0).T
        turned = jnp.concatenate([turned, jnp.ones((SINK_ROWS, turned.shape[1]), jnp.bfloat16)], axis=0)
        key_row = lax.broadcasted_iota(jnp.int32, (rows, 1), 0)
        scores = [[jnp.dot(k, qt[c, :, cols], preferred_element_type=jnp.float32) for k in keys] for cols in parts]
        olds = [top[c, :, cols] for cols in parts]
        weights, news, fades = [], [], []
        for pieces, old, cols in zip(scores, olds, parts):
            shown = []
            for s, shard in zip(pieces, shards):
                seen = key_row > low[c, :, cols] - shard * rows
                if causal:
                    column = lax.broadcasted_iota(jnp.int32, (1, step), 1) + cols.start
                    seen = seen & (key_row <= lax.rem(column, rows))
                shown.append(jnp.where(seen, s * scale, HIDDEN))
            if last:
                sink_row = lax.broadcasted_iota(jnp.int32, (SINK_ROWS, 1), 0)
                shown.append(jnp.where(sink_row <= few[c, :, cols], pieces[-1] * scale + lift[c, :, cols], HIDDEN))
            new = old
            for s in shown:
                new = jnp.maximum(new, jnp.max(s, axis=0, keepdims=True))
            e = [jnp.exp2(s - new) for s in shown]
            weights.append(jnp.concatenate([x.astype(jnp.bfloat16) for x in e], axis=0))
            news.append(new)
            fades.append(jnp.exp2(old - new))
        adds = [jnp.dot(turned, e, preferred_element_type=jnp.float32) for e in weights]
        mixed = []
        for new, fade, add, cols in zip(news, fades, adds, parts):
            whole = acc[c, :, cols] * fade + add[:width]
            weight = norm[c, :, cols] * fade + add[width:width + 1]
            if last:
                mixed.append((whole * (1.0 / weight)).T.astype(jnp.bfloat16))
            else:
                top[c, :, cols] = new
                norm[c, :, cols] = weight
                acc[c, :, cols] = whole
        if last:
            mixed = jnp.concatenate(mixed, axis=0)
            for g in range(group):
                att[:, g * width:(g + 1) * width] = mixed[g * rows:(g + 1) * rows]
                for d in range(n_head):
                    start = g * rows + d * share
                    att_for[d, :, g * width:(g + 1) * width] = mixed[start:start + share]

    def each(body):
        def one(c, carry):
            body(c)
            return carry
        lax.fori_loop(0, heads_kv, one, 0)

    each(lambda c: attend([own.at[c]], c, [me], causal=True))
    total[...] = jnp.zeros(total.shape, jnp.float32)

    @pl.when(z < 2)
    def _():
        def clear(i, carry):
            kv[i // heads_kv, lax.rem(i, heads_kv)] = jnp.zeros(own.shape[1:], jnp.bfloat16)
            return carry
        lax.fori_loop((z + 1) * PLANE * heads_kv, 3 * PLANE * heads_kv, clear, 0)

    @pl.when((z == 0) & (me > 0))
    def _():
        sink_copy(0, sink, me).wait_recv()
        sinks_on(sink, begin)

    @pl.when(z == 0)
    def _():
        for c in range(AHEAD, heads_kv):
            own_up(c, begin)

    def rows_of(c):
        return pl.ds(pl.multiple_of(c * depth, depth), depth)

    def at_position(choices):
        chosen = choices[0]
        for q in range(1, PLANE):
            chosen = jnp.where(p == q, choices[q], chosen)
        return chosen

    def packed(codes, bits):
        word = sum(code << (bits * j) for j, code in enumerate(codes))
        return jnp.int32(word - (1 << 32) if word >> 31 else word)

    def shifted(word, bits):
        return lax.shift_right_logical(word, bits)

    head_bits = (heads_kv - 1).bit_length()
    coded = [[((kind << head_bits | c) << 3) | links for kind, c, links in plan] for plan in plans]
    words = [
        at_position([packed(codes[i:i + PER_WORD], BITS) for codes in coded])
        for i in range(0, len(plans[0]), PER_WORD)
    ]
    slots_of = [[plane * PLANE + src for plane, src in kinds_of(q)] for q in range(PLANE)]
    kind_slots = at_position([packed(slots, 4) for slots in slots_of])
    pair_slots = at_position([packed([slots[k] for k in order], 4) for slots, order in zip(slots_of, orders)])

    def pair(j, c, last=False):
        both = shifted(pair_slots, 8 * j)
        slots = [both & 15, shifted(both, 4) & 15]
        blocks = [kv.at[slot, c] for slot in slots]
        shards = [base + (slot & 3) - (slot & 12) for slot in slots]
        if last:
            attend(blocks, c, shards, last=True)
            fetch(c).wait()
        else:
            @pl.when(z >= shifted(jnp.minimum(*slots), 2))
            def _():
                attend(blocks, c, shards)

    def event(code):
        links, c, kind = code & 7, shifted(code, 3) & ((1 << head_bits) - 1), shifted(code, 3 + head_bits)

        @pl.when(kind < KINDS)
        def _():
            slot = shifted(kind_slots, 4 * kind) & 15

            @pl.when(z >= shifted(slot, 2))
            def _():
                block = kv.at[slot, c]
                send(BY_X, kind, c, slot, block).wait_recv()

                @pl.when(links != 0)
                def _():
                    @pl.when(((links & BY_Z) != 0) & (z + 1 < n_z))
                    def _():
                        send(BY_Z, kind, c, slot, block).start()

                    @pl.when((links & BY_X) != 0)
                    def _():
                        send(BY_X, kind, c, slot, block).start()

                    @pl.when((links & BY_Y) != 0)
                    def _():
                        send(BY_Y, kind, c, slot, block).start()

                    @pl.when((kind == 0) & (c + AHEAD < heads_kv))
                    def _():
                        own_up(c + AHEAD, begin)

        @pl.when(kind >= KINDS)
        def _():
            @pl.when(kind < LAST)
            def _():
                pair(kind - PAIR, c)

            @pl.when((kind >= LAST) & (kind < SINK))
            def _():
                pair(kind - LAST, c, last=True)

                def project(t, carry):
                    cols = pl.ds(pl.multiple_of(t * wide, wide), wide)
                    total[:, cols] += jnp.dot(att[...], w[rows_of(c), cols], preferred_element_type=jnp.float32)
                    return carry
                lax.fori_loop(0, model // wide, project, 0)

            @pl.when((kind == SINK + jnp.minimum(z, 3) - 1) & (z > 0))
            def _():
                sink_copy(0, sink, me).wait_recv()
                sinks_on(sink, begin)

    def pick(index, choices):
        chosen = choices[-1]
        for i in range(len(choices) - 2, -1, -1):
            chosen = jnp.where(index == i, choices[i], chosen)
        return chosen

    def few_events(i, carry):
        def one(_, word):
            event(word & ((1 << BITS) - 1))
            return shifted(word, BITS)
        lax.fori_loop(0, PER_WORD, one, pick(i, words))
        return carry
    lax.fori_loop(0, len(words), few_events, 0)

    final = at_position([c for _, c in finals])
    pair(at_position([j for j, _ in finals]), final, last=True)
    tiles = model // tile

    def give(t, step):
        return pltpu.make_async_remote_copy(
            src_ref=part.at[t, step - 1],
            dst_ref=got.at[t, step - 1],
            send_sem=part_send.at[t, step - 1],
            recv_sem=part_recv.at[t, step - 1],
            device_id={"head": lax.rem(side + step, n_head)},
            device_id_type=MESH,
        )

    def projected(t, target):
        cols = pl.ds(pl.multiple_of(t * tile, tile), tile)
        kept = total[pl.ds(pl.multiple_of(target * share, 8), share), cols]
        return kept + jnp.dot(att_for[target], w[rows_of(final), cols], preferred_element_type=jnp.float32)

    def project(t, carry):
        for step in range(1, n_head):
            part[t, step - 1] = projected(t, lax.rem(side + step, n_head)).astype(jnp.bfloat16)

        @pl.when(t >= 1)
        def _():
            for step in range(1, n_head):
                give(t - 1, step).start()
        return carry
    lax.fori_loop(0, tiles, project, 0)
    for step in range(1, n_head):
        give(tiles - 1, step).start()

    def drain(q):
        for plane in range(3):
            kinds = [(k, c, links) for k, c, links in plans[q] if k < KINDS and kinds_of(q)[k][0] == plane]

            @pl.when(z >= plane)
            def _():
                for k, c, links in kinds:
                    for link in (BY_X, BY_Y):
                        if links & link:
                            send(link, k, c, 0, own.at[0]).wait_send()

            @pl.when((z >= plane) & (z + 1 < n_z))
            def _():
                for k, c, links in kinds:
                    if links & BY_Z:
                        send(BY_Z, k, c, 0, own.at[0]).wait_send()

    for q in range(PLANE):
        @pl.when(p == q)
        def _():
            drain(q)
    for c in range(heads_kv):
        own_up(c, sent)
        own_aside(c, sent)

    @pl.when((z > 0) | (me <= 1) | (n_z > 1))
    def _():
        sinks_on(sink, sent)

    def finish(t, carry):
        whole = projected(t, side).astype(jnp.bfloat16).astype(jnp.float32)
        for step in range(1, n_head):
            give(t, step).wait_recv()
            whole = whole + got[t, step - 1].astype(jnp.float32)
        out_ref[:, pl.ds(pl.multiple_of(t * tile, tile), tile)] = whole.astype(jnp.bfloat16)
        return carry
    lax.fori_loop(0, tiles, finish, 0)

    def gone(t, carry):
        for step in range(1, n_head):
            give(t, step).wait_send()
        return carry
    lax.fori_loop(0, tiles, gone, 0)


def shards(n_seq, n_head, queries, key_rows, value_rows, windows, sink_counts, sink_bias, out_weight):
    rows, heads, width = queries.shape
    kv_heads = key_rows.shape[1]
    group = heads // kv_heads
    lanes = group * rows
    depth, model = out_weight.shape
    assert (WINDOW - 1) // rows + 1 == 2 * PLANE and n_seq % PLANE == 0
    tile, wide = min(1024, model), min(4096, model)
    tiles = model // tile
    share = rows // n_head
    bf16, f32, i32 = jnp.bfloat16, jnp.float32, jnp.int32
    vmem = pl.BlockSpec(memory_space=pltpu.VMEM)
    smem = pl.BlockSpec(memory_space=pltpu.SMEM)
    dma = pltpu.SemaphoreType.DMA
    return pl.pallas_call(
        functools.partial(kernel, n_seq, n_head, tile, wide, *agenda(kv_heads)),
        out_shape=pltpu.VMEM((share, model), bf16),
        in_specs=[smem, smem, smem] + [pl.BlockSpec(memory_space=pl.ANY)] * 4,
        out_specs=vmem,
        scratch_shapes=[
            pltpu.VMEM((rows * kv_heads, width), bf16),
            pltpu.VMEM((rows * kv_heads, width), bf16),
            pltpu.VMEM((rows * heads, width), bf16),
            pltpu.VMEM((rows * kv_heads, width), f32),
            pltpu.VMEM((rows * kv_heads, width), f32),
            pltpu.VMEM((rows * heads, width), f32),
            pltpu.VMEM((kv_heads, 2, rows, width), bf16),
            pltpu.VMEM((3 * PLANE, kv_heads, 2, rows, width), bf16),
            pltpu.VMEM((kv_heads, 2, SINK_ROWS, width), bf16),
            pltpu.VMEM((kv_heads, width, lanes), bf16),
            pltpu.VMEM((kv_heads, 1, lanes), i32),
            pltpu.VMEM((kv_heads, 1, lanes), i32),
            pltpu.VMEM((kv_heads, 1, lanes), f32),
            pltpu.VMEM((kv_heads, 1, lanes), f32),
            pltpu.VMEM((kv_heads, 1, lanes), f32),
            pltpu.VMEM((kv_heads, width, lanes), f32),
            pltpu.VMEM((rows, group * width), bf16),
            pltpu.VMEM((n_head, share, group * width), bf16),
            pltpu.VMEM((depth, model), bf16),
            pltpu.VMEM((rows, model), f32),
            pltpu.VMEM((tiles, n_head - 1, share, tile), bf16),
            pltpu.VMEM((tiles, n_head - 1, share, tile), bf16),
            dma((3, 4, kv_heads)),
            dma((2 * PLANE, kv_heads)),
            dma((3,)),
            dma,
            dma((3,)),
            dma((kv_heads,)),
            dma((tiles, n_head - 1)),
            dma((tiles, n_head - 1)),
        ],
        compiler_params=pltpu.CompilerParams(
            collective_id=0, has_side_effects=True, vmem_limit_bytes=56 * 1024 * 1024
        ),
    )(
        windows,
        sink_counts,
        sink_bias,
        key_rows.reshape(rows * kv_heads, width),
        value_rows.reshape(rows * kv_heads, width),
        queries.reshape(rows * heads, width),
        out_weight,
    )


def solution(mesh):
    in_specs = (
        P("seq", "head", None),
        P("seq", "head", None),
        P("seq", "head", None),
        P("head"),
        P("head"),
        P("head"),
        P("head", None),
    )
    body = functools.partial(shards, mesh.shape["seq"], mesh.shape["head"])
    out_specs = P(("seq", "head"), None)
    return jax.shard_map(body, mesh=mesh, in_specs=in_specs, out_specs=out_specs, check_vma=False)
```

```python
import functools
import heapq

import jax
import jax.numpy as jnp
from jax import lax
from jax.experimental import pallas as pl
from jax.experimental.pallas import tpu as pltpu
from jax.sharding import PartitionSpec as P

WINDOW = 1536
SINKS = 4
PLANE = 4
SINK_ROWS = 16
HIDDEN = -1e30
LOG2E = 1.4426950408889634
MESH = pl.DeviceIdType.MESH

KINDS = 8
PAIRS = KINDS // 2
PAIR, LAST, SINK, NOTHING = KINDS, KINDS + PAIRS, KINDS + 2 * PAIRS, KINDS + 2 * PAIRS + 3
BITS, PER_WORD = 10, 3
AHEAD = 2
SEND_USES = (1, 0, 2, 3, 0, 0, 2, 0, 0)
CHUNK_US, HOP_US = 2.13, 2.0
BY_Z, BY_X, BY_Y = 1, 2, 4
ORDERS = {
    4: (
        ((0, 3), (2,), ()),
        [
            [0, 12, 8, 40, 1, 10, 20, 24, 4, 32, 2, 3, 5, 36, 28, 9, 13, 41, 25, 14, 42, 6, 21, 37, 33, 16, 44, 15, 11, 17, 22, 38, 26, 43, 34, 27, 35, 29, 45, 30, 18, 46, 19, 31, 47, 7, 23, 39],
            [0, 20, 1, 12, 40, 21, 2, 23, 22, 8, 24, 36, 5, 4, 32, 14, 42, 6, 3, 13, 41, 9, 33, 16, 25, 37, 26, 38, 15, 28, 44, 10, 34, 43, 7, 29, 17, 27, 39, 11, 35, 45, 30, 18, 46, 19, 31, 47],
            [0, 24, 32, 1, 4, 8, 5, 2, 26, 34, 12, 25, 29, 3, 44, 9, 45, 20, 33, 36, 27, 35, 6, 21, 16, 7, 28, 40, 14, 10, 11, 47, 13, 46, 37, 18, 30, 17, 41, 42, 23, 15, 39, 22, 38, 31, 19, 43],
            [0, 1, 25, 26, 4, 2, 23, 22, 34, 24, 5, 12, 8, 3, 44, 35, 9, 45, 21, 33, 28, 40, 16, 36, 7, 14, 13, 6, 27, 10, 46, 20, 32, 15, 30, 42, 29, 41, 11, 47, 17, 37, 18, 38, 19, 39, 31, 43],
        ],
        [[6, 0, 1, 5, 3, 2, 4, 7], [1, 2, 5, 6, 0, 3, 7, 4], [6, 0, 3, 5, 4, 7, 2, 1], [0, 5, 6, 4, 7, 3, 2, 1]],
        ((1, 5, 19), (3, 17, 28), (4, 17, 27), (5, 16, 32)),
    ),
}


def kinds_of(p):
    b0, b1 = p % 2, p // 2
    px, py, pd = p ^ 1, p ^ 2, 3 - p
    return [(1, p), (2, p), (1, px), (1, py), (1, pd), (2 - 2 * b0, px), (2 - 2 * b1, py), (2 - 2 * b1, pd)]


def forwards(p, plane, src, c, routes):
    over_z_x, over_z_y, corner_by_x = routes
    b0, b1 = p % 2, p // 2
    px, py = p ^ 1, p ^ 2
    links = 0
    if (plane, src) == (0, p):
        links |= BY_Z | (BY_X if b0 == 0 else 0) | (BY_Y if b1 == 0 else 0)
    if (plane, src) == (1, p):
        links |= BY_Z | BY_X | BY_Y
    if (plane, src) == (2, p):
        links |= (BY_X if b0 == 1 and c not in over_z_x else 0) | (BY_Y if b1 == 1 and c not in over_z_y else 0)
    if (plane, src) == (1, px):
        links |= (0 if c in corner_by_x else BY_Y) | (BY_Z if b0 == 0 and c in over_z_x else 0)
    if (plane, src) == (1, py):
        links |= (BY_X if c in corner_by_x else 0) | (BY_Z if b1 == 0 and c in over_z_y else 0)
    if (plane, src) == (2 - 2 * b1, py):
        links |= BY_X
    return links


def arrivals(heads, routes):
    queue, free, landed, tick = [], {}, {}, 0
    for c in range(heads):
        for z in range(3):
            for p in range(PLANE):
                heapq.heappush(queue, (1e-3 * c, tick, z, p, 0, p, c))
                tick += 1
    while queue:
        t, _, z, p, plane, src, c = heapq.heappop(queue)
        landed[z, p, plane, src, c] = t
        links = forwards(p, plane, src, c, routes)
        for link, z_to, p_to, plane_to in ((BY_Z, z + 1, p, plane + 1), (BY_X, z, p ^ 1, plane), (BY_Y, z, p ^ 2, plane)):
            if links & link and z_to < 3:
                start = max(t, free.get((z, p, link), 0.0))
                free[z, p, link] = start + CHUNK_US
                heapq.heappush(queue, (start + CHUNK_US + HOP_US, tick, z_to, p_to, plane_to, src, c))
                tick += 1
    return landed


def agenda(heads):
    if heads in ORDERS:
        routes, listed, orders, sinks = ORDERS[heads]
    else:
        routes, listed, orders, sinks = ((), (), ()), [], [], ((0, 0, 0),) * PLANE
        landed = arrivals(heads, routes)
        for p in range(PLANE):
            kinds = kinds_of(p)
            when = {k * heads + c: landed[2, p, *kinds[k], c] for k in range(KINDS) for c in range(heads)}
            orders.append(sorted(range(KINDS), key=lambda k: (sum(when[k * heads + c] for c in range(heads)), k)))
            for j in range(PAIRS):
                for c in range(heads):
                    when[(PAIR + j) * heads + c] = max(when[k * heads + c] for k in orders[p][2 * j:2 * j + 2])
            listed.append(sorted(when, key=lambda i: (when[i], i)))
    plans, finals = [], []
    for p in range(PLANE):
        plan, seen = [], set()
        for i, item in enumerate(listed[p]):
            plan += [(SINK + turn, 0, 0) for turn in range(3) if sinks[p][turn] == i]
            k, c = divmod(item, heads)
            if k < KINDS:
                plan.append((k, c, forwards(p, *kinds_of(p)[k], c, routes)))
            else:
                assert all((i, c) in seen for i in orders[p][2 * (k - PAIR):2 * (k - PAIR) + 2])
                plan.append((k, c, 0))
            seen.add((k, c))
        assert len(seen) == len(listed[p]) == (KINDS + PAIRS) * heads
        for c in range(heads):
            i = max(i for i, e in enumerate(plan) if PAIR <= e[0] < LAST and e[1] == c)
            plan[i] = (plan[i][0] - PAIR + LAST, c, 0)
        final = max(i for i, e in enumerate(plan) if LAST <= e[0] < SINK)
        finals.append((plan[final][0] - LAST, plan.pop(final)[1]))
        for i in [i for i, e in enumerate(plan) if LAST <= e[0] < SINK][-1:]:
            plan[i] = plan[i][:2] + (1,)
        plan += [(NOTHING, 0, 0)] * (-len(plan) % PER_WORD)
        plans.append(plan)
    return plans, orders, finals


def kernel(
    n_seq, n_head, tile, wide, plans, orders, finals,
    win_ref, cnt_ref, bias_ref, k_hbm, v_hbm, q_hbm, w_hbm, out_ref,
    k_raw, v_raw, q_raw, k_wide, v_wide, q_wide,
    own, kv, sink, qt, low, few, lift, top, norm, acc, held, faded, att, att_for, w, total, leave, far_att, far_w, far_total,
    send_sem, recv_sem, sink_send, sink_recv, raw_sem, w_sem, swap_send, swap_recv,
):
    me, side = lax.axis_index("seq"), lax.axis_index("head")
    heads_kv, _, rows, width = own.shape
    lanes = qt.shape[2]
    group = lanes // rows
    heads = heads_kv * group
    model = w.shape[1]
    depth = group * width
    share = rows // n_head
    z, p = me // PLANE, lax.rem(me, PLANE)
    bit0, bit1 = lax.rem(p, 2), p // 2
    px, py = p + 1 - 2 * bit0, p + 2 - 4 * bit1
    pd = 3 - p
    base = z * PLANE
    n_z = n_seq // PLANE
    scale = LOG2E / width**0.5

    barrier = pltpu.get_barrier_semaphore()

    def greet(where):
        pl.semaphore_signal(barrier, inc=1, device_id=where, device_id_type=MESH)

    above, below = (z + 1 < n_z).astype(jnp.int32), (z > 0).astype(jnp.int32)
    loads = [
        pltpu.make_async_copy(source, target, raw_sem.at[i])
        for i, (source, target) in enumerate(((k_hbm, k_raw), (v_hbm, v_raw), (q_hbm, q_raw)))
    ]
    for load in loads:
        load.start()
    greet({"seq": base + px})
    greet({"seq": base + py})

    @pl.when(z + 1 < n_z)
    def _():
        greet({"seq": me + PLANE})

    @pl.when(z > 0)
    def _():
        greet({"seq": me - PLANE})

    for step in range(1, n_head):
        greet({"head": lax.rem(side + step, n_head)})

    def use_of(kind):
        if isinstance(kind, int):
            return SEND_USES[kind]
        return lax.shift_right_logical(jnp.int32(sum(use << (2 * k) for k, use in enumerate(SEND_USES))), 2 * kind) & 3

    def send(link, kind, c, slot, src):
        way = {BY_Z: 0, BY_X: 1, BY_Y: 2}[link]
        slot_to = slot + PLANE if link == BY_Z else slot
        return pltpu.make_async_remote_copy(
            src_ref=src,
            dst_ref=kv.at[slot_to, c],
            send_sem=send_sem.at[way, use_of(kind), c],
            recv_sem=recv_sem.at[slot_to & (2 * PLANE - 1), c],
            device_id={"seq": [me + PLANE, base + px, base + py][way]},
            device_id_type=MESH,
        )

    def own_up(c, act):
        @pl.when(z + 1 < n_z)
        def _():
            act(send(BY_Z, KINDS, c, p, own.at[c]))

    def own_aside(c, act):
        @pl.when(bit0 == 0)
        def _():
            act(send(BY_X, KINDS, c, p, own.at[c]))

        @pl.when(bit1 == 0)
        def _():
            act(send(BY_Y, KINDS, c, p, own.at[c]))

    def begin(copy):
        copy.start()

    def sent(copy):
        copy.wait_send()

    def sink_copy(way, source, target):
        return pltpu.make_async_remote_copy(
            src_ref=source,
            dst_ref=sink,
            send_sem=sink_send.at[way],
            recv_sem=sink_recv,
            device_id={"seq": target},
            device_id_type=MESH,
        )

    first_rows = own.at[:, :, pl.ds(0, SINK_ROWS)]

    for i, (raw, spread) in enumerate(((k_raw, k_wide), (v_raw, v_wide))):
        loads[i].wait()
        spread[...] = raw[...].astype(jnp.float32)
        for c in range(heads_kv):
            own[c, i] = spread[pl.ds(c, rows, stride=heads_kv), :].astype(jnp.bfloat16)
    pl.semaphore_wait(barrier, n_head + 1 + above + below)

    def sinks_on(source, act):
        @pl.when(me == 0)
        def _():
            act(sink_copy(0, source, base + px))

        @pl.when(me <= 1)
        def _():
            act(sink_copy(1, source, base + py))

        @pl.when(z + 1 < n_z)
        def _():
            act(sink_copy(2, source, me + PLANE))

    @pl.when(me == 0)
    def _():
        sinks_on(first_rows, begin)
        sink[...] = own[:, :, :SINK_ROWS]

    for c in range(heads_kv):
        if c < AHEAD:
            own_up(c, begin)
        own_aside(c, begin)

    def at_position(choices):
        chosen = choices[0]
        for q in range(1, PLANE):
            chosen = jnp.where(p == q, choices[q], chosen)
        return chosen

    def rows_of(c):
        return pl.ds(pl.multiple_of(c * depth, depth), depth)

    def fetch(c):
        return pltpu.make_async_copy(w_hbm.at[rows_of(c)], w.at[rows_of(c)], w_sem.at[c])

    final = at_position([c for _, c in finals])

    loads[2].wait()
    for c in range(heads_kv):
        fetch(lax.rem(final + c, heads_kv)).start()
    q_wide[...] = q_raw[...].astype(jnp.float32)
    column = lax.broadcasted_iota(jnp.int32, (1, lanes), 1)
    for c in range(heads_kv):
        window, count, bias, token = (jnp.zeros((1, lanes), t) for t in (jnp.int32, jnp.int32, jnp.float32, jnp.int32))
        for g in range(group):
            mine = (column >= g * rows) & (column < (g + 1) * rows)
            h = c * group + g
            window = jnp.where(mine, win_ref[h], window)
            count = jnp.where(mine, cnt_ref[h], count)
            bias = jnp.where(mine, bias_ref[h], bias)
            token = jnp.where(mine, column - g * rows, token)
        token = token + me * rows
        low[c] = jnp.maximum(token - window, count - 1)
        few[c] = jnp.minimum(token, count - 1)
        lift[c] = bias * LOG2E
        picked = [q_wide[pl.ds(c * group + g, rows, stride=heads), :].astype(jnp.bfloat16) for g in range(group)]
        qt[c] = jnp.concatenate(picked, axis=0).T
        top[c] = jnp.full((1, lanes), HIDDEN, jnp.float32)
        norm[c] = jnp.zeros((1, lanes), jnp.float32)
        acc[c] = jnp.zeros((width, lanes), jnp.float32)

    step = min(256, lanes)
    parts = [slice(n, n + step) for n in range(0, lanes, step)]

    def upright(values):
        turned = jnp.concatenate(values, axis=0).T
        return jnp.concatenate([turned, jnp.ones((SINK_ROWS, turned.shape[1]), jnp.bfloat16)], axis=0)

    def settle(blocks, c):
        turned = upright([block[1] for block in blocks])
        adds = [jnp.dot(turned, held[:, cols], preferred_element_type=jnp.float32) for cols in parts]
        for add, cols in zip(adds, parts):
            fade = faded[:, cols]
            acc[c, :, cols] = acc[c, :, cols] * fade + add[:width]
            norm[c, :, cols] = norm[c, :, cols] * fade + add[width:width + 1]

    def attend(blocks, c, shards, causal=False, last=False, owed=None):
        keys = [block[0] for block in blocks] + ([sink[c, 0]] if last else [])
        values = [block[1] for block in blocks] + ([sink[c, 1]] if last else [])
        key_row = lax.broadcasted_iota(jnp.int32, (rows, 1), 0)
        scores = [[jnp.dot(k, qt[c, :, cols], preferred_element_type=jnp.float32) for k in keys] for cols in parts]
        olds = [top[c, :, cols] for cols in parts]
        if owed is not None:
            settle(*owed)
        weights, news, fades = [], [], []
        for pieces, old, cols in zip(scores, olds, parts):
            shown = []
            for s, shard in zip(pieces, shards):
                seen = key_row > low[c, :, cols] - shard * rows
                if causal:
                    column = lax.broadcasted_iota(jnp.int32, (1, step), 1) + cols.start
                    seen = seen & (key_row <= lax.rem(column, rows))
                shown.append(jnp.where(seen, s * scale, HIDDEN))
            if last:
                sink_row = lax.broadcasted_iota(jnp.int32, (SINK_ROWS, 1), 0)
                shown.append(jnp.where(sink_row <= few[c, :, cols], pieces[-1] * scale + lift[c, :, cols], HIDDEN))
            new = old
            for s in shown:
                new = jnp.maximum(new, jnp.max(s, axis=0, keepdims=True))
            e = [jnp.exp2(s - new) for s in shown]
            weights.append(jnp.concatenate([x.astype(jnp.bfloat16) for x in e], axis=0))
            news.append(new)
            fades.append(jnp.exp2(old - new))
        if owed is not None and not last:
            for new, fade, e, cols in zip(news, fades, weights, parts):
                top[c, :, cols] = new
                faded[:, cols] = fade
                held[:, cols] = e
            return
        turned = upright(values)
        adds = [jnp.dot(turned, e, preferred_element_type=jnp.float32) for e in weights]
        mixed = []
        for new, fade, add, cols in zip(news, fades, adds, parts):
            whole = acc[c, :, cols] * fade + add[:width]
            weight = norm[c, :, cols] * fade + add[width:width + 1]
            if last:
                mixed.append((whole * (1.0 / weight)).T.astype(jnp.bfloat16))
            else:
                top[c, :, cols] = new
                norm[c, :, cols] = weight
                acc[c, :, cols] = whole
        if last:
            held[...] = jnp.zeros(held.shape, jnp.bfloat16)
            faded[...] = jnp.ones(faded.shape, jnp.float32)
            mixed = jnp.concatenate(mixed, axis=0)
            for g in range(group):
                att[:, g * width:(g + 1) * width] = mixed[g * rows:(g + 1) * rows]
                for d in range(n_head):
                    start = g * rows + d * share
                    att_for[d, :, g * width:(g + 1) * width] = mixed[start:start + share]

    def each(body):
        def one(c, carry):
            body(c)
            return carry
        lax.fori_loop(0, heads_kv, one, 0)

    each(lambda c: attend([own.at[c]], c, [me], causal=True))
    total[...] = jnp.zeros(total.shape, jnp.float32)
    held[...] = jnp.zeros(held.shape, jnp.bfloat16)
    faded[...] = jnp.ones(faded.shape, jnp.float32)
    kv[p, 0] = jnp.zeros(own.shape[1:], jnp.bfloat16)

    def swap(what, step):
        target = lax.rem(side + step, n_head)
        source, landing = [
            (w.at[rows_of(final)], far_w), (leave.at[step - 1], far_total), (att_for.at[target], far_att)
        ][what]
        return pltpu.make_async_remote_copy(
            src_ref=source,
            dst_ref=landing.at[step - 1],
            send_sem=swap_send.at[what, step - 1],
            recv_sem=swap_recv.at[what, step - 1],
            device_id={"head": target},
            device_id_type=MESH,
        )

    fetch(final).wait()
    for step in range(1, n_head):
        swap(0, step).start()

    @pl.when(z < 2)
    def _():
        def clear(i, carry):
            kv[i // heads_kv, lax.rem(i, heads_kv)] = jnp.zeros(own.shape[1:], jnp.bfloat16)
            return carry
        lax.fori_loop((z + 1) * PLANE * heads_kv, 3 * PLANE * heads_kv, clear, 0)

    @pl.when((z == 0) & (me > 0))
    def _():
        sink_copy(0, sink, me).wait_recv()
        sinks_on(sink, begin)

    @pl.when(z == 0)
    def _():
        for c in range(AHEAD, heads_kv):
            own_up(c, begin)

    def packed(codes, bits):
        word = sum(code << (bits * j) for j, code in enumerate(codes))
        return jnp.int32(word - (1 << 32) if word >> 31 else word)

    def shifted(word, bits):
        return lax.shift_right_logical(word, bits)

    head_bits = (heads_kv - 1).bit_length()
    coded = [[((kind << head_bits | c) << 3) | links for kind, c, links in plan] for plan in plans]
    words = [
        at_position([packed(codes[i:i + PER_WORD], BITS) for codes in coded])
        for i in range(0, len(plans[0]), PER_WORD)
    ]
    slots_of = [[plane * PLANE + src for plane, src in kinds_of(q)] for q in range(PLANE)]
    kind_slots = at_position([packed(slots, 4) for slots in slots_of])
    pair_slots = at_position([packed([slots[k] for k in order], 4) for slots, order in zip(slots_of, orders)])

    def slots_at(j):
        both = shifted(pair_slots, 8 * j)
        return both & 15, shifted(both, 4) & 15

    def blocks_of(debt):
        c = shifted(debt, 8)
        return [kv.at[debt & 15, c], kv.at[shifted(debt, 4) & 15, c]], c

    def pair(j, c, debt, last=False):
        slots = slots_at(j)
        blocks = [kv.at[slot, c] for slot in slots]
        shards = [base + (slot & 3) - (slot & 12) for slot in slots]
        attend(blocks, c, shards, last=last, owed=blocks_of(debt))

    no_debt = p | (p << 4)

    def event(code, debt):
        links, c, kind = code & 7, shifted(code, 3) & ((1 << head_bits) - 1), shifted(code, 3 + head_bits)

        @pl.when(kind < KINDS)
        def _():
            slot = shifted(kind_slots, 4 * kind) & 15

            @pl.when(z >= shifted(slot, 2))
            def _():
                block = kv.at[slot, c]
                send(BY_X, kind, c, slot, block).wait_recv()

                @pl.when(links != 0)
                def _():
                    @pl.when(((links & BY_Z) != 0) & (z + 1 < n_z))
                    def _():
                        send(BY_Z, kind, c, slot, block).start()

                    @pl.when((links & BY_X) != 0)
                    def _():
                        send(BY_X, kind, c, slot, block).start()

                    @pl.when((links & BY_Y) != 0)
                    def _():
                        send(BY_Y, kind, c, slot, block).start()

                    @pl.when((kind == 0) & (c + AHEAD < heads_kv))
                    def _():
                        own_up(c + AHEAD, begin)

        slots = slots_at(kind & (PAIRS - 1))
        runs = (kind >= PAIR) & (kind < LAST) & (z >= shifted(jnp.minimum(slots[0], slots[1]), 2))

        @pl.when(kind >= KINDS)
        def _():
            @pl.when(runs)
            def _():
                pair(kind - PAIR, c, debt)

            @pl.when((kind >= LAST) & (kind < SINK))
            def _():
                pair(kind - LAST, c, debt, last=True)
                fetch(c).wait()

                def project(t, carry):
                    cols = pl.ds(pl.multiple_of(t * wide, wide), wide)
                    total[:, cols] += jnp.dot(att[...], w[rows_of(c), cols], preferred_element_type=jnp.float32)
                    return carry
                lax.fori_loop(0, model // wide, project, 0)

                @pl.when(links == 1)
                def _():
                    for step in range(1, n_head):
                        target = lax.rem(side + step, n_head)
                        leave[step - 1] = total[pl.ds(pl.multiple_of(target * share, 8), share)].astype(jnp.bfloat16)
                        swap(1, step).start()

            @pl.when((kind == SINK + jnp.minimum(z, 3) - 1) & (z > 0))
            def _():
                sink_copy(0, sink, me).wait_recv()
                sinks_on(sink, begin)

        closes = (kind >= LAST) & (kind < SINK)
        return jnp.where(runs, slots[0] | (slots[1] << 4) | (c << 8), jnp.where(closes, no_debt, debt))

    def pick(index, choices):
        chosen = choices[-1]
        for i in range(len(choices) - 2, -1, -1):
            chosen = jnp.where(index == i, choices[i], chosen)
        return chosen

    def few_events(i, debt):
        def one(_, carry):
            word, debt = carry
            return shifted(word, BITS), event(word & ((1 << BITS) - 1), debt)
        return lax.fori_loop(0, PER_WORD, one, (pick(i, words), debt))[1]
    debt = lax.fori_loop(0, len(words), few_events, no_debt)

    pair(at_position([j for j, _ in finals]), final, debt, last=True)
    for step in range(1, n_head):
        swap(2, step).start()
    mine = pl.ds(pl.multiple_of(side * share, 8), share)

    def project(t, carry):
        cols = pl.ds(pl.multiple_of(t * tile, tile), tile)
        total[mine, cols] += jnp.dot(att_for[side], w[rows_of(final), cols], preferred_element_type=jnp.float32)
        return carry
    lax.fori_loop(0, model // tile, project, 0)

    def drain(q):
        for plane in range(3):
            kinds = [(k, c, links) for k, c, links in plans[q] if k < KINDS and kinds_of(q)[k][0] == plane]

            @pl.when(z >= plane)
            def _():
                for k, c, links in kinds:
                    for link in (BY_X, BY_Y):
                        if links & link:
                            send(link, k, c, 0, own.at[0]).wait_send()

            @pl.when((z >= plane) & (z + 1 < n_z))
            def _():
                for k, c, links in kinds:
                    if links & BY_Z:
                        send(BY_Z, k, c, 0, own.at[0]).wait_send()

    for q in range(PLANE):
        @pl.when(p == q)
        def _():
            drain(q)
    for c in range(heads_kv):
        own_up(c, sent)
        own_aside(c, sent)

    @pl.when((z > 0) | (me <= 1) | (n_z > 1))
    def _():
        sinks_on(sink, sent)

    exchanged = (0, 1, 2) if heads_kv > 1 else (0, 2)
    for step in range(1, n_head):
        for what in exchanged:
            swap(what, step).wait_recv()

    def finish(t, carry):
        cols = pl.ds(pl.multiple_of(t * tile, tile), tile)
        whole = total[mine, cols].astype(jnp.bfloat16).astype(jnp.float32)
        for step in range(1, n_head):
            theirs = jnp.dot(far_att[step - 1], far_w[step - 1, :, cols], preferred_element_type=jnp.float32)
            if heads_kv > 1:
                theirs = theirs + far_total[step - 1, :, cols].astype(jnp.float32)
            whole = whole + theirs.astype(jnp.bfloat16).astype(jnp.float32)
        out_ref[:, cols] = whole.astype(jnp.bfloat16)
        return carry
    lax.fori_loop(0, model // tile, finish, 0)
    for step in range(1, n_head):
        for what in exchanged:
            swap(what, step).wait_send()


def shards(n_seq, n_head, queries, key_rows, value_rows, windows, sink_counts, sink_bias, out_weight):
    rows, heads, width = queries.shape
    kv_heads = key_rows.shape[1]
    group = heads // kv_heads
    lanes = group * rows
    depth, model = out_weight.shape
    assert (WINDOW - 1) // rows + 1 == 2 * PLANE and n_seq % PLANE == 0
    tile, wide = min(4096, model), min(4096, model)
    share = rows // n_head
    bf16, f32, i32 = jnp.bfloat16, jnp.float32, jnp.int32
    vmem = pl.BlockSpec(memory_space=pltpu.VMEM)
    smem = pl.BlockSpec(memory_space=pltpu.SMEM)
    dma = pltpu.SemaphoreType.DMA
    return pl.pallas_call(
        functools.partial(kernel, n_seq, n_head, tile, wide, *agenda(kv_heads)),
        out_shape=pltpu.VMEM((share, model), bf16),
        in_specs=[smem, smem, smem] + [pl.BlockSpec(memory_space=pl.ANY)] * 4,
        out_specs=vmem,
        scratch_shapes=[
            pltpu.VMEM((rows * kv_heads, width), bf16),
            pltpu.VMEM((rows * kv_heads, width), bf16),
            pltpu.VMEM((rows * heads, width), bf16),
            pltpu.VMEM((rows * kv_heads, width), f32),
            pltpu.VMEM((rows * kv_heads, width), f32),
            pltpu.VMEM((rows * heads, width), f32),
            pltpu.VMEM((kv_heads, 2, rows, width), bf16),
            pltpu.VMEM((3 * PLANE, kv_heads, 2, rows, width), bf16),
            pltpu.VMEM((kv_heads, 2, SINK_ROWS, width), bf16),
            pltpu.VMEM((kv_heads, width, lanes), bf16),
            pltpu.VMEM((kv_heads, 1, lanes), i32),
            pltpu.VMEM((kv_heads, 1, lanes), i32),
            pltpu.VMEM((kv_heads, 1, lanes), f32),
            pltpu.VMEM((kv_heads, 1, lanes), f32),
            pltpu.VMEM((kv_heads, 1, lanes), f32),
            pltpu.VMEM((kv_heads, width, lanes), f32),
            pltpu.VMEM((2 * rows, lanes), bf16),
            pltpu.VMEM((1, lanes), f32),
            pltpu.VMEM((rows, group * width), bf16),
            pltpu.VMEM((n_head, share, group * width), bf16),
            pltpu.VMEM((depth, model), bf16),
            pltpu.VMEM((rows, model), f32),
            pltpu.VMEM((n_head - 1, share, model), bf16),
            pltpu.VMEM((n_head - 1, share, group * width), bf16),
            pltpu.VMEM((n_head - 1, group * width, model), bf16),
            pltpu.VMEM((n_head - 1, share, model), bf16),
            dma((3, 4, kv_heads)),
            dma((2 * PLANE, kv_heads)),
            dma((3,)),
            dma,
            dma((3,)),
            dma((kv_heads,)),
            dma((3, n_head - 1)),
            dma((3, n_head - 1)),
        ],
        compiler_params=pltpu.CompilerParams(
            collective_id=0, has_side_effects=True, vmem_limit_bytes=56 * 1024 * 1024
        ),
    )(
        windows,
        sink_counts,
        sink_bias,
        key_rows.reshape(rows * kv_heads, width),
        value_rows.reshape(rows * kv_heads, width),
        queries.reshape(rows * heads, width),
        out_weight,
    )


def solution(mesh):
    in_specs = (
        P("seq", "head", None),
        P("seq", "head", None),
        P("seq", "head", None),
        P("head"),
        P("head"),
        P("head"),
        P("head", None),
    )
    body = functools.partial(shards, mesh.shape["seq"], mesh.shape["head"])
    out_specs = P(("seq", "head"), None)
    return jax.shard_map(body, mesh=mesh, in_specs=in_specs, out_specs=out_specs, check_vma=False)
```

```python
import functools
import heapq

import jax
import jax.numpy as jnp
from jax import lax
from jax.experimental import pallas as pl
from jax.experimental.pallas import tpu as pltpu
from jax.sharding import PartitionSpec as P

WINDOW = 1536
SINKS = 4
PLANE = 4
SINK_ROWS = 16
HIDDEN = -1e30
LOG2E = 1.4426950408889634
MESH = pl.DeviceIdType.MESH

KINDS = 8
PAIRS = KINDS // 2
PAIR, LAST, SINK, NOTHING = KINDS, KINDS + PAIRS, KINDS + 2 * PAIRS, KINDS + 2 * PAIRS + 3
BITS, PER_WORD = 10, 3
AHEAD = 2
SEND_USES = (1, 0, 2, 2, 0, 0, 2, 0, 0)
CHUNK_US, HOP_US = 2.13, 2.0
BY_Z, BY_X, BY_Y = 1, 2, 4
ORDERS = {
    4: (
        ((0, 3), (2,), ()),
        [
            [0, 8, 12, 40, 1, 10, 20, 9, 24, 32, 2, 13, 3, 5, 4, 36, 28, 41, 25, 33, 14, 42, 6, 21, 37, 16, 44, 17, 15, 11, 43, 22, 38, 26, 34, 27, 35, 29, 45, 30, 18, 46, 19, 31, 47, 7, 23, 39],
            [0, 20, 1, 12, 23, 2, 24, 36, 21, 22, 5, 33, 8, 40, 4, 32, 14, 6, 34, 3, 13, 16, 25, 37, 26, 38, 9, 41, 28, 44, 10, 42, 15, 7, 35, 17, 27, 39, 11, 43, 29, 45, 30, 18, 46, 19, 31, 47],
            [0, 24, 32, 1, 4, 8, 44, 5, 2, 26, 34, 12, 25, 33, 29, 3, 9, 45, 20, 36, 16, 27, 35, 6, 7, 28, 40, 21, 10, 46, 14, 11, 47, 13, 37, 30, 17, 41, 18, 42, 23, 15, 39, 22, 38, 31, 19, 43],
            [0, 24, 1, 4, 21, 25, 26, 2, 23, 22, 5, 12, 40, 8, 28, 44, 3, 9, 14, 45, 13, 32, 42, 16, 41, 6, 27, 7, 10, 46, 20, 36, 15, 43, 30, 34, 29, 33, 11, 47, 17, 37, 18, 38, 19, 39, 31, 35],
        ],
        [[6, 0, 1, 5, 3, 2, 7, 4], [1, 0, 5, 6, 3, 2, 7, 4], [6, 0, 3, 5, 4, 7, 2, 1], [7, 6, 5, 4, 0, 3, 2, 1]],
        ((1, 5, 20), (4, 17, 29), (7, 23, 26), (14, 23, 31)),
    ),
}


def kinds_of(p):
    b0, b1 = p % 2, p // 2
    px, py, pd = p ^ 1, p ^ 2, 3 - p
    return [(1, p), (2, p), (1, px), (1, py), (1, pd), (2 - 2 * b0, px), (2 - 2 * b1, py), (2 - 2 * b1, pd)]


def forwards(p, plane, src, c, routes):
    over_z_x, over_z_y, corner_by_x = routes
    b0, b1 = p % 2, p // 2
    px, py = p ^ 1, p ^ 2
    links = 0
    if (plane, src) == (0, p):
        links |= BY_Z | (BY_X if b0 == 0 else 0) | (BY_Y if b1 == 0 else 0)
    if (plane, src) == (1, p):
        links |= BY_Z | BY_X | BY_Y
    if (plane, src) == (2, p):
        links |= (BY_X if b0 == 1 and c not in over_z_x else 0) | (BY_Y if b1 == 1 and c not in over_z_y else 0)
    if (plane, src) == (1, px):
        links |= (0 if c in corner_by_x else BY_Y) | (BY_Z if b0 == 0 and c in over_z_x else 0)
    if (plane, src) == (1, py):
        links |= (BY_X if c in corner_by_x else 0) | (BY_Z if b1 == 0 and c in over_z_y else 0)
    if (plane, src) == (2 - 2 * b1, py):
        links |= BY_X
    return links


def arrivals(heads, routes):
    queue, free, landed, tick = [], {}, {}, 0
    for c in range(heads):
        for z in range(3):
            for p in range(PLANE):
                heapq.heappush(queue, (1e-3 * c, tick, z, p, 0, p, c))
                tick += 1
    while queue:
        t, _, z, p, plane, src, c = heapq.heappop(queue)
        landed[z, p, plane, src, c] = t
        links = forwards(p, plane, src, c, routes)
        for link, z_to, p_to, plane_to in ((BY_Z, z + 1, p, plane + 1), (BY_X, z, p ^ 1, plane), (BY_Y, z, p ^ 2, plane)):
            if links & link and z_to < 3:
                start = max(t, free.get((z, p, link), 0.0))
                free[z, p, link] = start + CHUNK_US
                heapq.heappush(queue, (start + CHUNK_US + HOP_US, tick, z_to, p_to, plane_to, src, c))
                tick += 1
    return landed


def agenda(heads):
    if heads in ORDERS:
        routes, listed, orders, sinks = ORDERS[heads]
        assert not set(routes[0]) & set(routes[1]) and not routes[2]
    else:
        routes, listed, orders, sinks = ((), (), ()), [], [], ((0, 0, 0),) * PLANE
        landed = arrivals(heads, routes)
        for p in range(PLANE):
            kinds = kinds_of(p)
            when = {k * heads + c: landed[2, p, *kinds[k], c] for k in range(KINDS) for c in range(heads)}
            orders.append(sorted(range(KINDS), key=lambda k: (sum(when[k * heads + c] for c in range(heads)), k)))
            for j in range(PAIRS):
                for c in range(heads):
                    when[(PAIR + j) * heads + c] = max(when[k * heads + c] for k in orders[p][2 * j:2 * j + 2])
            listed.append(sorted(when, key=lambda i: (when[i], i)))
    plans, finals = [], []
    for p in range(PLANE):
        plan, seen = [], set()
        for i, item in enumerate(listed[p]):
            plan += [(SINK + turn, 0, 0) for turn in range(3) if sinks[p][turn] == i]
            k, c = divmod(item, heads)
            if k < KINDS:
                plan.append((k, c, forwards(p, *kinds_of(p)[k], c, routes)))
            else:
                assert all((i, c) in seen for i in orders[p][2 * (k - PAIR):2 * (k - PAIR) + 2])
                plan.append((k, c, 0))
            seen.add((k, c))
        assert len(seen) == len(listed[p]) == (KINDS + PAIRS) * heads
        for c in range(heads):
            i = max(i for i, e in enumerate(plan) if PAIR <= e[0] < LAST and e[1] == c)
            plan[i] = (plan[i][0] - PAIR + LAST, c, 0)
        final = max(i for i, e in enumerate(plan) if LAST <= e[0] < SINK)
        finals.append((plan[final][0] - LAST, plan.pop(final)[1]))
        for i in [i for i, e in enumerate(plan) if LAST <= e[0] < SINK][-1:]:
            plan[i] = plan[i][:2] + (1,)
        plan += [(NOTHING, 0, 0)] * (-len(plan) % PER_WORD)
        plans.append(plan)
    return plans, orders, finals


def kernel(
    n_seq, n_head, tile, wide, plans, orders, finals,
    win_hbm, cnt_hbm, bias_hbm, k_hbm, v_hbm, q_hbm, w_hbm, out_ref,
    win_ref, cnt_ref, bias_ref, k_raw, v_raw, q_raw, k_wide, v_wide, q_wide,
    own, kv, sink, qt, low, few, lift, top, norm, acc, held, faded, att, att_for, w, total, leave, far_att, far_w, far_total,
    send_sem, recv_sem, sink_send, sink_recv, raw_sem, w_sem, swap_send, swap_recv,
):
    me, side = lax.axis_index("seq"), lax.axis_index("head")
    heads_kv, _, rows, width = own.shape
    lanes = qt.shape[2]
    group = lanes // rows
    heads = heads_kv * group
    model = w.shape[1]
    depth = group * width
    share = rows // n_head
    z, p = me // PLANE, lax.rem(me, PLANE)
    bit0, bit1 = lax.rem(p, 2), p // 2
    px, py = p + 1 - 2 * bit0, p + 2 - 4 * bit1
    pd = 3 - p
    base = z * PLANE
    n_z = n_seq // PLANE
    scale = LOG2E / width**0.5

    barrier = pltpu.get_barrier_semaphore()

    def greet(where):
        pl.semaphore_signal(barrier, inc=1, device_id=where, device_id_type=MESH)

    above, below = (z + 1 < n_z).astype(jnp.int32), (z > 0).astype(jnp.int32)
    loads = [
        pltpu.make_async_copy(source, target, raw_sem.at[i])
        for i, (source, target) in enumerate((
            (k_hbm, k_raw), (v_hbm, v_raw), (q_hbm, q_raw),
            (win_hbm, win_ref), (cnt_hbm, cnt_ref), (bias_hbm, bias_ref),
        ))
    ]
    for load in loads:
        load.start()
    greet({"seq": base + px})
    greet({"seq": base + py})

    @pl.when(z + 1 < n_z)
    def _():
        greet({"seq": me + PLANE})

    @pl.when(z > 0)
    def _():
        greet({"seq": me - PLANE})

    for step in range(1, n_head):
        greet({"head": lax.rem(side + step, n_head)})

    def use_of(kind):
        if isinstance(kind, int):
            return SEND_USES[kind]
        return lax.shift_right_logical(jnp.int32(sum(use << (2 * k) for k, use in enumerate(SEND_USES))), 2 * kind) & 3

    def send(link, kind, c, slot, src):
        way = {BY_Z: 0, BY_X: 1, BY_Y: 2}[link]
        slot_to = slot + PLANE if link == BY_Z else slot
        return pltpu.make_async_remote_copy(
            src_ref=src,
            dst_ref=kv.at[slot_to, c],
            send_sem=send_sem.at[way, use_of(kind), c],
            recv_sem=recv_sem.at[slot_to & (2 * PLANE - 1), c],
            device_id={"seq": [me + PLANE, base + px, base + py][way]},
            device_id_type=MESH,
        )

    def own_up(c, act):
        @pl.when(z + 1 < n_z)
        def _():
            act(send(BY_Z, KINDS, c, p, own.at[c]))

    def own_aside(c, act):
        @pl.when(bit0 == 0)
        def _():
            act(send(BY_X, KINDS, c, p, own.at[c]))

        @pl.when(bit1 == 0)
        def _():
            act(send(BY_Y, KINDS, c, p, own.at[c]))

    def begin(copy):
        copy.start()

    def sent(copy):
        copy.wait_send()

    def sink_copy(way, source, target):
        return pltpu.make_async_remote_copy(
            src_ref=source,
            dst_ref=sink,
            send_sem=sink_send.at[way],
            recv_sem=sink_recv,
            device_id={"seq": target},
            device_id_type=MESH,
        )

    first_rows = own.at[:, :, pl.ds(0, SINK_ROWS)]

    for i, (raw, spread) in enumerate(((k_raw, k_wide), (v_raw, v_wide))):
        loads[i].wait()
        spread[...] = raw[...].astype(jnp.float32)
        for c in range(heads_kv):
            own[c, i] = spread[pl.ds(c, rows, stride=heads_kv), :].astype(jnp.bfloat16)
    pl.semaphore_wait(barrier, n_head + 1 + above + below)

    def sinks_on(source, act):
        @pl.when(me == 0)
        def _():
            act(sink_copy(0, source, base + px))

        @pl.when(me <= 1)
        def _():
            act(sink_copy(1, source, base + py))

        @pl.when(z + 1 < n_z)
        def _():
            act(sink_copy(2, source, me + PLANE))

    @pl.when(me == 0)
    def _():
        sinks_on(first_rows, begin)
        sink[...] = own[:, :, :SINK_ROWS]

    for c in range(heads_kv):
        if c < AHEAD:
            own_up(c, begin)
        if c == AHEAD:
            @pl.when(z == 0)
            def _():
                own_up(c, begin)
        own_aside(c, begin)

    def at_position(choices):
        chosen = choices[0]
        for q in range(1, PLANE):
            chosen = jnp.where(p == q, choices[q], chosen)
        return chosen

    def rows_of(c):
        return pl.ds(pl.multiple_of(c * depth, depth), depth)

    def fetch(c):
        return pltpu.make_async_copy(w_hbm.at[rows_of(c)], w.at[rows_of(c)], w_sem.at[c])

    final = at_position([c for _, c in finals])

    for load in loads[2:]:
        load.wait()
    for c in range(heads_kv):
        fetch(lax.rem(final + c, heads_kv)).start()
    q_wide[...] = q_raw[...].astype(jnp.float32)
    column = lax.broadcasted_iota(jnp.int32, (1, lanes), 1)
    for c in range(heads_kv):
        window, count, bias, token = (jnp.zeros((1, lanes), t) for t in (jnp.int32, jnp.int32, jnp.float32, jnp.int32))
        for g in range(group):
            mine = (column >= g * rows) & (column < (g + 1) * rows)
            h = c * group + g
            window = jnp.where(mine, win_ref[h], window)
            count = jnp.where(mine, cnt_ref[h], count)
            bias = jnp.where(mine, bias_ref[h], bias)
            token = jnp.where(mine, column - g * rows, token)
        token = token + me * rows
        low[c] = jnp.maximum(token - window, count - 1)
        few[c] = jnp.minimum(token, count - 1)
        lift[c] = bias * LOG2E
        picked = [q_wide[pl.ds(c * group + g, rows, stride=heads), :].astype(jnp.bfloat16) for g in range(group)]
        qt[c] = jnp.concatenate(picked, axis=0).T
        top[c] = jnp.full((1, lanes), HIDDEN, jnp.float32)
        norm[c] = jnp.zeros((1, lanes), jnp.float32)
        acc[c] = jnp.zeros((width, lanes), jnp.float32)

    step = min(256, lanes)
    parts = [slice(n, n + step) for n in range(0, lanes, step)]

    def upright(values):
        turned = jnp.concatenate(values, axis=0).T
        return jnp.concatenate([turned, jnp.ones((SINK_ROWS, turned.shape[1]), jnp.bfloat16)], axis=0)

    def settle(blocks, c):
        turned = upright([block[1] for block in blocks])
        adds = [jnp.dot(turned, held[:, cols], preferred_element_type=jnp.float32) for cols in parts]
        for add, cols in zip(adds, parts):
            fade = faded[:, cols]
            acc[c, :, cols] = acc[c, :, cols] * fade + add[:width]
            norm[c, :, cols] = norm[c, :, cols] * fade + add[width:width + 1]

    def attend(blocks, c, shards, causal=False, last=False, owed=None):
        keys = [block[0] for block in blocks] + ([sink[c, 0]] if last else [])
        values = [block[1] for block in blocks] + ([sink[c, 1]] if last else [])
        key_row = lax.broadcasted_iota(jnp.int32, (rows, 1), 0)
        scores = [[jnp.dot(k, qt[c, :, cols], preferred_element_type=jnp.float32) for k in keys] for cols in parts]
        olds = [top[c, :, cols] for cols in parts]
        if owed is not None:
            settle(*owed)
        weights, news, fades = [], [], []
        for pieces, old, cols in zip(scores, olds, parts):
            shown = []
            for s, shard in zip(pieces, shards):
                seen = key_row > low[c, :, cols] - shard * rows
                if causal:
                    column = lax.broadcasted_iota(jnp.int32, (1, step), 1) + cols.start
                    seen = seen & (key_row <= lax.rem(column, rows))
                shown.append(jnp.where(seen, s * scale, HIDDEN))
            if last:
                sink_row = lax.broadcasted_iota(jnp.int32, (SINK_ROWS, 1), 0)
                shown.append(jnp.where(sink_row <= few[c, :, cols], pieces[-1] * scale + lift[c, :, cols], HIDDEN))
            new = old
            for s in shown:
                new = jnp.maximum(new, jnp.max(s, axis=0, keepdims=True))
            e = [jnp.exp2(s - new) for s in shown]
            weights.append(jnp.concatenate([x.astype(jnp.bfloat16) for x in e], axis=0))
            news.append(new)
            fades.append(jnp.exp2(old - new))
        if owed is not None and not last:
            for new, fade, e, cols in zip(news, fades, weights, parts):
                top[c, :, cols] = new
                faded[:, cols] = fade
                held[:, cols] = e
            return
        turned = upright(values)
        adds = [jnp.dot(turned, e, preferred_element_type=jnp.float32) for e in weights]
        mixed = []
        for new, fade, add, cols in zip(news, fades, adds, parts):
            whole = acc[c, :, cols] * fade + add[:width]
            weight = norm[c, :, cols] * fade + add[width:width + 1]
            if last:
                mixed.append((whole * (1.0 / weight)).T.astype(jnp.bfloat16))
            else:
                top[c, :, cols] = new
                norm[c, :, cols] = weight
                acc[c, :, cols] = whole
        if last:
            held[...] = jnp.zeros(held.shape, jnp.bfloat16)
            faded[...] = jnp.ones(faded.shape, jnp.float32)
            mixed = jnp.concatenate(mixed, axis=0)
            for g in range(group):
                att[:, g * width:(g + 1) * width] = mixed[g * rows:(g + 1) * rows]
                for d in range(n_head):
                    start = g * rows + d * share
                    att_for[d, :, g * width:(g + 1) * width] = mixed[start:start + share]

    def each(body):
        def one(c, carry):
            body(c)
            return carry
        lax.fori_loop(0, heads_kv, one, 0)

    each(lambda c: attend([own.at[c]], c, [me], causal=True))
    total[...] = jnp.zeros(total.shape, jnp.float32)
    held[...] = jnp.zeros(held.shape, jnp.bfloat16)
    faded[...] = jnp.ones(faded.shape, jnp.float32)
    kv[p, 0] = jnp.zeros(own.shape[1:], jnp.bfloat16)

    def swap(what, step):
        target = lax.rem(side + step, n_head)
        source, landing = [
            (w.at[rows_of(final)], far_w), (leave.at[step - 1], far_total), (att_for.at[target], far_att)
        ][what]
        return pltpu.make_async_remote_copy(
            src_ref=source,
            dst_ref=landing.at[step - 1],
            send_sem=swap_send.at[what, step - 1],
            recv_sem=swap_recv.at[what, step - 1],
            device_id={"head": target},
            device_id_type=MESH,
        )

    fetch(final).wait()
    for step in range(1, n_head):
        swap(0, step).start()

    @pl.when(z < 2)
    def _():
        def clear(i, carry):
            kv[i // heads_kv, lax.rem(i, heads_kv)] = jnp.zeros(own.shape[1:], jnp.bfloat16)
            return carry
        lax.fori_loop((z + 1) * PLANE * heads_kv, 3 * PLANE * heads_kv, clear, 0)

    @pl.when((z == 0) & (me > 0))
    def _():
        sink_copy(0, sink, me).wait_recv()
        sinks_on(sink, begin)

    @pl.when(z == 0)
    def _():
        for c in range(AHEAD + 1, heads_kv):
            own_up(c, begin)

    def packed(codes, bits):
        word = sum(code << (bits * j) for j, code in enumerate(codes))
        return jnp.int32(word - (1 << 32) if word >> 31 else word)

    def shifted(word, bits):
        return lax.shift_right_logical(word, bits)

    head_bits = (heads_kv - 1).bit_length()
    coded = [[((kind << head_bits | c) << 3) | links for kind, c, links in plan] for plan in plans]
    words = [
        at_position([packed(codes[i:i + PER_WORD], BITS) for codes in coded])
        for i in range(0, len(plans[0]), PER_WORD)
    ]
    slots_of = [[plane * PLANE + src for plane, src in kinds_of(q)] for q in range(PLANE)]
    kind_slots = at_position([packed(slots, 4) for slots in slots_of])
    pair_slots = at_position([packed([slots[k] for k in order], 4) for slots, order in zip(slots_of, orders)])

    def slots_at(j):
        both = shifted(pair_slots, 8 * j)
        return both & 15, shifted(both, 4) & 15

    def blocks_of(debt):
        c = shifted(debt, 8)
        return [kv.at[debt & 15, c], kv.at[shifted(debt, 4) & 15, c]], c

    def pair(j, c, debt, last=False):
        slots = slots_at(j)
        blocks = [kv.at[slot, c] for slot in slots]
        shards = [base + (slot & 3) - (slot & 12) for slot in slots]
        attend(blocks, c, shards, last=last, owed=blocks_of(debt))

    no_debt = p | (p << 4)

    def event(code, debt):
        links, c, kind = code & 7, shifted(code, 3) & ((1 << head_bits) - 1), shifted(code, 3 + head_bits)

        @pl.when(kind < KINDS)
        def _():
            slot = shifted(kind_slots, 4 * kind) & 15

            @pl.when(z >= shifted(slot, 2))
            def _():
                block = kv.at[slot, c]
                send(BY_X, kind, c, slot, block).wait_recv()

                @pl.when(links != 0)
                def _():
                    @pl.when(((links & BY_Z) != 0) & (z + 1 < n_z))
                    def _():
                        send(BY_Z, kind, c, slot, block).start()

                    @pl.when((links & BY_X) != 0)
                    def _():
                        send(BY_X, kind, c, slot, block).start()

                    @pl.when((links & BY_Y) != 0)
                    def _():
                        send(BY_Y, kind, c, slot, block).start()

                    @pl.when((kind == 0) & (c + AHEAD < heads_kv))
                    def _():
                        own_up(c + AHEAD, begin)

        slots = slots_at(kind & (PAIRS - 1))
        runs = (kind >= PAIR) & (kind < LAST) & (z >= shifted(jnp.minimum(slots[0], slots[1]), 2))

        @pl.when(kind >= KINDS)
        def _():
            @pl.when(runs)
            def _():
                pair(kind - PAIR, c, debt)

            @pl.when((kind >= LAST) & (kind < SINK))
            def _():
                pair(kind - LAST, c, debt, last=True)
                fetch(c).wait()

                def project(t, carry):
                    cols = pl.ds(pl.multiple_of(t * wide, wide), wide)
                    total[:, cols] += jnp.dot(att[...], w[rows_of(c), cols], preferred_element_type=jnp.float32)
                    return carry
                lax.fori_loop(0, model // wide, project, 0)

                @pl.when(links == 1)
                def _():
                    for step in range(1, n_head):
                        target = lax.rem(side + step, n_head)
                        leave[step - 1] = total[pl.ds(pl.multiple_of(target * share, 8), share)].astype(jnp.bfloat16)
                        swap(1, step).start()

            @pl.when((kind == SINK + jnp.minimum(z, 3) - 1) & (z > 0))
            def _():
                sink_copy(0, sink, me).wait_recv()
                sinks_on(sink, begin)

        closes = (kind >= LAST) & (kind < SINK)
        return jnp.where(runs, slots[0] | (slots[1] << 4) | (c << 8), jnp.where(closes, no_debt, debt))

    def pick(index, choices):
        chosen = choices[-1]
        for i in range(len(choices) - 2, -1, -1):
            chosen = jnp.where(index == i, choices[i], chosen)
        return chosen

    def few_events(i, debt):
        def one(_, carry):
            word, debt = carry
            return shifted(word, BITS), event(word & ((1 << BITS) - 1), debt)
        return lax.fori_loop(0, PER_WORD, one, (pick(i, words), debt))[1]
    debt = lax.fori_loop(0, len(words), few_events, no_debt)

    pair(at_position([j for j, _ in finals]), final, debt, last=True)
    for step in range(1, n_head):
        swap(2, step).start()
    mine = pl.ds(pl.multiple_of(side * share, 8), share)

    def project(t, carry):
        cols = pl.ds(pl.multiple_of(t * tile, tile), tile)
        total[mine, cols] += jnp.dot(att_for[side], w[rows_of(final), cols], preferred_element_type=jnp.float32)
        return carry
    lax.fori_loop(0, model // tile, project, 0)

    def drain(q):
        for plane in range(3):
            kinds = [(k, c, links) for k, c, links in plans[q] if k < KINDS and kinds_of(q)[k][0] == plane]

            @pl.when(z >= plane)
            def _():
                for k, c, links in kinds:
                    for link in (BY_X, BY_Y):
                        if links & link:
                            send(link, k, c, 0, own.at[0]).wait_send()

            @pl.when((z >= plane) & (z + 1 < n_z))
            def _():
                for k, c, links in kinds:
                    if links & BY_Z:
                        send(BY_Z, k, c, 0, own.at[0]).wait_send()

    for q in range(PLANE):
        @pl.when(p == q)
        def _():
            drain(q)
    for c in range(heads_kv):
        own_up(c, sent)
        own_aside(c, sent)

    @pl.when((z > 0) | (me <= 1) | (n_z > 1))
    def _():
        sinks_on(sink, sent)

    exchanged = (0, 1, 2) if heads_kv > 1 else (0, 2)
    for step in range(1, n_head):
        for what in exchanged:
            swap(what, step).wait_recv()

    def finish(t, carry):
        cols = pl.ds(pl.multiple_of(t * tile, tile), tile)
        whole = total[mine, cols].astype(jnp.bfloat16).astype(jnp.float32)
        for step in range(1, n_head):
            theirs = jnp.dot(far_att[step - 1], far_w[step - 1, :, cols], preferred_element_type=jnp.float32)
            if heads_kv > 1:
                theirs = theirs + far_total[step - 1, :, cols].astype(jnp.float32)
            whole = whole + theirs.astype(jnp.bfloat16).astype(jnp.float32)
        out_ref[:, cols] = whole.astype(jnp.bfloat16)
        return carry
    lax.fori_loop(0, model // tile, finish, 0)
    for step in range(1, n_head):
        for what in exchanged:
            swap(what, step).wait_send()


def shards(n_seq, n_head, queries, key_rows, value_rows, windows, sink_counts, sink_bias, out_weight):
    rows, heads, width = queries.shape
    kv_heads = key_rows.shape[1]
    group = heads // kv_heads
    lanes = group * rows
    depth, model = out_weight.shape
    assert (WINDOW - 1) // rows + 1 == 2 * PLANE and n_seq % PLANE == 0
    tile, wide = min(4096, model), min(4096, model)
    share = rows // n_head
    bf16, f32, i32 = jnp.bfloat16, jnp.float32, jnp.int32
    vmem = pl.BlockSpec(memory_space=pltpu.VMEM)
    dma = pltpu.SemaphoreType.DMA
    return pl.pallas_call(
        functools.partial(kernel, n_seq, n_head, tile, wide, *agenda(kv_heads)),
        out_shape=pltpu.VMEM((share, model), bf16),
        in_specs=[pl.BlockSpec(memory_space=pl.ANY)] * 7,
        out_specs=vmem,
        scratch_shapes=[
            pltpu.SMEM((heads,), i32),
            pltpu.SMEM((heads,), i32),
            pltpu.SMEM((heads,), f32),
            pltpu.VMEM((rows * kv_heads, width), bf16),
            pltpu.VMEM((rows * kv_heads, width), bf16),
            pltpu.VMEM((rows * heads, width), bf16),
            pltpu.VMEM((rows * kv_heads, width), f32),
            pltpu.VMEM((rows * kv_heads, width), f32),
            pltpu.VMEM((rows * heads, width), f32),
            pltpu.VMEM((kv_heads, 2, rows, width), bf16),
            pltpu.VMEM((3 * PLANE, kv_heads, 2, rows, width), bf16),
            pltpu.VMEM((kv_heads, 2, SINK_ROWS, width), bf16),
            pltpu.VMEM((kv_heads, width, lanes), bf16),
            pltpu.VMEM((kv_heads, 1, lanes), i32),
            pltpu.VMEM((kv_heads, 1, lanes), i32),
            pltpu.VMEM((kv_heads, 1, lanes), f32),
            pltpu.VMEM((kv_heads, 1, lanes), f32),
            pltpu.VMEM((kv_heads, 1, lanes), f32),
            pltpu.VMEM((kv_heads, width, lanes), f32),
            pltpu.VMEM((2 * rows, lanes), bf16),
            pltpu.VMEM((1, lanes), f32),
            pltpu.VMEM((rows, group * width), bf16),
            pltpu.VMEM((n_head, share, group * width), bf16),
            pltpu.VMEM((depth, model), bf16),
            pltpu.VMEM((rows, model), f32),
            pltpu.VMEM((n_head - 1, share, model), bf16),
            pltpu.VMEM((n_head - 1, share, group * width), bf16),
            pltpu.VMEM((n_head - 1, group * width, model), bf16),
            pltpu.VMEM((n_head - 1, share, model), bf16),
            dma((3, 3, kv_heads)),
            dma((2 * PLANE, kv_heads)),
            dma((3,)),
            dma,
            dma((6,)),
            dma((kv_heads,)),
            dma((3, n_head - 1)),
            dma((3, n_head - 1)),
        ],
        compiler_params=pltpu.CompilerParams(
            collective_id=0, has_side_effects=True, vmem_limit_bytes=56 * 1024 * 1024
        ),
    )(
        windows,
        sink_counts,
        sink_bias,
        key_rows.reshape(rows * kv_heads, width),
        value_rows.reshape(rows * kv_heads, width),
        queries.reshape(rows * heads, width),
        out_weight,
    )


def solution(mesh):
    in_specs = (
        P("seq", "head", None),
        P("seq", "head", None),
        P("seq", "head", None),
        P("head"),
        P("head"),
        P("head"),
        P("head", None),
    )
    body = functools.partial(shards, mesh.shape["seq"], mesh.shape["head"])
    out_specs = P(("seq", "head"), None)
    return jax.shard_map(body, mesh=mesh, in_specs=in_specs, out_specs=out_specs, check_vma=False)
```

```python
import functools
import heapq

import jax
import jax.numpy as jnp
from jax import lax
from jax.experimental import pallas as pl
from jax.experimental.pallas import tpu as pltpu
from jax.sharding import PartitionSpec as P

WINDOW = 1536
SINKS = 4
PLANE = 4
SINK_ROWS = 16
HIDDEN = -1e30
LOG2E = 1.4426950408889634
MESH = pl.DeviceIdType.MESH

KINDS = 8
PAIRS = KINDS // 2
PAIR, LAST, SINK, NOTHING = KINDS, KINDS + PAIRS, KINDS + 2 * PAIRS, KINDS + 2 * PAIRS + 3
BITS, PER_WORD = 10, 3
AHEAD = 2
SEND_USES = (1, 0, 2, 2, 0, 0, 2, 0, 0)
CHUNK_US, HOP_US = 2.13, 2.0
BY_Z, BY_X, BY_Y = 1, 2, 4
ORDERS = {
    4: (
        ((0, 3), (2,), ()),
        [
            [0, 12, 32, 8, 9, 1, 24, 2, 10, 20, 36, 13, 33, 5, 41, 4, 40, 21, 28, 25, 37, 14, 34, 3, 6, 16, 44, 15, 35, 11, 42, 17, 22, 26, 38, 27, 29, 45, 30, 18, 46, 19, 31, 47, 7, 43, 23, 39],
            [0, 1, 20, 12, 23, 21, 2, 22, 24, 36, 5, 8, 4, 33, 40, 13, 14, 6, 34, 3, 32, 9, 28, 16, 25, 37, 26, 38, 41, 44, 10, 42, 17, 15, 7, 35, 29, 27, 39, 11, 43, 45, 30, 18, 46, 19, 31, 47],
            [24, 0, 32, 1, 4, 8, 2, 44, 5, 26, 34, 12, 25, 9, 29, 20, 3, 45, 36, 33, 6, 27, 35, 16, 21, 28, 7, 40, 10, 14, 46, 17, 11, 47, 13, 37, 18, 30, 41, 42, 23, 15, 39, 22, 38, 31, 19, 43],
            [0, 1, 25, 26, 4, 2, 23, 22, 38, 24, 5, 12, 32, 8, 3, 9, 45, 21, 37, 44, 28, 7, 14, 16, 40, 13, 33, 20, 34, 6, 27, 39, 10, 30, 46, 15, 29, 36, 35, 11, 47, 17, 41, 18, 42, 19, 31, 43],
        ],
        [[3, 0, 6, 5, 1, 2, 4, 7], [1, 0, 5, 6, 2, 3, 7, 4], [6, 0, 3, 5, 4, 7, 2, 1], [3, 0, 5, 6, 7, 4, 2, 1]],
        ((1, 6, 17), (4, 17, 29), (6, 20, 27), (13, 21, 35)),
    ),
}


def kinds_of(p):
    b0, b1 = p % 2, p // 2
    px, py, pd = p ^ 1, p ^ 2, 3 - p
    return [(1, p), (2, p), (1, px), (1, py), (1, pd), (2 - 2 * b0, px), (2 - 2 * b1, py), (2 - 2 * b1, pd)]


def forwards(p, plane, src, c, routes):
    over_z_x, over_z_y, corner_by_x = routes
    b0, b1 = p % 2, p // 2
    px, py = p ^ 1, p ^ 2
    links = 0
    if (plane, src) == (0, p):
        links |= BY_Z | (BY_X if b0 == 0 else 0) | (BY_Y if b1 == 0 else 0)
    if (plane, src) == (1, p):
        links |= BY_Z | BY_X | BY_Y
    if (plane, src) == (2, p):
        links |= (BY_X if b0 == 1 and c not in over_z_x else 0) | (BY_Y if b1 == 1 and c not in over_z_y else 0)
    if (plane, src) == (1, px):
        links |= (0 if c in corner_by_x else BY_Y) | (BY_Z if b0 == 0 and c in over_z_x else 0)
    if (plane, src) == (1, py):
        links |= (BY_X if c in corner_by_x else 0) | (BY_Z if b1 == 0 and c in over_z_y else 0)
    if (plane, src) == (2 - 2 * b1, py):
        links |= BY_X
    return links


def arrivals(heads, routes):
    queue, free, landed, tick = [], {}, {}, 0
    for c in range(heads):
        for z in range(3):
            for p in range(PLANE):
                heapq.heappush(queue, (1e-3 * c, tick, z, p, 0, p, c))
                tick += 1
    while queue:
        t, _, z, p, plane, src, c = heapq.heappop(queue)
        landed[z, p, plane, src, c] = t
        links = forwards(p, plane, src, c, routes)
        for link, z_to, p_to, plane_to in ((BY_Z, z + 1, p, plane + 1), (BY_X, z, p ^ 1, plane), (BY_Y, z, p ^ 2, plane)):
            if links & link and z_to < 3:
                start = max(t, free.get((z, p, link), 0.0))
                free[z, p, link] = start + CHUNK_US
                heapq.heappush(queue, (start + CHUNK_US + HOP_US, tick, z_to, p_to, plane_to, src, c))
                tick += 1
    return landed


def agenda(heads):
    if heads in ORDERS:
        routes, listed, orders, sinks = ORDERS[heads]
        assert not set(routes[0]) & set(routes[1]) and not routes[2]
    else:
        routes, listed, orders, sinks = ((), (), ()), [], [], ((0, 0, 0),) * PLANE
        landed = arrivals(heads, routes)
        for p in range(PLANE):
            kinds = kinds_of(p)
            when = {k * heads + c: landed[2, p, *kinds[k], c] for k in range(KINDS) for c in range(heads)}
            orders.append(sorted(range(KINDS), key=lambda k: (sum(when[k * heads + c] for c in range(heads)), k)))
            for j in range(PAIRS):
                for c in range(heads):
                    when[(PAIR + j) * heads + c] = max(when[k * heads + c] for k in orders[p][2 * j:2 * j + 2])
            listed.append(sorted(when, key=lambda i: (when[i], i)))
    plans, finals = [], []
    for p in range(PLANE):
        plan, seen = [], set()
        for i, item in enumerate(listed[p]):
            plan += [(SINK + turn, 0, 0) for turn in range(3) if sinks[p][turn] == i]
            k, c = divmod(item, heads)
            if k < KINDS:
                plan.append((k, c, forwards(p, *kinds_of(p)[k], c, routes)))
            else:
                assert all((i, c) in seen for i in orders[p][2 * (k - PAIR):2 * (k - PAIR) + 2])
                plan.append((k, c, 0))
            seen.add((k, c))
        assert len(seen) == len(listed[p]) == (KINDS + PAIRS) * heads
        for c in range(heads):
            i = max(i for i, e in enumerate(plan) if PAIR <= e[0] < LAST and e[1] == c)
            plan[i] = (plan[i][0] - PAIR + LAST, c, 0)
        final = max(i for i, e in enumerate(plan) if LAST <= e[0] < SINK)
        finals.append((plan[final][0] - LAST, plan.pop(final)[1]))
        for i in [i for i, e in enumerate(plan) if LAST <= e[0] < SINK][-1:]:
            plan[i] = plan[i][:2] + (1,)
        plan += [(NOTHING, 0, 0)] * (-len(plan) % PER_WORD)
        plans.append(plan)
    return plans, orders, finals


def kernel(
    n_seq, n_head, tile, wide, plans, orders, finals,
    win_hbm, cnt_hbm, bias_hbm, k_hbm, v_hbm, q_hbm, w_hbm, out_ref,
    win_ref, cnt_ref, bias_ref, k_raw, v_raw, q_raw, k_wide, v_wide, q_wide,
    own, kv, sink, qt, low, few, lift, top, norm, acc, held, faded, att, att_for, w, total, leave, far_att, far_w, far_total,
    send_sem, recv_sem, sink_send, sink_recv, raw_sem, w_sem, swap_send, swap_recv,
):
    me, side = lax.axis_index("seq"), lax.axis_index("head")
    heads_kv, _, rows, width = own.shape
    lanes = qt.shape[2]
    group = lanes // rows
    heads = heads_kv * group
    model = w.shape[1]
    depth = group * width
    share = rows // n_head
    z, p = me // PLANE, lax.rem(me, PLANE)
    bit0, bit1 = lax.rem(p, 2), p // 2
    px, py = p + 1 - 2 * bit0, p + 2 - 4 * bit1
    pd = 3 - p
    base = z * PLANE
    n_z = n_seq // PLANE
    scale = LOG2E / width**0.5

    barrier = pltpu.get_barrier_semaphore()

    def greet(where):
        pl.semaphore_signal(barrier, inc=1, device_id=where, device_id_type=MESH)

    above, below = (z + 1 < n_z).astype(jnp.int32), (z > 0).astype(jnp.int32)
    loads = [
        pltpu.make_async_copy(source, target, raw_sem.at[i])
        for i, (source, target) in enumerate((
            (k_hbm, k_raw), (v_hbm, v_raw), (q_hbm, q_raw),
            (win_hbm, win_ref), (cnt_hbm, cnt_ref), (bias_hbm, bias_ref),
        ))
    ]
    for load in loads:
        load.start()
    greet({"seq": base + px})
    greet({"seq": base + py})

    @pl.when(z + 1 < n_z)
    def _():
        greet({"seq": me + PLANE})

    @pl.when(z > 0)
    def _():
        greet({"seq": me - PLANE})

    for step in range(1, n_head):
        greet({"head": lax.rem(side + step, n_head)})

    def use_of(kind):
        if isinstance(kind, int):
            return SEND_USES[kind]
        return lax.shift_right_logical(jnp.int32(sum(use << (2 * k) for k, use in enumerate(SEND_USES))), 2 * kind) & 3

    def send(link, kind, c, slot, src):
        way = {BY_Z: 0, BY_X: 1, BY_Y: 2}[link]
        slot_to = slot + PLANE if link == BY_Z else slot
        return pltpu.make_async_remote_copy(
            src_ref=src,
            dst_ref=kv.at[slot_to, c],
            send_sem=send_sem.at[way, use_of(kind), c],
            recv_sem=recv_sem.at[slot_to & (2 * PLANE - 1), c],
            device_id={"seq": [me + PLANE, base + px, base + py][way]},
            device_id_type=MESH,
        )

    def own_up(c, act):
        @pl.when(z + 1 < n_z)
        def _():
            act(send(BY_Z, KINDS, c, p, own.at[c]))

    def own_aside(c, act):
        @pl.when(bit0 == 0)
        def _():
            act(send(BY_X, KINDS, c, p, own.at[c]))

        @pl.when(bit1 == 0)
        def _():
            act(send(BY_Y, KINDS, c, p, own.at[c]))

    def begin(copy):
        copy.start()

    def sent(copy):
        copy.wait_send()

    def sink_copy(way, source, target):
        return pltpu.make_async_remote_copy(
            src_ref=source,
            dst_ref=sink,
            send_sem=sink_send.at[way],
            recv_sem=sink_recv,
            device_id={"seq": target},
            device_id_type=MESH,
        )

    first_rows = own.at[:, :, pl.ds(0, SINK_ROWS)]

    for i, (raw, spread) in enumerate(((k_raw, k_wide), (v_raw, v_wide))):
        loads[i].wait()
        spread[...] = raw[...].astype(jnp.float32)
        for c in range(heads_kv):
            own[c, i] = spread[pl.ds(c, rows, stride=heads_kv), :].astype(jnp.bfloat16)
    pl.semaphore_wait(barrier, n_head + 1 + above + below)

    def sinks_on(source, act):
        @pl.when(me == 0)
        def _():
            act(sink_copy(0, source, base + px))

        @pl.when(me <= 1)
        def _():
            act(sink_copy(1, source, base + py))

        @pl.when(z + 1 < n_z)
        def _():
            act(sink_copy(2, source, me + PLANE))

    @pl.when(me == 0)
    def _():
        sinks_on(first_rows, begin)
        sink[...] = own[:, :, :SINK_ROWS]

    for c in range(heads_kv):
        if c < AHEAD:
            own_up(c, begin)
        if c == AHEAD:
            @pl.when(z == 0)
            def _():
                own_up(c, begin)
        own_aside(c, begin)

    def at_position(choices):
        chosen = choices[0]
        for q in range(1, PLANE):
            chosen = jnp.where(p == q, choices[q], chosen)
        return chosen

    def rows_of(c):
        return pl.ds(pl.multiple_of(c * depth, depth), depth)

    def fetch(c):
        return pltpu.make_async_copy(w_hbm.at[rows_of(c)], w.at[rows_of(c)], w_sem.at[c])

    final = at_position([c for _, c in finals])

    for load in loads[2:]:
        load.wait()
    for c in range(heads_kv):
        fetch(lax.rem(final + c, heads_kv)).start()
    q_wide[...] = q_raw[...].astype(jnp.float32)
    column = lax.broadcasted_iota(jnp.int32, (1, lanes), 1)
    for c in range(heads_kv):
        window, count, bias, token = (jnp.zeros((1, lanes), t) for t in (jnp.int32, jnp.int32, jnp.float32, jnp.int32))
        for g in range(group):
            mine = (column >= g * rows) & (column < (g + 1) * rows)
            h = c * group + g
            window = jnp.where(mine, win_ref[h], window)
            count = jnp.where(mine, cnt_ref[h], count)
            bias = jnp.where(mine, bias_ref[h], bias)
            token = jnp.where(mine, column - g * rows, token)
        token = token + me * rows
        low[c] = jnp.maximum(token - window, count - 1)
        few[c] = jnp.minimum(token, count - 1)
        lift[c] = bias * LOG2E
        picked = [q_wide[pl.ds(c * group + g, rows, stride=heads), :].astype(jnp.bfloat16) for g in range(group)]
        qt[c] = jnp.concatenate(picked, axis=0).T
        top[c] = jnp.full((1, lanes), HIDDEN, jnp.float32)
        norm[c] = jnp.zeros((1, lanes), jnp.float32)
        acc[c] = jnp.zeros((width, lanes), jnp.float32)

    step = min(256, lanes)
    parts = [slice(n, n + step) for n in range(0, lanes, step)]

    def upright(values):
        turned = jnp.concatenate(values, axis=0).T
        return jnp.concatenate([turned, jnp.ones((SINK_ROWS, turned.shape[1]), jnp.bfloat16)], axis=0)

    def settle(blocks, c):
        turned = upright([block[1] for block in blocks])
        adds = [jnp.dot(turned, held[:, cols], preferred_element_type=jnp.float32) for cols in parts]
        for add, cols in zip(adds, parts):
            fade = faded[:, cols]
            acc[c, :, cols] = acc[c, :, cols] * fade + add[:width]
            norm[c, :, cols] = norm[c, :, cols] * fade + add[width:width + 1]

    def attend(blocks, c, shards, causal=False, last=False, owed=None):
        keys = [block[0] for block in blocks] + ([sink[c, 0]] if last else [])
        values = [block[1] for block in blocks] + ([sink[c, 1]] if last else [])
        key_row = lax.broadcasted_iota(jnp.int32, (rows, 1), 0)
        scores = [[jnp.dot(k, qt[c, :, cols], preferred_element_type=jnp.float32) for k in keys] for cols in parts]
        olds = [top[c, :, cols] for cols in parts]
        if owed is not None:
            settle(*owed)
        weights, news, fades = [], [], []
        for pieces, old, cols in zip(scores, olds, parts):
            shown = []
            for s, shard in zip(pieces, shards):
                seen = key_row > low[c, :, cols] - shard * rows
                if causal:
                    column = lax.broadcasted_iota(jnp.int32, (1, step), 1) + cols.start
                    seen = seen & (key_row <= lax.rem(column, rows))
                shown.append(jnp.where(seen, s * scale, HIDDEN))
            if last:
                sink_row = lax.broadcasted_iota(jnp.int32, (SINK_ROWS, 1), 0)
                shown.append(jnp.where(sink_row <= few[c, :, cols], pieces[-1] * scale + lift[c, :, cols], HIDDEN))
            new = old
            for s in shown:
                new = jnp.maximum(new, jnp.max(s, axis=0, keepdims=True))
            e = [jnp.exp2(s - new) for s in shown]
            weights.append(jnp.concatenate([x.astype(jnp.bfloat16) for x in e], axis=0))
            news.append(new)
            fades.append(jnp.exp2(old - new))
        if owed is not None and not last:
            for new, fade, e, cols in zip(news, fades, weights, parts):
                top[c, :, cols] = new
                faded[:, cols] = fade
                held[:, cols] = e
            return
        turned = upright(values)
        adds = [jnp.dot(turned, e, preferred_element_type=jnp.float32) for e in weights]
        mixed = []
        for new, fade, add, cols in zip(news, fades, adds, parts):
            whole = acc[c, :, cols] * fade + add[:width]
            weight = norm[c, :, cols] * fade + add[width:width + 1]
            if last:
                mixed.append((whole * (1.0 / weight)).T.astype(jnp.bfloat16))
            else:
                top[c, :, cols] = new
                norm[c, :, cols] = weight
                acc[c, :, cols] = whole
        if last:
            held[...] = jnp.zeros(held.shape, jnp.bfloat16)
            faded[...] = jnp.ones(faded.shape, jnp.float32)
            mixed = jnp.concatenate(mixed, axis=0)
            for g in range(group):
                att[:, g * width:(g + 1) * width] = mixed[g * rows:(g + 1) * rows]
                for d in range(n_head):
                    start = g * rows + d * share
                    att_for[d, :, g * width:(g + 1) * width] = mixed[start:start + share]

    def each(body):
        def one(c, carry):
            body(c)
            return carry
        lax.fori_loop(0, heads_kv, one, 0)

    each(lambda c: attend([own.at[c]], c, [me], causal=True))
    total[...] = jnp.zeros(total.shape, jnp.float32)
    held[...] = jnp.zeros(held.shape, jnp.bfloat16)
    faded[...] = jnp.ones(faded.shape, jnp.float32)
    kv[p, 0] = jnp.zeros(own.shape[1:], jnp.bfloat16)

    def swap(what, step):
        target = lax.rem(side + step, n_head)
        source, landing = [
            (w.at[rows_of(final)], far_w), (leave.at[step - 1], far_total), (att_for.at[target], far_att)
        ][what]
        return pltpu.make_async_remote_copy(
            src_ref=source,
            dst_ref=landing.at[step - 1],
            send_sem=swap_send.at[what, step - 1],
            recv_sem=swap_recv.at[what, step - 1],
            device_id={"head": target},
            device_id_type=MESH,
        )

    fetch(final).wait()
    for step in range(1, n_head):
        swap(0, step).start()

    @pl.when(z < 2)
    def _():
        def clear(i, carry):
            kv[i // heads_kv, lax.rem(i, heads_kv)] = jnp.zeros(own.shape[1:], jnp.bfloat16)
            return carry
        lax.fori_loop((z + 1) * PLANE * heads_kv, 3 * PLANE * heads_kv, clear, 0)

    @pl.when((z == 0) & (me > 0))
    def _():
        sink_copy(0, sink, me).wait_recv()
        sinks_on(sink, begin)

    @pl.when(z == 0)
    def _():
        for c in range(AHEAD + 1, heads_kv):
            own_up(c, begin)

    def packed(codes, bits):
        word = sum(code << (bits * j) for j, code in enumerate(codes))
        return jnp.int32(word - (1 << 32) if word >> 31 else word)

    def shifted(word, bits):
        return lax.shift_right_logical(word, bits)

    head_bits = (heads_kv - 1).bit_length()
    coded = [[((kind << head_bits | c) << 3) | links for kind, c, links in plan] for plan in plans]
    words = [
        at_position([packed(codes[i:i + PER_WORD], BITS) for codes in coded])
        for i in range(0, len(plans[0]), PER_WORD)
    ]
    slots_of = [[plane * PLANE + src for plane, src in kinds_of(q)] for q in range(PLANE)]
    kind_slots = at_position([packed(slots, 4) for slots in slots_of])
    pair_slots = at_position([packed([slots[k] for k in order], 4) for slots, order in zip(slots_of, orders)])

    def slots_at(j):
        both = shifted(pair_slots, 8 * j)
        return both & 15, shifted(both, 4) & 15

    def blocks_of(debt):
        c = shifted(debt, 8)
        return [kv.at[debt & 15, c], kv.at[shifted(debt, 4) & 15, c]], c

    def pair(j, c, debt, last=False):
        slots = slots_at(j)
        blocks = [kv.at[slot, c] for slot in slots]
        shards = [base + (slot & 3) - (slot & 12) for slot in slots]
        attend(blocks, c, shards, last=last, owed=blocks_of(debt))

    no_debt = p | (p << 4)

    def event(code, debt):
        links, c, kind = code & 7, shifted(code, 3) & ((1 << head_bits) - 1), shifted(code, 3 + head_bits)

        @pl.when(kind < KINDS)
        def _():
            slot = shifted(kind_slots, 4 * kind) & 15

            @pl.when(z >= shifted(slot, 2))
            def _():
                block = kv.at[slot, c]
                send(BY_X, kind, c, slot, block).wait_recv()

                @pl.when(links != 0)
                def _():
                    @pl.when(((links & BY_Z) != 0) & (z + 1 < n_z))
                    def _():
                        send(BY_Z, kind, c, slot, block).start()

                    @pl.when((links & BY_X) != 0)
                    def _():
                        send(BY_X, kind, c, slot, block).start()

                    @pl.when((links & BY_Y) != 0)
                    def _():
                        send(BY_Y, kind, c, slot, block).start()

                    @pl.when((kind == 0) & (c + AHEAD < heads_kv))
                    def _():
                        own_up(c + AHEAD, begin)

        slots = slots_at(kind & (PAIRS - 1))
        runs = (kind >= PAIR) & (kind < LAST) & (z >= shifted(jnp.minimum(slots[0], slots[1]), 2))

        @pl.when(kind >= KINDS)
        def _():
            @pl.when(runs)
            def _():
                pair(kind - PAIR, c, debt)

            @pl.when((kind >= LAST) & (kind < SINK))
            def _():
                pair(kind - LAST, c, debt, last=True)
                fetch(c).wait()

                def project(t, carry):
                    cols = pl.ds(pl.multiple_of(t * wide, wide), wide)
                    total[:, cols] += jnp.dot(att[...], w[rows_of(c), cols], preferred_element_type=jnp.float32)
                    return carry
                lax.fori_loop(0, model // wide, project, 0)

                @pl.when(links == 1)
                def _():
                    for step in range(1, n_head):
                        target = lax.rem(side + step, n_head)
                        leave[step - 1] = total[pl.ds(pl.multiple_of(target * share, 8), share)].astype(jnp.bfloat16)
                        swap(1, step).start()

            @pl.when((kind == SINK + jnp.minimum(z, 3) - 1) & (z > 0))
            def _():
                sink_copy(0, sink, me).wait_recv()
                sinks_on(sink, begin)

        closes = (kind >= LAST) & (kind < SINK)
        return jnp.where(runs, slots[0] | (slots[1] << 4) | (c << 8), jnp.where(closes, no_debt, debt))

    def pick(index, choices):
        chosen = choices[-1]
        for i in range(len(choices) - 2, -1, -1):
            chosen = jnp.where(index == i, choices[i], chosen)
        return chosen

    def few_events(i, debt):
        def one(_, carry):
            word, debt = carry
            return shifted(word, BITS), event(word & ((1 << BITS) - 1), debt)
        return lax.fori_loop(0, PER_WORD, one, (pick(i, words), debt))[1]
    debt = lax.fori_loop(0, len(words), few_events, no_debt)

    pair(at_position([j for j, _ in finals]), final, debt, last=True)
    for step in range(1, n_head):
        swap(2, step).start()
    mine = pl.ds(pl.multiple_of(side * share, 8), share)

    def project(t, carry):
        cols = pl.ds(pl.multiple_of(t * tile, tile), tile)
        total[mine, cols] += jnp.dot(att_for[side], w[rows_of(final), cols], preferred_element_type=jnp.float32)
        return carry
    lax.fori_loop(0, model // tile, project, 0)

    def drain(q):
        for plane in range(3):
            kinds = [(k, c, links) for k, c, links in plans[q] if k < KINDS and kinds_of(q)[k][0] == plane]

            @pl.when(z >= plane)
            def _():
                for k, c, links in kinds:
                    for link in (BY_X, BY_Y):
                        if links & link:
                            send(link, k, c, 0, own.at[0]).wait_send()

            @pl.when((z >= plane) & (z + 1 < n_z))
            def _():
                for k, c, links in kinds:
                    if links & BY_Z:
                        send(BY_Z, k, c, 0, own.at[0]).wait_send()

    for q in range(PLANE):
        @pl.when(p == q)
        def _():
            drain(q)
    for c in range(heads_kv):
        own_up(c, sent)
        own_aside(c, sent)

    @pl.when((z > 0) | (me <= 1) | (n_z > 1))
    def _():
        sinks_on(sink, sent)

    exchanged = (0, 1, 2) if heads_kv > 1 else (0, 2)
    for step in range(1, n_head):
        for what in exchanged:
            swap(what, step).wait_recv()

    def finish(t, carry):
        cols = pl.ds(pl.multiple_of(t * tile, tile), tile)
        whole = total[mine, cols].astype(jnp.bfloat16).astype(jnp.float32)
        for step in range(1, n_head):
            theirs = jnp.dot(far_att[step - 1], far_w[step - 1, :, cols], preferred_element_type=jnp.float32)
            if heads_kv > 1:
                theirs = theirs + far_total[step - 1, :, cols].astype(jnp.float32)
            whole = whole + theirs.astype(jnp.bfloat16).astype(jnp.float32)
        out_ref[:, cols] = whole.astype(jnp.bfloat16)
        return carry
    lax.fori_loop(0, model // tile, finish, 0)
    for step in range(1, n_head):
        for what in exchanged:
            swap(what, step).wait_send()


def shards(n_seq, n_head, queries, key_rows, value_rows, windows, sink_counts, sink_bias, out_weight):
    rows, heads, width = queries.shape
    kv_heads = key_rows.shape[1]
    group = heads // kv_heads
    lanes = group * rows
    depth, model = out_weight.shape
    assert (WINDOW - 1) // rows + 1 == 2 * PLANE and n_seq % PLANE == 0
    tile, wide = min(4096, model), min(4096, model)
    share = rows // n_head
    bf16, f32, i32 = jnp.bfloat16, jnp.float32, jnp.int32
    vmem = pl.BlockSpec(memory_space=pltpu.VMEM)
    dma = pltpu.SemaphoreType.DMA
    return pl.pallas_call(
        functools.partial(kernel, n_seq, n_head, tile, wide, *agenda(kv_heads)),
        out_shape=pltpu.VMEM((share, model), bf16),
        in_specs=[pl.BlockSpec(memory_space=pl.ANY)] * 7,
        out_specs=vmem,
        scratch_shapes=[
            pltpu.SMEM((heads,), i32),
            pltpu.SMEM((heads,), i32),
            pltpu.SMEM((heads,), f32),
            pltpu.VMEM((rows * kv_heads, width), bf16),
            pltpu.VMEM((rows * kv_heads, width), bf16),
            pltpu.VMEM((rows * heads, width), bf16),
            pltpu.VMEM((rows * kv_heads, width), f32),
            pltpu.VMEM((rows * kv_heads, width), f32),
            pltpu.VMEM((rows * heads, width), f32),
            pltpu.VMEM((kv_heads, 2, rows, width), bf16),
            pltpu.VMEM((3 * PLANE, kv_heads, 2, rows, width), bf16),
            pltpu.VMEM((kv_heads, 2, SINK_ROWS, width), bf16),
            pltpu.VMEM((kv_heads, width, lanes), bf16),
            pltpu.VMEM((kv_heads, 1, lanes), i32),
            pltpu.VMEM((kv_heads, 1, lanes), i32),
            pltpu.VMEM((kv_heads, 1, lanes), f32),
            pltpu.VMEM((kv_heads, 1, lanes), f32),
            pltpu.VMEM((kv_heads, 1, lanes), f32),
            pltpu.VMEM((kv_heads, width, lanes), f32),
            pltpu.VMEM((2 * rows, lanes), bf16),
            pltpu.VMEM((1, lanes), f32),
            pltpu.VMEM((rows, group * width), bf16),
            pltpu.VMEM((n_head, share, group * width), bf16),
            pltpu.VMEM((depth, model), bf16),
            pltpu.VMEM((rows, model), f32),
            pltpu.VMEM((n_head - 1, share, model), bf16),
            pltpu.VMEM((n_head - 1, share, group * width), bf16),
            pltpu.VMEM((n_head - 1, group * width, model), bf16),
            pltpu.VMEM((n_head - 1, share, model), bf16),
            dma((3, 3, kv_heads)),
            dma((2 * PLANE, kv_heads)),
            dma((3,)),
            dma,
            dma((6,)),
            dma((kv_heads,)),
            dma((3, n_head - 1)),
            dma((3, n_head - 1)),
        ],
        compiler_params=pltpu.CompilerParams(
            collective_id=0, has_side_effects=True, vmem_limit_bytes=56 * 1024 * 1024
        ),
    )(
        windows,
        sink_counts,
        sink_bias,
        key_rows.reshape(rows * kv_heads, width),
        value_rows.reshape(rows * kv_heads, width),
        queries.reshape(rows * heads, width),
        out_weight,
    )


def solution(mesh):
    in_specs = (
        P("seq", "head", None),
        P("seq", "head", None),
        P("seq", "head", None),
        P("head"),
        P("head"),
        P("head"),
        P("head", None),
    )
    body = functools.partial(shards, mesh.shape["seq"], mesh.shape["head"])
    out_specs = P(("seq", "head"), None)
    return jax.shard_map(body, mesh=mesh, in_specs=in_specs, out_specs=out_specs, check_vma=False)
```

```python
import functools
import heapq

import jax
import jax.numpy as jnp
from jax import lax
from jax.experimental import pallas as pl
from jax.experimental.pallas import tpu as pltpu
from jax.sharding import PartitionSpec as P

WINDOW = 1536
SINKS = 4
PLANE = 4
SINK_ROWS = 16
HIDDEN = -1e30
LOG2E = 1.4426950408889634
MESH = pl.DeviceIdType.MESH

KINDS = 8
PAIRS = KINDS // 2
PAIR, LAST, SINK, NOTHING = KINDS, KINDS + PAIRS, KINDS + 2 * PAIRS, KINDS + 2 * PAIRS + 3
BITS, PER_WORD = 10, 3
AHEAD = 2
SEND_USES = (1, 0, 2, 2, 0, 0, 2, 0, 0)
CHUNK_US, HOP_US = 2.13, 2.0
BY_Z, BY_X, BY_Y = 1, 2, 4
ORDERS = {
    4: (
        ((0, 3), (2,), ()),
        [
            [0, 12, 32, 8, 9, 1, 24, 2, 10, 20, 36, 13, 33, 5, 41, 4, 40, 21, 28, 25, 37, 14, 34, 3, 6, 16, 44, 15, 35, 11, 42, 17, 22, 26, 38, 27, 29, 45, 30, 18, 46, 19, 31, 47, 7, 43, 23, 39],
            [0, 1, 20, 12, 23, 21, 2, 22, 24, 36, 5, 8, 4, 33, 40, 13, 14, 6, 34, 3, 32, 9, 28, 16, 25, 37, 26, 38, 41, 44, 10, 42, 17, 15, 7, 35, 29, 27, 39, 11, 43, 45, 30, 18, 46, 19, 31, 47],
            [24, 0, 32, 1, 4, 8, 2, 44, 5, 26, 34, 12, 25, 9, 29, 20, 3, 45, 36, 33, 6, 27, 35, 16, 21, 28, 7, 40, 10, 14, 46, 17, 11, 47, 13, 37, 18, 30, 41, 42, 23, 15, 39, 22, 38, 31, 19, 43],
            [0, 1, 25, 26, 4, 2, 23, 22, 38, 24, 5, 12, 32, 8, 3, 9, 45, 21, 37, 44, 28, 7, 14, 16, 40, 13, 33, 20, 34, 6, 27, 39, 10, 30, 46, 15, 29, 36, 35, 11, 47, 17, 41, 18, 42, 19, 31, 43],
        ],
        [[3, 0, 6, 5, 1, 2, 4, 7], [1, 0, 5, 6, 2, 3, 7, 4], [6, 0, 3, 5, 4, 7, 2, 1], [3, 0, 5, 6, 7, 4, 2, 1]],
        ((1, 6, 17), (4, 17, 29), (6, 20, 27), (13, 21, 35)),
    ),
}


def kinds_of(p):
    b0, b1 = p % 2, p // 2
    px, py, pd = p ^ 1, p ^ 2, 3 - p
    return [(1, p), (2, p), (1, px), (1, py), (1, pd), (2 - 2 * b0, px), (2 - 2 * b1, py), (2 - 2 * b1, pd)]


def forwards(p, plane, src, c, routes):
    over_z_x, over_z_y, corner_by_x = routes
    b0, b1 = p % 2, p // 2
    px, py = p ^ 1, p ^ 2
    links = 0
    if (plane, src) == (0, p):
        links |= BY_Z | (BY_X if b0 == 0 else 0) | (BY_Y if b1 == 0 else 0)
    if (plane, src) == (1, p):
        links |= BY_Z | BY_X | BY_Y
    if (plane, src) == (2, p):
        links |= (BY_X if b0 == 1 and c not in over_z_x else 0) | (BY_Y if b1 == 1 and c not in over_z_y else 0)
    if (plane, src) == (1, px):
        links |= (0 if c in corner_by_x else BY_Y) | (BY_Z if b0 == 0 and c in over_z_x else 0)
    if (plane, src) == (1, py):
        links |= (BY_X if c in corner_by_x else 0) | (BY_Z if b1 == 0 and c in over_z_y else 0)
    if (plane, src) == (2 - 2 * b1, py):
        links |= BY_X
    return links


def arrivals(heads, routes):
    queue, free, landed, tick = [], {}, {}, 0
    for c in range(heads):
        for z in range(3):
            for p in range(PLANE):
                heapq.heappush(queue, (1e-3 * c, tick, z, p, 0, p, c))
                tick += 1
    while queue:
        t, _, z, p, plane, src, c = heapq.heappop(queue)
        landed[z, p, plane, src, c] = t
        links = forwards(p, plane, src, c, routes)
        for link, z_to, p_to, plane_to in ((BY_Z, z + 1, p, plane + 1), (BY_X, z, p ^ 1, plane), (BY_Y, z, p ^ 2, plane)):
            if links & link and z_to < 3:
                start = max(t, free.get((z, p, link), 0.0))
                free[z, p, link] = start + CHUNK_US
                heapq.heappush(queue, (start + CHUNK_US + HOP_US, tick, z_to, p_to, plane_to, src, c))
                tick += 1
    return landed


def agenda(heads):
    if heads in ORDERS:
        routes, listed, orders, sinks = ORDERS[heads]
        assert not set(routes[0]) & set(routes[1]) and not routes[2]
    else:
        routes, listed, orders, sinks = ((), (), ()), [], [], ((0, 0, 0),) * PLANE
        landed = arrivals(heads, routes)
        for p in range(PLANE):
            kinds = kinds_of(p)
            when = {k * heads + c: landed[2, p, *kinds[k], c] for k in range(KINDS) for c in range(heads)}
            orders.append(sorted(range(KINDS), key=lambda k: (sum(when[k * heads + c] for c in range(heads)), k)))
            for j in range(PAIRS):
                for c in range(heads):
                    when[(PAIR + j) * heads + c] = max(when[k * heads + c] for k in orders[p][2 * j:2 * j + 2])
            listed.append(sorted(when, key=lambda i: (when[i], i)))
    plans, finals = [], []
    for p in range(PLANE):
        plan, seen = [], set()
        for i, item in enumerate(listed[p]):
            plan += [(SINK + turn, 0, 0) for turn in range(3) if sinks[p][turn] == i]
            k, c = divmod(item, heads)
            if k < KINDS:
                plan.append((k, c, forwards(p, *kinds_of(p)[k], c, routes)))
            else:
                assert all((i, c) in seen for i in orders[p][2 * (k - PAIR):2 * (k - PAIR) + 2])
                plan.append((k, c, 0))
            seen.add((k, c))
        assert len(seen) == len(listed[p]) == (KINDS + PAIRS) * heads
        for c in range(heads):
            i = max(i for i, e in enumerate(plan) if PAIR <= e[0] < LAST and e[1] == c)
            plan[i] = (plan[i][0] - PAIR + LAST, c, 0)
        final = max(i for i, e in enumerate(plan) if LAST <= e[0] < SINK)
        finals.append((plan[final][0] - LAST, plan.pop(final)[1]))
        for i in [i for i, e in enumerate(plan) if LAST <= e[0] < SINK][-1:]:
            plan[i] = plan[i][:2] + (1,)
        plan += [(NOTHING, 0, 0)] * (-len(plan) % PER_WORD)
        plans.append(plan)
    return plans, orders, finals


def kernel(
    n_seq, n_head, tile, wide, plans, orders, finals,
    win_hbm, cnt_hbm, bias_hbm, k_hbm, v_hbm, q_hbm, w_hbm, out_ref,
    win_ref, cnt_ref, bias_ref, k_raw, v_raw, q_raw, k_wide, v_wide, q_wide,
    own, kv, sink, qt, low, few, lift, top, norm, acc, held, faded, att, att_for, w, total, leave, far_att, far_w, far_total,
    send_sem, recv_sem, sink_send, sink_recv, raw_sem, w_sem, swap_send, swap_recv,
):
    me, side = lax.axis_index("seq"), lax.axis_index("head")
    heads_kv, _, rows, width = own.shape
    lanes = qt.shape[2]
    group = lanes // rows
    heads = heads_kv * group
    model = w.shape[1]
    depth = group * width
    share = rows // n_head
    z, p = me // PLANE, lax.rem(me, PLANE)
    bit0, bit1 = lax.rem(p, 2), p // 2
    px, py = p + 1 - 2 * bit0, p + 2 - 4 * bit1
    pd = 3 - p
    base = z * PLANE
    n_z = n_seq // PLANE
    scale = LOG2E / width**0.5

    barrier = pltpu.get_barrier_semaphore()

    def greet(where):
        pl.semaphore_signal(barrier, inc=1, device_id=where, device_id_type=MESH)

    above, below = (z + 1 < n_z).astype(jnp.int32), (z > 0).astype(jnp.int32)
    loads = [
        pltpu.make_async_copy(source, target, raw_sem.at[i])
        for i, (source, target) in enumerate((
            (k_hbm, k_raw), (v_hbm, v_raw), (q_hbm, q_raw),
            (win_hbm, win_ref), (cnt_hbm, cnt_ref), (bias_hbm, bias_ref),
        ))
    ]
    for load in loads:
        load.start()
    greet({"seq": base + px})
    greet({"seq": base + py})

    @pl.when(z + 1 < n_z)
    def _():
        greet({"seq": me + PLANE})

    @pl.when(z > 0)
    def _():
        greet({"seq": me - PLANE})

    for step in range(1, n_head):
        greet({"head": lax.rem(side + step, n_head)})

    def use_of(kind):
        if isinstance(kind, int):
            return SEND_USES[kind]
        return lax.shift_right_logical(jnp.int32(sum(use << (2 * k) for k, use in enumerate(SEND_USES))), 2 * kind) & 3

    def send(link, kind, c, slot, src):
        way = {BY_Z: 0, BY_X: 1, BY_Y: 2}[link]
        slot_to = slot + PLANE if link == BY_Z else slot
        return pltpu.make_async_remote_copy(
            src_ref=src,
            dst_ref=kv.at[slot_to, c],
            send_sem=send_sem.at[way, use_of(kind), c],
            recv_sem=recv_sem.at[slot_to & (2 * PLANE - 1), c],
            device_id={"seq": [me + PLANE, base + px, base + py][way]},
            device_id_type=MESH,
        )

    def own_up(c, act):
        @pl.when(z + 1 < n_z)
        def _():
            act(send(BY_Z, KINDS, c, p, own.at[c]))

    def own_aside(c, act):
        @pl.when(bit0 == 0)
        def _():
            act(send(BY_X, KINDS, c, p, own.at[c]))

        @pl.when(bit1 == 0)
        def _():
            act(send(BY_Y, KINDS, c, p, own.at[c]))

    def begin(copy):
        copy.start()

    def sent(copy):
        copy.wait_send()

    def sink_copy(way, source, target):
        return pltpu.make_async_remote_copy(
            src_ref=source,
            dst_ref=sink,
            send_sem=sink_send.at[way],
            recv_sem=sink_recv,
            device_id={"seq": target},
            device_id_type=MESH,
        )

    first_rows = own.at[:, :, pl.ds(0, SINK_ROWS)]

    for i, (raw, spread) in enumerate(((k_raw, k_wide), (v_raw, v_wide))):
        loads[i].wait()
        spread[...] = raw[...].astype(jnp.float32)
        for c in range(heads_kv):
            own[c, i] = spread[pl.ds(c, rows, stride=heads_kv), :].astype(jnp.bfloat16)
    pl.semaphore_wait(barrier, n_head + 1 + above + below)

    def sinks_on(source, act):
        @pl.when(me == 0)
        def _():
            act(sink_copy(0, source, base + px))

        @pl.when(me <= 1)
        def _():
            act(sink_copy(1, source, base + py))

        @pl.when(z + 1 < n_z)
        def _():
            act(sink_copy(2, source, me + PLANE))

    @pl.when(me == 0)
    def _():
        sinks_on(first_rows, begin)
        sink[...] = own[:, :, :SINK_ROWS]

    for c in range(heads_kv):
        if c < AHEAD:
            own_up(c, begin)
        if c == AHEAD:
            @pl.when(z == 0)
            def _():
                own_up(c, begin)
        own_aside(c, begin)

    def at_position(choices):
        chosen = choices[0]
        for q in range(1, PLANE):
            chosen = jnp.where(p == q, choices[q], chosen)
        return chosen

    def rows_of(c):
        return pl.ds(pl.multiple_of(c * depth, depth), depth)

    def fetch(c):
        return pltpu.make_async_copy(w_hbm.at[rows_of(c)], w.at[rows_of(c)], w_sem.at[c])

    final = at_position([c for _, c in finals])

    for load in loads[2:]:
        load.wait()
    for c in range(heads_kv):
        fetch(lax.rem(final + c, heads_kv)).start()
    q_wide[...] = q_raw[...].astype(jnp.float32)
    column = lax.broadcasted_iota(jnp.int32, (1, lanes), 1)
    for c in range(heads_kv):
        window, count, bias, token = (jnp.zeros((1, lanes), t) for t in (jnp.int32, jnp.int32, jnp.float32, jnp.int32))
        for g in range(group):
            mine = (column >= g * rows) & (column < (g + 1) * rows)
            h = c * group + g
            window = jnp.where(mine, win_ref[h], window)
            count = jnp.where(mine, cnt_ref[h], count)
            bias = jnp.where(mine, bias_ref[h], bias)
            token = jnp.where(mine, column - g * rows, token)
        token = token + me * rows
        low[c] = jnp.maximum(token - window, count - 1)
        few[c] = jnp.minimum(token, count - 1)
        lift[c] = bias * LOG2E
        picked = [q_wide[pl.ds(c * group + g, rows, stride=heads), :].astype(jnp.bfloat16) for g in range(group)]
        qt[c] = jnp.concatenate(picked, axis=0).T
        top[c] = jnp.full((1, lanes), HIDDEN, jnp.float32)
        norm[c] = jnp.zeros((1, lanes), jnp.float32)
        acc[c] = jnp.zeros((width, lanes), jnp.float32)

    step = min(256, lanes)
    parts = [slice(n, n + step) for n in range(0, lanes, step)]

    def upright(values):
        turned = jnp.concatenate(values, axis=0).T
        return jnp.concatenate([turned, jnp.ones((SINK_ROWS, turned.shape[1]), jnp.bfloat16)], axis=0)

    def settle(blocks, c):
        turned = upright([block[1] for block in blocks])
        adds = [jnp.dot(turned, held[:, cols], preferred_element_type=jnp.float32) for cols in parts]
        for add, cols in zip(adds, parts):
            fade = faded[:, cols]
            acc[c, :, cols] = acc[c, :, cols] * fade + add[:width]
            norm[c, :, cols] = norm[c, :, cols] * fade + add[width:width + 1]

    def attend(blocks, c, shards, causal=False, last=False, owed=None, clear=True):
        keys = [block[0] for block in blocks] + ([sink[c, 0]] if last else [])
        values = [block[1] for block in blocks] + ([sink[c, 1]] if last else [])
        key_row = lax.broadcasted_iota(jnp.int32, (rows, 1), 0)
        scores = [[jnp.dot(k, qt[c, :, cols], preferred_element_type=jnp.float32) for k in keys] for cols in parts]
        olds = [top[c, :, cols] for cols in parts]
        if owed is not None:
            settle(*owed)
        weights, news, fades = [], [], []
        for pieces, old, cols in zip(scores, olds, parts):
            shown = []
            for s, shard in zip(pieces, shards):
                seen = key_row > low[c, :, cols] - shard * rows
                if causal:
                    column = lax.broadcasted_iota(jnp.int32, (1, step), 1) + cols.start
                    seen = seen & (key_row <= lax.rem(column, rows))
                shown.append(jnp.where(seen, s * scale, HIDDEN))
            if last:
                sink_row = lax.broadcasted_iota(jnp.int32, (SINK_ROWS, 1), 0)
                shown.append(jnp.where(sink_row <= few[c, :, cols], pieces[-1] * scale + lift[c, :, cols], HIDDEN))
            new = old
            for s in shown:
                new = jnp.maximum(new, jnp.max(s, axis=0, keepdims=True))
            e = [jnp.exp2(s - new) for s in shown]
            weights.append(jnp.concatenate([x.astype(jnp.bfloat16) for x in e], axis=0))
            news.append(new)
            fades.append(jnp.exp2(old - new))
        if owed is not None and not last:
            for new, fade, e, cols in zip(news, fades, weights, parts):
                top[c, :, cols] = new
                faded[:, cols] = fade
                held[:, cols] = e
            return
        turned = upright(values)
        adds = [jnp.dot(turned, e, preferred_element_type=jnp.float32) for e in weights]
        mixed = []
        for new, fade, add, cols in zip(news, fades, adds, parts):
            whole = acc[c, :, cols] * fade + add[:width]
            weight = norm[c, :, cols] * fade + add[width:width + 1]
            if last:
                mixed.append((whole * (1.0 / weight)).T.astype(jnp.bfloat16))
            else:
                top[c, :, cols] = new
                norm[c, :, cols] = weight
                acc[c, :, cols] = whole
        if last:
            if clear:
                held[...] = jnp.zeros(held.shape, jnp.bfloat16)
                faded[...] = jnp.ones(faded.shape, jnp.float32)
            mixed = jnp.concatenate(mixed, axis=0)
            for g in range(group):
                att[:, g * width:(g + 1) * width] = mixed[g * rows:(g + 1) * rows]
                for d in range(n_head):
                    start = g * rows + d * share
                    att_for[d, :, g * width:(g + 1) * width] = mixed[start:start + share]

    def each(body):
        def one(c, carry):
            body(c)
            return carry
        lax.fori_loop(0, heads_kv, one, 0)

    each(lambda c: attend([own.at[c]], c, [me], causal=True))
    total[...] = jnp.zeros(total.shape, jnp.float32)
    held[...] = jnp.zeros(held.shape, jnp.bfloat16)
    faded[...] = jnp.ones(faded.shape, jnp.float32)
    kv[p, 0] = jnp.zeros(own.shape[1:], jnp.bfloat16)

    def swap(what, step):
        target = lax.rem(side + step, n_head)
        source, landing = [
            (w.at[rows_of(final)], far_w), (leave.at[step - 1], far_total), (att_for.at[target], far_att)
        ][what]
        return pltpu.make_async_remote_copy(
            src_ref=source,
            dst_ref=landing.at[step - 1],
            send_sem=swap_send.at[what, step - 1],
            recv_sem=swap_recv.at[what, step - 1],
            device_id={"head": target},
            device_id_type=MESH,
        )

    fetch(final).wait()
    for step in range(1, n_head):
        swap(0, step).start()

    @pl.when(z < 2)
    def _():
        def clear(i, carry):
            kv[i // heads_kv, lax.rem(i, heads_kv)] = jnp.zeros(own.shape[1:], jnp.bfloat16)
            return carry
        lax.fori_loop((z + 1) * PLANE * heads_kv, 3 * PLANE * heads_kv, clear, 0)

    @pl.when((z == 0) & (me > 0))
    def _():
        sink_copy(0, sink, me).wait_recv()
        sinks_on(sink, begin)

    @pl.when(z == 0)
    def _():
        for c in range(AHEAD + 1, heads_kv):
            own_up(c, begin)

    def packed(codes, bits):
        word = sum(code << (bits * j) for j, code in enumerate(codes))
        return jnp.int32(word - (1 << 32) if word >> 31 else word)

    def shifted(word, bits):
        return lax.shift_right_logical(word, bits)

    head_bits = (heads_kv - 1).bit_length()
    coded = [[((kind << head_bits | c) << 3) | links for kind, c, links in plan] for plan in plans]
    words = [
        at_position([packed(codes[i:i + PER_WORD], BITS) for codes in coded])
        for i in range(0, len(plans[0]), PER_WORD)
    ]
    slots_of = [[plane * PLANE + src for plane, src in kinds_of(q)] for q in range(PLANE)]
    kind_slots = at_position([packed(slots, 4) for slots in slots_of])
    pair_slots = at_position([packed([slots[k] for k in order], 4) for slots, order in zip(slots_of, orders)])

    def slots_at(j):
        both = shifted(pair_slots, 8 * j)
        return both & 15, shifted(both, 4) & 15

    def blocks_of(debt):
        c = shifted(debt, 8)
        return [kv.at[debt & 15, c], kv.at[shifted(debt, 4) & 15, c]], c

    def pair(j, c, debt, last=False, clear=True):
        slots = slots_at(j)
        blocks = [kv.at[slot, c] for slot in slots]
        shards = [base + (slot & 3) - (slot & 12) for slot in slots]
        attend(blocks, c, shards, last=last, owed=blocks_of(debt), clear=clear)

    no_debt = p | (p << 4)

    def event(code, debt):
        links, c, kind = code & 7, shifted(code, 3) & ((1 << head_bits) - 1), shifted(code, 3 + head_bits)

        @pl.when(kind < KINDS)
        def _():
            slot = shifted(kind_slots, 4 * kind) & 15

            @pl.when(z >= shifted(slot, 2))
            def _():
                block = kv.at[slot, c]
                send(BY_X, kind, c, slot, block).wait_recv()

                @pl.when(links != 0)
                def _():
                    @pl.when(((links & BY_Z) != 0) & (z + 1 < n_z))
                    def _():
                        send(BY_Z, kind, c, slot, block).start()

                    @pl.when((links & BY_X) != 0)
                    def _():
                        send(BY_X, kind, c, slot, block).start()

                    @pl.when((links & BY_Y) != 0)
                    def _():
                        send(BY_Y, kind, c, slot, block).start()

                    @pl.when((kind == 0) & (c + AHEAD < heads_kv))
                    def _():
                        own_up(c + AHEAD, begin)

        slots = slots_at(kind & (PAIRS - 1))
        runs = (kind >= PAIR) & (kind < LAST) & (z >= shifted(jnp.minimum(slots[0], slots[1]), 2))

        @pl.when(kind >= KINDS)
        def _():
            @pl.when(runs)
            def _():
                pair(kind - PAIR, c, debt)

            @pl.when((kind >= LAST) & (kind < SINK))
            def _():
                pair(kind - LAST, c, debt, last=True)
                fetch(c).wait()

                def project(t, carry):
                    cols = pl.ds(pl.multiple_of(t * wide, wide), wide)
                    total[:, cols] += jnp.dot(att[...], w[rows_of(c), cols], preferred_element_type=jnp.float32)
                    return carry
                lax.fori_loop(0, model // wide, project, 0)

                @pl.when(links == 1)
                def _():
                    for step in range(1, n_head):
                        target = lax.rem(side + step, n_head)
                        leave[step - 1] = total[pl.ds(pl.multiple_of(target * share, 8), share)].astype(jnp.bfloat16)
                        swap(1, step).start()

            @pl.when((kind == SINK + jnp.minimum(z, 3) - 1) & (z > 0))
            def _():
                sink_copy(0, sink, me).wait_recv()
                sinks_on(sink, begin)

        closes = (kind >= LAST) & (kind < SINK)
        return jnp.where(runs, slots[0] | (slots[1] << 4) | (c << 8), jnp.where(closes, no_debt, debt))

    def pick(index, choices):
        chosen = choices[-1]
        for i in range(len(choices) - 2, -1, -1):
            chosen = jnp.where(index == i, choices[i], chosen)
        return chosen

    def few_events(i, debt):
        def one(_, carry):
            word, debt = carry
            return shifted(word, BITS), event(word & ((1 << BITS) - 1), debt)
        return lax.fori_loop(0, PER_WORD, one, (pick(i, words), debt))[1]
    debt = lax.fori_loop(0, len(words), few_events, no_debt)

    pair(at_position([j for j, _ in finals]), final, debt, last=True, clear=False)
    for step in range(1, n_head):
        swap(2, step).start()
    mine = pl.ds(pl.multiple_of(side * share, 8), share)

    def project(t, carry):
        cols = pl.ds(pl.multiple_of(t * tile, tile), tile)
        total[mine, cols] += jnp.dot(att_for[side], w[rows_of(final), cols], preferred_element_type=jnp.float32)
        return carry
    lax.fori_loop(0, model // tile, project, 0)

    def drain(q):
        for plane in range(3):
            kinds = [(k, c, links) for k, c, links in plans[q] if k < KINDS and kinds_of(q)[k][0] == plane]

            @pl.when(z >= plane)
            def _():
                for k, c, links in kinds:
                    for link in (BY_X, BY_Y):
                        if links & link:
                            send(link, k, c, 0, own.at[0]).wait_send()

            @pl.when((z >= plane) & (z + 1 < n_z))
            def _():
                for k, c, links in kinds:
                    if links & BY_Z:
                        send(BY_Z, k, c, 0, own.at[0]).wait_send()

    for q in range(PLANE):
        @pl.when(p == q)
        def _():
            drain(q)
    for c in range(heads_kv):
        own_up(c, sent)
        own_aside(c, sent)

    @pl.when((z > 0) | (me <= 1) | (n_z > 1))
    def _():
        sinks_on(sink, sent)

    exchanged = (0, 1, 2) if heads_kv > 1 else (0, 2)
    for step in range(1, n_head):
        for what in exchanged:
            swap(what, step).wait_recv()

    def finish(t, carry):
        cols = pl.ds(pl.multiple_of(t * tile, tile), tile)
        whole = total[mine, cols].astype(jnp.bfloat16).astype(jnp.float32)
        for step in range(1, n_head):
            theirs = jnp.dot(far_att[step - 1], far_w[step - 1, :, cols], preferred_element_type=jnp.float32)
            if heads_kv > 1:
                theirs = theirs + far_total[step - 1, :, cols].astype(jnp.float32)
            whole = whole + theirs.astype(jnp.bfloat16).astype(jnp.float32)
        out_ref[:, cols] = whole.astype(jnp.bfloat16)
        return carry
    lax.fori_loop(0, model // tile, finish, 0)
    for step in range(1, n_head):
        for what in exchanged:
            swap(what, step).wait_send()


def shards(n_seq, n_head, queries, key_rows, value_rows, windows, sink_counts, sink_bias, out_weight):
    rows, heads, width = queries.shape
    kv_heads = key_rows.shape[1]
    group = heads // kv_heads
    lanes = group * rows
    depth, model = out_weight.shape
    assert (WINDOW - 1) // rows + 1 == 2 * PLANE and n_seq % PLANE == 0
    tile, wide = min(4096, model), min(4096, model)
    share = rows // n_head
    bf16, f32, i32 = jnp.bfloat16, jnp.float32, jnp.int32
    vmem = pl.BlockSpec(memory_space=pltpu.VMEM)
    dma = pltpu.SemaphoreType.DMA
    return pl.pallas_call(
        functools.partial(kernel, n_seq, n_head, tile, wide, *agenda(kv_heads)),
        out_shape=pltpu.VMEM((share, model), bf16),
        in_specs=[pl.BlockSpec(memory_space=pl.ANY)] * 7,
        out_specs=vmem,
        scratch_shapes=[
            pltpu.SMEM((heads,), i32),
            pltpu.SMEM((heads,), i32),
            pltpu.SMEM((heads,), f32),
            pltpu.VMEM((rows * kv_heads, width), bf16),
            pltpu.VMEM((rows * kv_heads, width), bf16),
            pltpu.VMEM((rows * heads, width), bf16),
            pltpu.VMEM((rows * kv_heads, width), f32),
            pltpu.VMEM((rows * kv_heads, width), f32),
            pltpu.VMEM((rows * heads, width), f32),
            pltpu.VMEM((kv_heads, 2, rows, width), bf16),
            pltpu.VMEM((3 * PLANE, kv_heads, 2, rows, width), bf16),
            pltpu.VMEM((kv_heads, 2, SINK_ROWS, width), bf16),
            pltpu.VMEM((kv_heads, width, lanes), bf16),
            pltpu.VMEM((kv_heads, 1, lanes), i32),
            pltpu.VMEM((kv_heads, 1, lanes), i32),
            pltpu.VMEM((kv_heads, 1, lanes), f32),
            pltpu.VMEM((kv_heads, 1, lanes), f32),
            pltpu.VMEM((kv_heads, 1, lanes), f32),
            pltpu.VMEM((kv_heads, width, lanes), f32),
            pltpu.VMEM((2 * rows, lanes), bf16),
            pltpu.VMEM((1, lanes), f32),
            pltpu.VMEM((rows, group * width), bf16),
            pltpu.VMEM((n_head, share, group * width), bf16),
            pltpu.VMEM((depth, model), bf16),
            pltpu.VMEM((rows, model), f32),
            pltpu.VMEM((n_head - 1, share, model), bf16),
            pltpu.VMEM((n_head - 1, share, group * width), bf16),
            pltpu.VMEM((n_head - 1, group * width, model), bf16),
            pltpu.VMEM((n_head - 1, share, model), bf16),
            dma((3, 3, kv_heads)),
            dma((2 * PLANE, kv_heads)),
            dma((3,)),
            dma,
            dma((6,)),
            dma((kv_heads,)),
            dma((3, n_head - 1)),
            dma((3, n_head - 1)),
        ],
        compiler_params=pltpu.CompilerParams(
            collective_id=0, has_side_effects=True, vmem_limit_bytes=56 * 1024 * 1024
        ),
    )(
        windows,
        sink_counts,
        sink_bias,
        key_rows.reshape(rows * kv_heads, width),
        value_rows.reshape(rows * kv_heads, width),
        queries.reshape(rows * heads, width),
        out_weight,
    )


def solution(mesh):
    in_specs = (
        P("seq", "head", None),
        P("seq", "head", None),
        P("seq", "head", None),
        P("head"),
        P("head"),
        P("head"),
        P("head", None),
    )
    body = functools.partial(shards, mesh.shape["seq"], mesh.shape["head"])
    out_specs = P(("seq", "head"), None)
    return jax.shard_map(body, mesh=mesh, in_specs=in_specs, out_specs=out_specs, check_vma=False)
```
